32 devices in a mesh: cube: 2 (over x), chan: 8 (over z, y), split: 2 (over core).
Axes of the slice: x: 2, y: 2, z: 4, core: 2. Of those that a mesh axis runs over, the one named last changes fastest.
Arguments:
- sky_image: bfloat16 [16, 8, 1, 2, 512, 128], P(('cube', 'chan'), None, None, 'split'), parts along dimension 0, may hold values from 0 to 8
- dirty_image: bfloat16 [16, 8, 1, 2, 512, 128], P(('cube', 'chan'), None, None, 'split'), parts along dimension 0, may hold values from -6 to 6
- uv_weights: int32 [16, 1024, 512], P(('cube', 'chan'), 'split'), parts along dimension 0, may hold values from 0 to 7
- dual_coeffs: bfloat16 [4, 16, 8, 2, 512, 128], P(None, 'cube', 'chan', 'split'), parts along dimension 1, may hold values from -3 to 3
- support_mask: int32 [8, 2, 512, 128], P('chan', 'split'), may hold values 0 or 1
- row_taps: float32 [4, 17], replicated, may hold values from -1.5 to 1.5
- col_taps: float32 [4, 17], replicated, may hold values from -1.5 to 1.5
Outputs:
- new_image: bfloat16 [16, 8, 1, 2, 512, 128], P(('cube', 'chan'), None, None, 'split'), parts along dimension 0
- new_dual: bfloat16 [4, 16, 8, 2, 512, 128], P(None, 'cube', 'chan', 'split'), parts along dimension 1
The draws below stay inside these ranges and needn't reach their ends.
There are 2 independent parts, one for each index of `cube`. The reference program is written for one: setup_inputs(seed, part) draws one part's arguments, and reference() takes and returns one part's arrays. A program takes and returns all parts, laid end to end along the dimension named above; an argument that names none is the same for every part. Nothing has to cross between parts.
All inputs are finite; a program needn't handle non-finite values. No bound on the sum of `support_mask` on one device may be relied on, other than what follows from the above.
Results may differ from the reference program's by a relative error of at most 0.015.
Values may be sent and summed in bfloat16 or wider, within the bound.
No kernel may reach another device: no remote copies, remote signals or barrier semaphores. Data moves between devices by JAX's collectives and lax.ppermute only.
A program may use at most 128 MiB of HBM per device.

```python
import math
import jax
import jax.numpy as jnp
from jax import lax

NPIX = 1024
FCOLS = 8
NB = 4
MARGIN = 8
TAPS = 17
CH = 8
FACETS = 8
FROWS = 1
FS = 128
SR = 512
HALF = 512


def draw_sky_image(key, part):
    full_shape = (CH, FCOLS, FROWS, 2, SR, FS)
    key_space = jax.random.fold_in(key, 12)
    key_fresh = jax.random.fold_in(key, 13)
    key_jitter = jax.random.fold_in(key, 14)
    channel_ramp = jnp.arange(CH, dtype=jnp.float32) / max(CH - 1, 1)
    fresh = jax.random.uniform(key_fresh, full_shape, jnp.float32, 0.0, 2.0)
    jitter = jnp.exp(jax.random.uniform(key_jitter, (CH,), jnp.float32, -0.2, 0.2))
    channel_scale = 0.15 * jnp.exp(channel_ramp * math.log(10.0)) * jitter
    spatial = jnp.exp(jax.random.uniform(key_space, full_shape[1:], jnp.float32, -math.log(3.0), math.log(3.0)))
    values = channel_scale[:, None, None, None, None, None] * spatial[None] * fresh
    return jnp.minimum(values, 8.0).astype(jnp.bfloat16)


def place_ends(result, own_key, smallest, largest):
    dims = result.shape
    spot = [jax.random.randint(jax.random.fold_in(own_key, axis), (), 0, dims[axis]) for axis in range(len(dims))]
    result = result.at[tuple(spot)].set(smallest)
    longest = dims.index(max(dims))
    spot[longest] = (spot[longest] + 1) % dims[longest]
    return result.at[tuple(spot)].set(largest)


def block_scale(stream_key, dims, pieces, low, largest):
    factor_of, own = 1.0, jax.random.fold_in(stream_key, 6)
    for axis_at, shards_of in pieces:
        heights = jnp.exp(jax.random.uniform(jax.random.fold_in(own, axis_at), (shards_of,), jnp.float32, low / len(pieces), largest / len(pieces)))
        factor_of = factor_of * jnp.repeat(heights, dims[axis_at] // shards_of).reshape([-1 if axis == axis_at else 1 for axis in range(len(dims))])
    return factor_of


def centred(stream_key, shape, scale, reach, shards=(), kind=jnp.bfloat16):
    entries = jax.random.normal(stream_key, shape, jnp.float32) * scale
    if len(shards) > 0:
        entries = block_scale(stream_key, shape, shards, -0.22, 0.18) * entries
    return jnp.clip(entries, min=-reach, max=reach).astype(kind)


def setup_inputs(seed: int = 0, part: int = 0) -> dict:
    streams_of = jax.random.split(jax.random.key(seed), 8)
    part_keys = jax.random.split(jax.random.fold_in(streams_of[7], part), 8)
    sky_image = draw_sky_image(jax.random.fold_in(jax.random.fold_in(streams_of[7], part), 71), part)
    dirty_image = centred(part_keys[1], (CH, FCOLS, FROWS, 2, SR, FS), 1.0, 6.0, ((0, 8), (3, 2)))
    uv_weights = place_ends(jax.random.randint(part_keys[2], (CH, NPIX, HALF), 0, 8), jax.random.fold_in(part_keys[2], 1), 0, 7).astype(jnp.int32)
    dual_coeffs = centred(part_keys[3], (NB, CH, FACETS, 2, SR, FS), 0.5, 3.0, ((2, 8), (3, 2)))
    support_mask = place_ends((jax.random.randint(streams_of[4], (FACETS, 2, SR, FS), 0, 4) < 3).astype(jnp.int32), jax.random.fold_in(streams_of[4], 1), 0, 1)
    row_taps = centred(streams_of[5], (NB, TAPS), TAPS ** -0.5, 1.5, (), jnp.float32)
    col_taps = centred(streams_of[6], (NB, TAPS), TAPS ** -0.5, 1.5, (), jnp.float32)
    return dict(sky_image=sky_image, dirty_image=dirty_image, uv_weights=uv_weights, dual_coeffs=dual_coeffs, support_mask=support_mask, row_taps=row_taps, col_taps=col_taps)


primal_step = 0.5
dual_step = 0.5
radius = 6.0
weight_unit = 0.25

def dft_block(out_rows, in_rows):
    product = out_rows[:, None] * in_rows[None, :] % NPIX
    phases = product.astype(jnp.float32) * (2.0 * math.pi / NPIX)
    factor = 1.0 / math.sqrt(NPIX)
    return ((jnp.cos(phases) * factor).astype(jnp.bfloat16), (-jnp.sin(phases) * factor).astype(jnp.bfloat16))

def to_full(blocks, leading):
    count = len(leading)
    shaped = blocks.reshape(leading + (FCOLS, FROWS, 2, SR, FS))
    axes_order = tuple(range(count)) + (count + 1, count + 2, count + 3, count, count + 4)
    return shaped.transpose(axes_order).reshape(leading + (NPIX, NPIX))

def from_full(full, leading, target):
    count = len(leading)
    shaped = full.reshape(leading + (FROWS, 2, SR, FCOLS, FS))
    axes_order = tuple(range(count)) + (count + 3, count, count + 1, count + 2, count + 4)
    return shaped.transpose(axes_order).reshape(target)

def filter_axis(values, tap_values, axis, adjoint):
    as_float = values.astype(jnp.float32)
    padding = [(0, 0)] * as_float.ndim
    padding[axis] = (MARGIN, MARGIN)
    padded = jnp.pad(as_float, padding)
    extent = as_float.shape[axis]
    summed = jnp.zeros_like(as_float)
    for tap_index in range(TAPS):
        offset = 2 * MARGIN - tap_index if adjoint else tap_index
        summed = summed + tap_values[tap_index].astype(jnp.float32) * lax.slice_in_dim(padded, offset, offset + extent, axis=axis)
    return summed

def reference(sky_image, dirty_image, uv_weights, dual_coeffs, support_mask, row_taps, col_taps):
    pixel_index = jnp.arange(NPIX, dtype=jnp.int32)
    freq_index = jnp.arange(HALF, dtype=jnp.int32)
    cx_re, cx_im = dft_block(freq_index, pixel_index)
    cy_re, cy_im = dft_block(pixel_index, pixel_index)

    def channel_gradient(pair):
        picture, counts = pair
        half_re = jnp.dot(picture, cx_re.T, preferred_element_type=jnp.float32).astype(jnp.bfloat16)
        half_im = jnp.dot(picture, cx_im.T, preferred_element_type=jnp.float32).astype(jnp.bfloat16)
        vis_re = jnp.dot(cy_re, half_re, preferred_element_type=jnp.float32) - jnp.dot(cy_im, half_im, preferred_element_type=jnp.float32)
        vis_im = jnp.dot(cy_re, half_im, preferred_element_type=jnp.float32) + jnp.dot(cy_im, half_re, preferred_element_type=jnp.float32)
        weight_scale = weight_unit * counts.astype(jnp.float32)
        res_re = (weight_scale * vis_re).astype(jnp.bfloat16)
        res_im = (weight_scale * vis_im).astype(jnp.bfloat16)
        back_re = (jnp.dot(cy_re.T, res_re, preferred_element_type=jnp.float32) + jnp.dot(cy_im.T, res_im, preferred_element_type=jnp.float32)).astype(jnp.bfloat16)
        back_im = (jnp.dot(cy_re.T, res_im, preferred_element_type=jnp.float32) - jnp.dot(cy_im.T, res_re, preferred_element_type=jnp.float32)).astype(jnp.bfloat16)
        return jnp.dot(back_re, cx_re, preferred_element_type=jnp.float32) + jnp.dot(back_im, cx_im, preferred_element_type=jnp.float32)
    picture = to_full(sky_image, (CH,))
    dirty = to_full(dirty_image, (CH,)).astype(jnp.float32)
    gradient = lax.map(channel_gradient, (picture, uv_weights))
    row_bf = row_taps.astype(jnp.bfloat16)
    col_bf = col_taps.astype(jnp.bfloat16)
    dual_full = to_full(dual_coeffs, (NB, CH))
    adjoint = jnp.zeros((CH, NPIX, NPIX), jnp.float32)
    for basis in range(NB):
        along = filter_axis(dual_full[basis], col_bf[basis], 2, True).astype(jnp.bfloat16)
        adjoint = adjoint + filter_axis(along, row_bf[basis], 1, True)
    adjoint_rounded = lax.optimization_barrier(adjoint.astype(jnp.bfloat16)).astype(jnp.float32)
    updated = jnp.maximum(picture.astype(jnp.float32) - primal_step * (gradient - dirty + adjoint_rounded), 0.0)
    new_full = updated.astype(jnp.bfloat16)
    extrapolated = (2.0 * new_full.astype(jnp.float32) - picture.astype(jnp.float32)).astype(jnp.bfloat16)
    keep_mask = to_full(support_mask, ()).astype(jnp.float32)
    duals = []
    for basis in range(NB):
        along = filter_axis(extrapolated, col_bf[basis], 2, False).astype(jnp.bfloat16)
        coefficients = filter_axis(along, row_bf[basis], 1, False)
        stepped = dual_full[basis].astype(jnp.float32) + dual_step * coefficients
        length = jnp.sqrt(lax.optimization_barrier(jnp.sum(stepped * stepped, axis=0)))
        shrink = radius * keep_mask / jnp.maximum(length, radius)
        duals.append((stepped * shrink[None]).astype(jnp.bfloat16))
    new_dual = from_full(jnp.stack(duals), (NB, CH), (NB, CH, FACETS, 2, SR, FS))
    new_image = from_full(new_full, (CH,), (CH, FCOLS, FROWS, 2, SR, FS))
    return (new_image, new_dual)
```

```python
import functools
import math

import jax
import jax.numpy as jnp
import numpy as np
from jax import lax
from jax.experimental import pallas as pl
from jax.experimental.pallas import tpu as pltpu
from jax.sharding import PartitionSpec as P

LANES = 128
WIDE = 2 * LANES
BAND_ROWS = 224
primal_step = 0.5
dual_step = 0.5
radius = 6.0
weight_unit = 0.25


def whole_block(shape):
    zeros = (0,) * len(shape)
    return pl.BlockSpec(tuple(shape), lambda *_: zeros)


def in_scalar_memory():
    return pl.BlockSpec(memory_space=pltpu.SMEM)


def exact_dot(left, right):
    return jnp.dot(left, right, preferred_element_type=jnp.float32)


def each(count, body):
    if count <= 8:
        for index in range(count):
            body(index)
    else:

        def step(index, carry):
            body(index)
            return carry

        lax.fori_loop(0, count, step, 0)


def hint(value, multiple):
    return value if isinstance(value, int) else pl.multiple_of(value, multiple)


def band_seed(taps, basis, positions):
    lane = lax.broadcasted_iota(jnp.int32, (8, WIDE), 1)
    row = lax.broadcasted_iota(jnp.int32, (8, WIDE), 0)
    offset = lane - row & WIDE - 1
    seed = jnp.zeros((8, WIDE), jnp.float32)
    for tap, position in enumerate(positions):
        seed = jnp.where(offset == position % WIDE, taps[basis, tap], seed)
    return seed


def fill_band(target, first_row, rows, seed):
    for start in range(0, rows, 16):
        upper = seed if start == 0 else pltpu.roll(seed, start, axis=1)
        lower = pltpu.roll(seed, start + 8, axis=1)
        target[first_row + start : first_row + start + 16, :] = jnp.concatenate(
            [upper, lower], axis=0
        ).astype(jnp.bfloat16)


def fill_col_bands(target, taps, bases, margin):
    for basis in range(bases):
        count = taps.shape[1]
        seed = band_seed(taps, basis, [tap - margin for tap in range(count)])
        fill_band(target, basis * LANES, LANES, seed)


def pack_height(rows):
    return -(-rows // (8 * 16)) * 16


def payload_rows(rows):
    return rows + pack_height(rows)


def row_groups(rows):
    height = pack_height(rows)
    return [(g, g * height, min(height, rows - g * height)) for g in range(-(-rows // height))]


def padded_rows(strip_rows):
    chunks = -(-strip_rows // BAND_ROWS)
    return (chunks - 1) * BAND_ROWS + WIDE


def adjoint_kernel(
    order, row_taps, col_taps, dual, above, below, *rest, bases, margin, strip_rows, single
):
    outs, (row_band, edge_band, col_band, tall, mixed, wide) = rest[:-6], rest[-6:]
    step = pl.program_id(0)
    taps = row_taps.shape[1]
    halo = 2 * margin
    rows = strip_rows + halo

    @pl.when(step == 0)
    def _():
        lane = lax.broadcasted_iota(jnp.int32, (16, LANES), 1)
        row = lax.broadcasted_iota(jnp.int32, (16, LANES), 0)
        for basis in range(bases):
            seed = band_seed(row_taps, basis, [halo + margin - tap for tap in range(taps)])
            fill_band(row_band.at[basis], 0, BAND_ROWS, seed)
            source = jnp.where(
                row < margin,
                jnp.where(lane < 2 * halo, halo + row - lane, -1),
                jnp.where(lane >= 2 * halo, row + 3 * halo - lane, -1),
            )
            edge = jnp.zeros((16, LANES), jnp.float32)
            for tap in range(taps):
                edge = jnp.where(source == tap, row_taps[basis, tap], edge)
            edge_band[basis] = edge.astype(jnp.bfloat16)
        fill_col_bands(col_band, col_taps, bases, margin)
        tall[...] = jnp.zeros(tall.shape, tall.dtype)

    for basis in range(bases):
        tall[basis, :halo] = above[basis, 0]
        tall[basis, halo : halo + strip_rows] = dual[basis, 0]
        tall[basis, halo + strip_rows : 2 * halo + strip_rows] = below[basis, 0]
    for basis in range(bases):
        lanes = slice(basis * LANES, (basis + 1) * LANES)
        for first in range(0, strip_rows, BAND_ROWS):
            count = min(BAND_ROWS, strip_rows - first)
            mixed[first : first + count, lanes] = exact_dot(
                row_band[basis, :count], tall[basis, first : first + WIDE]
            ).astype(jnp.bfloat16)
        ends = jnp.concatenate(
            [
                tall[basis, : 2 * halo],
                tall[basis, strip_rows : strip_rows + 2 * halo],
                jnp.zeros((LANES - 4 * halo, LANES), jnp.bfloat16),
            ],
            axis=0,
        )
        mixed[strip_rows:rows, lanes] = exact_dot(edge_band[basis], ends).astype(jnp.bfloat16)
    wide[...] = exact_dot(mixed[...], col_band[...])
    height = pack_height(rows)

    def write(out):
        packed = jnp.zeros((height, LANES), jnp.float32)
        for group, first, count in row_groups(rows):
            out[first : first + count, :] = wide[first : first + count, :LANES].astype(jnp.bfloat16)
            side = wide[first : first + count, LANES:]
            side = pltpu.roll(side, margin + 2 * margin * group, axis=1)
            if count < height:
                side = jnp.concatenate(
                    [side, jnp.zeros((height - count, LANES), jnp.float32)], axis=0
                )
            packed = packed + side
        out[rows : rows + height, :] = packed.astype(jnp.bfloat16)

    if single:
        write(outs[0].at[0])
    else:
        for place, out in enumerate(outs):

            @pl.when(step == place)
            def _(out=out):
                write(out)


def adjoint_payloads(dual, above, below, row_taps, col_taps, order, single):
    bases, _, strip_rows, _ = dual.shape
    taps = row_taps.shape[1]
    margin = taps // 2
    count = order.shape[0]
    rows = strip_rows + 2 * margin
    tall_rows = payload_rows(rows)
    if single:
        out_shape = [jax.ShapeDtypeStruct((count, tall_rows, LANES), jnp.bfloat16)]
        out_specs = [pl.BlockSpec((1, tall_rows, LANES), lambda j, *_: (j, 0, 0))]
    else:
        out_shape = [jax.ShapeDtypeStruct((tall_rows, LANES), jnp.bfloat16)] * count
        out_specs = [whole_block((tall_rows, LANES))] * count

    def picked(height):
        return pl.BlockSpec((bases, 1, height, LANES), lambda j, o: (0, o[j], 0, 0))

    return pl.pallas_call(
        functools.partial(
            adjoint_kernel, bases=bases, margin=margin, strip_rows=strip_rows, single=single
        ),
        out_shape=out_shape,
        grid_spec=pltpu.PrefetchScalarGridSpec(
            num_scalar_prefetch=1,
            grid=(count,),
            in_specs=[
                in_scalar_memory(),
                in_scalar_memory(),
                picked(strip_rows),
                picked(2 * margin),
                picked(2 * margin),
            ],
            out_specs=out_specs,
            scratch_shapes=[
                pltpu.VMEM((bases, BAND_ROWS, WIDE), jnp.bfloat16),
                pltpu.VMEM((bases, 16, LANES), jnp.bfloat16),
                pltpu.VMEM((bases * LANES, WIDE), jnp.bfloat16),
                pltpu.VMEM((bases, max(padded_rows(strip_rows), strip_rows + 4 * margin), LANES), jnp.bfloat16),
                pltpu.VMEM((rows, bases * LANES), jnp.bfloat16),
                pltpu.VMEM((rows, WIDE), jnp.float32),
            ],
        ),
        name="adjoint",
    )(order, row_taps, col_taps, dual, above, below)


def phase_tables(pixels):
    step = 2.0 * math.pi / pixels
    coarse = 32
    fine = pixels // coarse
    where = np.arange(pixels)
    big = (np.arange(fine)[:, None] * coarse * where[None, :]) % pixels * step
    small = (np.arange(coarse)[:, None] * where[None, :]) % pixels * step
    scale = 1.0 / math.sqrt(pixels)
    return tuple(
        np.asarray(v, np.float32)
        for v in (np.cos(big), -np.sin(big), np.cos(small) * scale, -np.sin(small) * scale)
    )


def fill_phases(big_re, big_im, small_re, small_im, groups, store):
    def step(group, carry):
        far_re = big_re[pl.ds(group, 1), :]
        far_im = big_im[pl.ds(group, 1), :]
        near_re = small_re[...]
        near_im = small_im[...]
        store(
            group,
            (far_re * near_re - far_im * near_im).astype(jnp.bfloat16),
            (far_re * near_im + far_im * near_re).astype(jnp.bfloat16),
        )
        return carry

    lax.fori_loop(0, groups, step, 0)


def spectrum_kernel(
    own, other, own_counts, other_counts, big_re, big_im, small_re, small_im, keep, send,
    cosine, sine, picture, upper, lower, back, *, margin
):
    split = lax.axis_index("split")
    cols, facet_rows, strip_rows, _ = own.shape
    pixels = picture.shape[0]
    half = pixels // 2
    part = upper.shape[1] // 2
    coarse = small_re.shape[0]

    def store(group, re, im):
        at = pl.ds(pl.multiple_of(group * coarse, coarse), coarse)
        cosine[at, :] = re
        sine[at, :] = im

    fill_phases(big_re, big_im, small_re, small_im, pixels // coarse, store)

    def strip_at(facet_row, which):
        return pl.multiple_of((2 * facet_row + which) * strip_rows, strip_rows)

    for facet_row in range(facet_rows):
        for col in range(cols):
            lanes = slice(col * LANES, (col + 1) * LANES)
            picture[pl.ds(strip_at(facet_row, split), strip_rows), lanes] = own[col, facet_row]
            picture[pl.ds(strip_at(facet_row, 1 - split), strip_rows), lanes] = other[col, facet_row]
    kept = pl.ds(pl.multiple_of(split * part, part), part)

    def first(block, carry):
        at = pl.ds(pl.multiple_of(block * half, half), half)
        re = exact_dot(picture[at, :], cosine[:, kept]).astype(jnp.bfloat16)
        im = exact_dot(picture[at, :], sine[:, kept]).astype(jnp.bfloat16)
        upper[at, :part] = re
        upper[at, part:] = im
        lower[at, :part] = -im
        lower[at, part:] = re
        return carry

    lax.fori_loop(0, 2, first, 0)

    def second(rows, counts, at_rows):
        vis = exact_dot(cosine[at_rows, :], upper[...]) + exact_dot(sine[at_rows, :], lower[...])
        scale = weight_unit * counts[:, kept].astype(jnp.float32)
        back[at_rows, :part] = (vis[:, :part] * scale).astype(jnp.bfloat16)
        back[at_rows, part:] = (vis[:, part:] * scale).astype(jnp.bfloat16)

    second(half, own_counts, pl.ds(pl.multiple_of(split * half, half), half))
    second(half, other_counts, pl.ds(pl.multiple_of((1 - split) * half, half), half))
    upper[...] = back[...]
    lower[:, :part] = back[:, part:]
    lower[:, part:] = -back[:, :part]

    def third(block, carry):
        at = pl.ds(pl.multiple_of(block * half, half), half)
        value = exact_dot(cosine[at, :], upper[...]) + exact_dot(sine[at, :], lower[...])
        back[at, :] = value.astype(jnp.bfloat16)
        return carry

    lax.fori_loop(0, 2, third, 0)
    rows = strip_rows + 2 * margin
    for facet_row in range(facet_rows):
        for target, which in ((keep, split), (send, 1 - split)):
            at = strip_at(facet_row, which)
            base = facet_row * rows
            target[base : base + strip_rows, :] = back[pl.ds(at, strip_rows), :]
            before = pl.multiple_of(lax.rem(at + pixels - 16, pixels), 16)
            after = pl.multiple_of(lax.rem(at + strip_rows, pixels), 16)
            ends = jnp.concatenate(
                [
                    back[pl.ds(before, 16), :].astype(jnp.float32)[16 - margin :],
                    back[pl.ds(after, 16), :].astype(jnp.float32)[:margin],
                ],
                axis=0,
            )
            target[base + strip_rows : base + rows, :] = ends.astype(jnp.bfloat16)


def spectrum(own, other, own_counts, other_counts, tables, margin):
    cols, facet_rows, strip_rows, lanes = own.shape
    pixels = cols * lanes
    part = own_counts.shape[1] // 2
    rows = facet_rows * (strip_rows + 2 * margin)
    shape = jax.ShapeDtypeStruct((rows, 2 * part), jnp.bfloat16)
    return pl.pallas_call(
        functools.partial(spectrum_kernel, margin=margin),
        out_shape=[shape, shape],
        scratch_shapes=[
            pltpu.VMEM((pixels, pixels), jnp.bfloat16),
            pltpu.VMEM((pixels, pixels), jnp.bfloat16),
            pltpu.VMEM((pixels, pixels), jnp.bfloat16),
            pltpu.VMEM((pixels, 2 * part), jnp.bfloat16),
            pltpu.VMEM((pixels, 2 * part), jnp.bfloat16),
            pltpu.VMEM((pixels, 2 * part), jnp.bfloat16),
        ],
        name="spectrum",
    )(own, other, own_counts, other_counts, *tables)


def edge_rows(other, facet_row, facet_rows, split, margin):
    strip_rows = other.shape[1]
    above = jnp.maximum(facet_row - 1 + split, 0)
    below = jnp.minimum(facet_row + split, facet_rows - 1)
    top = other[above, strip_rows - 16 :, :].astype(jnp.float32)[16 - margin :]
    low = other[below, :16, :].astype(jnp.float32)[:margin]
    return jnp.concatenate([top, low], axis=0)


def gradient_kernel(
    kept, got, own, other, own_dirty, other_dirty, big_re, big_im, small_re, small_im,
    stepped, pixels_out, table, joined, *, margin
):
    split = lax.axis_index("split")
    cols, facet_rows, strip_rows, _ = own.shape
    part = kept.shape[1] // 2
    coarse = small_re.shape[0]
    groups = 2 * part // coarse
    rows = strip_rows + 2 * margin

    def store(group, re, im):
        side = group // (part // coarse)
        within = lax.rem(group, part // coarse)
        place = jnp.where(side == split, 0, 2 * part) + within * coarse
        table[pl.ds(pl.multiple_of(place, coarse), coarse), :] = re
        table[pl.ds(pl.multiple_of(place + part, coarse), coarse), :] = im

    fill_phases(big_re, big_im, small_re, small_im, groups, store)
    joined[:, : 2 * part] = kept[...]
    joined[:, 2 * part :] = got[...]
    for col in range(0, cols, 2):
        value = exact_dot(joined[...], table[:, col * LANES : (col + 2) * LANES])
        for side in range(2):
            here = col + side
            for facet_row in range(facet_rows):
                base = facet_row * rows
                grad = value[base : base + rows, side * LANES : (side + 1) * LANES]
                image = own[here, facet_row]
                dirty = own_dirty[here, facet_row].astype(jnp.float32)
                stepped[here, facet_row, :strip_rows] = image.astype(
                    jnp.float32
                ) - primal_step * (grad[:strip_rows] - dirty)
                pixels_out[here, facet_row, :strip_rows] = image
                image = edge_rows(other.at[here], facet_row, facet_rows, split, margin)
                dirty = edge_rows(other_dirty.at[here], facet_row, facet_rows, split, margin)
                stepped[here, facet_row, strip_rows:] = image - primal_step * (
                    grad[strip_rows:] - dirty
                )
                pixels_out[here, facet_row, strip_rows:] = image.astype(jnp.bfloat16)


def gradient_step(kept, got, own, other, own_dirty, other_dirty, tables, margin):
    cols, facet_rows, strip_rows, lanes = own.shape
    pixels = cols * lanes
    rows = strip_rows + 2 * margin
    return pl.pallas_call(
        functools.partial(gradient_kernel, margin=margin),
        out_shape=[
            jax.ShapeDtypeStruct((cols, facet_rows, rows, lanes), jnp.float32),
            jax.ShapeDtypeStruct((cols, facet_rows, rows, lanes), jnp.bfloat16),
        ],
        scratch_shapes=[
            pltpu.VMEM((2 * kept.shape[1], pixels), jnp.bfloat16),
            pltpu.VMEM((kept.shape[0], 2 * kept.shape[1]), jnp.bfloat16),
        ],
        name="gradient",
    )(kept, got, own, other, own_dirty, other_dirty, *tables)


def unpacked(packed, group, count, margin):
    return pltpu.roll(
        packed[:count], LANES - (margin + 2 * margin * group) % LANES, axis=1
    )


def update_kernel(stepped, image, *rest, margin, facets, single):
    arrivals = 1 if single else facets
    blocks = rest[:arrivals]
    new_image = rest[arrivals]
    outs = rest[arrivals + 1 : 2 * arrivals + 1]
    adjoint, extrapolated = rest[2 * arrivals + 1 :]
    me = lax.axis_index("chan")
    split = lax.axis_index("split")
    cols, facet_rows, rows, _ = stepped.shape
    strip_rows = rows - 2 * margin
    height = pack_height(rows)
    lane = lax.broadcasted_iota(jnp.int32, (1, LANES), 1)
    if single:
        adjoint = blocks[0]
    else:
        for place, block in enumerate(blocks):
            adjoint[me ^ place] = block[...]

    def sides(take, group, count, left, has_left, right, has_right):
        from_left = take(left, group, count)
        from_right = take(right, group, count)
        return (
            jnp.where(lane < jnp.where(has_left, margin, 0), from_left, 0.0),
            jnp.where(lane >= jnp.where(has_right, LANES - margin, LANES), from_right, 0.0),
        )

    def packed_of(facet, group, count):
        tile = adjoint[facet, rows : rows + height, :].astype(jnp.float32)
        return unpacked(tile, group, count, margin)

    def update(facet):
        col = facet // facet_rows
        facet_row = facet % facet_rows
        left, has_left = jnp.maximum(facet - facet_rows, 0), facet >= facet_rows
        right, has_right = jnp.minimum(facet + facet_rows, facets - 1), facet < facets - facet_rows
        for group, first, count in row_groups(rows):
            add_left, add_right = sides(packed_of, group, count, left, has_left, right, has_right)
            at = slice(first, first + count)
            total = adjoint[facet, at, :].astype(jnp.float32) + add_left + add_right
            value = stepped[col, facet_row, at, :] - primal_step * total
            value = jnp.maximum(value, 0.0).astype(jnp.bfloat16).astype(jnp.float32)
            ahead = 2.0 * value - image[col, facet_row, at, :].astype(jnp.float32)
            if first + count > strip_rows:
                row = first + lax.broadcasted_iota(jnp.int32, (count, LANES), 0)
                top_there = (facet_row > 0) | (split > 0)
                low_there = (facet_row < facet_rows - 1) | (split < 1)
                middle = strip_rows + margin
                from_top = jnp.where(top_there, middle, strip_rows)
                to_low = jnp.where(low_there, rows, middle)
                ahead = jnp.where((row >= from_top) & (row < middle), 0.0, ahead)
                ahead = jnp.where(row >= to_low, 0.0, ahead)
            extrapolated[facet, at, :] = ahead.astype(jnp.bfloat16)
            main = min(first + count, strip_rows) - first
            if main > 0:
                new_image[col, facet_row, first : first + main, :] = value[:main].astype(jnp.bfloat16)

    each(facets, update)

    def whole_of(facet, group, count):
        first = group * height
        return extrapolated[facet, first : first + count, :].astype(jnp.float32)

    def write(out, facet):
        left, has_left = jnp.maximum(facet - facet_rows, 0), facet >= facet_rows
        right, has_right = jnp.minimum(facet + facet_rows, facets - 1), facet < facets - facet_rows
        packed = jnp.zeros((height, LANES), jnp.float32)
        for group, first, count in row_groups(rows):
            after, before = sides(whole_of, group, count, right, has_right, left, has_left)
            side = pltpu.roll(after + before, margin + 2 * margin * group, axis=1)
            if count < height:
                side = jnp.concatenate(
                    [side, jnp.zeros((height - count, LANES), jnp.float32)], axis=0
                )
            packed = packed + side
        out[:rows, :] = extrapolated[facet]
        out[rows:, :] = packed.astype(jnp.bfloat16)

    if single:
        each(facets, lambda facet: write(outs[0].at[facet], facet))
    else:
        for place, out in enumerate(outs):
            write(out, me ^ place)


def update_step(stepped, image, blocks, margin, single):
    cols, facet_rows, rows, lanes = stepped.shape
    facets = cols * facet_rows
    tall_rows = payload_rows(rows)
    arrivals = (
        [jax.ShapeDtypeStruct((facets, tall_rows, lanes), jnp.bfloat16)]
        if single
        else [jax.ShapeDtypeStruct((tall_rows, lanes), jnp.bfloat16)] * facets
    )
    held = (8, 16, lanes) if single else (facets, tall_rows, lanes)
    results = pl.pallas_call(
        functools.partial(update_kernel, margin=margin, facets=facets, single=single),
        out_shape=[
            jax.ShapeDtypeStruct((cols, facet_rows, rows - 2 * margin, lanes), jnp.bfloat16)
        ]
        + arrivals,
        scratch_shapes=[
            pltpu.VMEM(held, jnp.bfloat16),
            pltpu.VMEM((facets, rows, lanes), jnp.bfloat16),
        ],
        name="update",
    )(stepped, image, *blocks)
    return results[0], results[1:]


def shrink_kernel(row_taps, col_taps, mask, dual, *rest, margin, channels, single):
    arrivals = 1 if single else channels
    blocks = rest[:arrivals]
    out = rest[arrivals]
    row_band, col_band, wide, tall = rest[arrivals + 1 :]
    me = lax.axis_index("chan")
    basis = pl.program_id(0)
    bases = pl.num_programs(0)
    taps = row_taps.shape[1]
    halo = 2 * margin
    strip_rows = dual.shape[2]
    rows = strip_rows + halo
    height = pack_height(rows)

    @pl.when(basis == 0)
    def _():
        for each_basis in range(row_taps.shape[0]):
            seed = band_seed(row_taps, each_basis, [margin + tap for tap in range(taps)])
            fill_band(row_band.at[each_basis], 0, BAND_ROWS, seed)
            seed = band_seed(col_taps, each_basis, [tap - margin for tap in range(taps)])
            fill_band(col_band.at[each_basis], 0, LANES, seed)
        tall[...] = jnp.zeros(tall.shape, tall.dtype)

        def unpack(channel, block):
            wide[channel, :, :LANES] = block[:rows, :]
            packed = block[rows : rows + height, :].astype(jnp.float32)
            for group, first, count in row_groups(rows):
                side = unpacked(packed, group, count, margin)
                wide[channel, first : first + count, LANES:] = side.astype(jnp.bfloat16)

        if single:
            each(channels, lambda channel: unpack(channel, blocks[0].at[channel]))
        else:
            for place, block in enumerate(blocks):
                unpack(me ^ place, block)

    def columns(channel):
        lanes = pl.ds(hint(channel * LANES, LANES), LANES)
        value = lax.dot_general(
            wide[channel], col_band[basis], (((1,), (1,)), ((), ())),
            preferred_element_type=jnp.float32,
        )
        blank = jnp.zeros((halo - margin, LANES), jnp.float32)
        tall[halo : halo + strip_rows, lanes] = value[:strip_rows].astype(jnp.bfloat16)
        tall[:halo, lanes] = jnp.concatenate(
            [blank, value[strip_rows : strip_rows + margin]], axis=0
        ).astype(jnp.bfloat16)
        tall[halo + strip_rows : 2 * halo + strip_rows, lanes] = jnp.concatenate(
            [value[strip_rows + margin :], blank], axis=0
        ).astype(jnp.bfloat16)

    each(channels, columns)
    piece = min(channels, 8)
    for first in range(0, strip_rows, BAND_ROWS):
        count = min(BAND_ROWS, strip_rows - first)
        stepped = []
        total = jnp.zeros((count, LANES), jnp.float32)
        for channel in range(0, channels, piece):
            value = exact_dot(
                row_band[basis, :count],
                tall[first : first + WIDE, channel * LANES : (channel + piece) * LANES],
            )
            for side in range(piece):
                coefficient = value[:, side * LANES : (side + 1) * LANES]
                moved = (
                    dual[0, channel + side, first : first + count].astype(jnp.float32)
                    + dual_step * coefficient
                )
                stepped.append(moved)
                total = total + moved * moved
        kept = mask[first : first + count].astype(jnp.float32)
        shrink = radius * kept / jnp.maximum(jnp.sqrt(total), radius)
        for channel in range(channels):
            out[0, channel, first : first + count] = (stepped[channel] * shrink).astype(jnp.bfloat16)


def shrink_step(row_taps, col_taps, mask, dual, blocks, single):
    bases, channels, strip_rows, lanes = dual.shape
    margin = row_taps.shape[1] // 2
    rows = strip_rows + 2 * margin
    return pl.pallas_call(
        functools.partial(shrink_kernel, margin=margin, channels=channels, single=single),
        out_shape=jax.ShapeDtypeStruct(dual.shape, jnp.bfloat16),
        grid=(bases,),
        in_specs=[
            in_scalar_memory(),
            in_scalar_memory(),
            whole_block(mask.shape),
            pl.BlockSpec((1, channels, strip_rows, lanes), lambda n: (n, 0, 0, 0)),
        ]
        + [whole_block(block.shape) for block in blocks],
        out_specs=pl.BlockSpec((1, channels, strip_rows, lanes), lambda n: (n, 0, 0, 0)),
        scratch_shapes=[
            pltpu.VMEM((bases, BAND_ROWS, WIDE), jnp.bfloat16),
            pltpu.VMEM((bases, LANES, WIDE), jnp.bfloat16),
            pltpu.VMEM((channels, rows, WIDE), jnp.bfloat16),
            pltpu.VMEM((max(padded_rows(strip_rows), strip_rows + 4 * margin), channels * lanes), jnp.bfloat16),
        ],
        name="shrink",
    )(row_taps, col_taps, mask, dual, *blocks)


def swapped(value):
    return lax.ppermute(value, "split", [(0, 1), (1, 0)])


def along_chain(value, by, facet_rows):
    count = lax.axis_size("chan") * 2
    chain = 2 * facet_rows
    pairs = [
        (i, i + by) for i in range(count) if 0 <= i + by < count and i // chain == (i + by) // chain
    ]
    return lax.ppermute(value, ("chan", "split"), pairs)


def crossed(blocks, single):
    count = lax.axis_size("chan")
    if single:
        return [lax.all_to_all(blocks[0], "chan", split_axis=0, concat_axis=0, tiled=True)]
    result = list(blocks)
    for place in reversed(range(1, count)):
        result[place] = lax.ppermute(
            blocks[place], "chan", [(i, i ^ place) for i in range(count)]
        )
    return result


def per_device(sky_image, dirty_image, uv_weights, dual_coeffs, support_mask, row_taps, col_taps):
    facet_cols, facet_rows, strip_rows, lanes = (sky_image.shape[i] for i in (1, 2, 4, 5))
    bases, channels = dual_coeffs.shape[:2]
    margin = row_taps.shape[1] // 2
    count = lax.axis_size("chan")
    single = count > 8 or count & count - 1 != 0
    image = sky_image.reshape(facet_cols, facet_rows, strip_rows, lanes)
    dirty = dirty_image.reshape(image.shape)
    counts = uv_weights.reshape(uv_weights.shape[1:])
    dual = dual_coeffs.reshape(bases, channels, strip_rows, lanes)
    mask = support_mask.reshape(strip_rows, lanes)
    tables = phase_tables(facet_cols * lanes)

    halo = 2 * margin
    above = along_chain(dual[:, :, strip_rows - halo :], 1, facet_rows)
    below = along_chain(dual[:, :, :halo], -1, facet_rows)
    other_image = swapped(image)
    other_counts = swapped(counts)
    other_dirty = swapped(dirty)
    me = lax.axis_index("chan")
    order = jnp.arange(count, dtype=jnp.int32)
    if not single:
        order = order ^ me
    blocks = adjoint_payloads(dual, above, below, row_taps, col_taps, order, single)
    arrived = crossed(blocks, single)
    kept, sent = spectrum(image, other_image, counts, other_counts, tables, margin)
    got = swapped(sent)
    stepped, wide_image = gradient_step(
        kept, got, image, other_image, dirty, other_dirty, tables, margin
    )
    new_image, blocks = update_step(stepped, wide_image, arrived, margin, single)
    arrived = crossed(blocks, single)
    new_dual = shrink_step(row_taps, col_taps, mask, dual, arrived, single)
    return (new_image.reshape(sky_image.shape), new_dual.reshape(dual_coeffs.shape))


def solution(mesh):
    placed = (
        P(("cube", "chan"), None, None, "split", None, None),
        P(("cube", "chan"), None, None, "split", None, None),
        P(("cube", "chan"), "split", None),
        P(None, "cube", "chan", "split", None, None),
        P("chan", "split", None, None),
        P(),
        P(),
    )
    return jax.shard_map(
        per_device,
        mesh=mesh,
        in_specs=placed,
        out_specs=(
            P(("cube", "chan"), None, None, "split", None, None),
            P(None, "cube", "chan", "split", None, None),
        ),
        check_vma=False,
    )
```

```python
import functools
import math

import jax
import jax.numpy as jnp
import numpy as np
from jax import lax
from jax.experimental import pallas as pl
from jax.experimental.pallas import tpu as pltpu
from jax.sharding import PartitionSpec as P


LANES = 128
WIDE = 2 * LANES
BAND_ROWS = 224
primal_step = 0.5
dual_step = 0.5
radius = 6.0
weight_unit = 0.25


def whole_block(shape):
    zeros = (0,) * len(shape)
    return pl.BlockSpec(tuple(shape), lambda *_: zeros)


def in_scalar_memory():
    return pl.BlockSpec(memory_space=pltpu.SMEM)


def exact_dot(left, right):
    return jnp.dot(left, right, preferred_element_type=jnp.float32)


def each(count, body):
    if count <= 8:
        for index in range(count):
            body(index)
    else:

        def step(index, carry):
            body(index)
            return carry

        lax.fori_loop(0, count, step, 0)


def hint(value, multiple):
    return value if isinstance(value, int) else pl.multiple_of(value, multiple)


def band_seed(taps, basis, positions):
    lane = lax.broadcasted_iota(jnp.int32, (8, WIDE), 1)
    row = lax.broadcasted_iota(jnp.int32, (8, WIDE), 0)
    offset = lane - row & WIDE - 1
    seed = jnp.zeros((8, WIDE), jnp.float32)
    for tap, position in enumerate(positions):
        seed = jnp.where(offset == position % WIDE, taps[basis, tap], seed)
    return seed


def fill_band(target, first_row, rows, seed):
    for start in range(0, rows, 16):
        upper = seed if start == 0 else pltpu.roll(seed, start, axis=1)
        lower = pltpu.roll(seed, start + 8, axis=1)
        target[first_row + start : first_row + start + 16, :] = jnp.concatenate(
            [upper, lower], axis=0
        ).astype(jnp.bfloat16)


def fill_col_bands(target, taps, bases, margin):
    for basis in range(bases):
        count = taps.shape[1]
        seed = band_seed(taps, basis, [tap - margin for tap in range(count)])
        fill_band(target, basis * LANES, LANES, seed)


def pack_height(rows):
    return -(-rows // (8 * 16)) * 16


def payload_rows(rows):
    return rows + pack_height(rows)


def row_groups(rows):
    height = pack_height(rows)
    return [(g, g * height, min(height, rows - g * height)) for g in range(-(-rows // height))]


def padded_rows(strip_rows):
    chunks = -(-strip_rows // BAND_ROWS)
    return (chunks - 1) * BAND_ROWS + WIDE


def edge_band_of(taps, basis, margin):
    halo = 2 * margin
    lane = lax.broadcasted_iota(jnp.int32, (halo, LANES), 1)
    row = lax.broadcasted_iota(jnp.int32, (halo, LANES), 0)
    source = jnp.where(
        row < margin,
        jnp.where(lane < 2 * halo, halo + row - lane, -1),
        jnp.where(lane >= 2 * halo, row + 3 * halo - lane, -1),
    )
    edge = jnp.zeros((halo, LANES), jnp.float32)
    for tap in range(taps.shape[1]):
        edge = jnp.where(source == tap, taps[basis, tap], edge)
    return edge


def products(far_re, far_im, near_re, near_im):
    return (
        (far_re * near_re - far_im * near_im).astype(jnp.bfloat16),
        (far_re * near_im + far_im * near_re).astype(jnp.bfloat16),
    )


def fill_transforms(seeds, cosine, sine, freq):
    big_re, big_im, small_re, small_im, even_re, even_im = seeds
    split = lax.axis_index("split")
    coarse = small_re.shape[0]
    half = cosine.shape[0]
    part = half // 2

    def even_rows(group, carry):
        at = pl.ds(pl.multiple_of(group * coarse, coarse), coarse)
        one = pl.ds(group, 1)
        cosine[at, :], sine[at, :] = products(
            even_re[one, :], even_im[one, :], even_re[half // coarse :, :], even_im[half // coarse :, :]
        )
        return carry

    lax.fori_loop(0, half // coarse, even_rows, 0)

    def freq_rows(group, carry):
        at = pl.ds(pl.multiple_of(group * coarse, coarse), coarse)
        one = pl.ds(group, 1)
        for place in range(2):
            side = jnp.where(split == place, 0, 1) * part
            lanes = pl.ds(pl.multiple_of(side, part), part)
            re, im = products(
                big_re[one, lanes], big_im[one, lanes], small_re[:, lanes], small_im[:, lanes]
            )
            freq[at, 2 * place * part : (2 * place + 1) * part] = re
            freq[at, (2 * place + 1) * part : (2 * place + 2) * part] = im
        return carry

    lax.fori_loop(0, 2 * half // coarse, freq_rows, 0)


def fill_adjoint_bands(row_taps, col_taps, row_band, edge_band, col_band, margin):
    bases, taps = row_taps.shape
    for basis in range(bases):
        seed = band_seed(row_taps, basis, [3 * margin - tap for tap in range(taps)])
        fill_band(row_band.at[basis], 0, BAND_ROWS, seed)
        edge_band[basis] = edge_band_of(row_taps, basis, margin).astype(jnp.bfloat16)
    fill_col_bands(col_band, col_taps, bases, margin)


def is_at_ends(facet_rows):
    split = lax.axis_index("split")
    facet_row = lax.rem(lax.axis_index("chan"), facet_rows)
    return (facet_row == 0) & (split == 0), (facet_row == facet_rows - 1) & (split == 1)


def adjoint_of(tall, bands, mixed, wide, strip_rows, margin):
    row_band, edge_band, col_band = bands
    bases = tall.shape[0]
    width = tall.shape[2] // LANES
    halo = 2 * margin
    for basis in range(bases):
        into = slice(basis * LANES, (basis + 1) * LANES)

        def put(first, count, value):
            for side in range(width):
                mixed[side, first : first + count, into] = value[
                    :, side * LANES : (side + 1) * LANES
                ].astype(jnp.bfloat16)

        for first in range(0, strip_rows, BAND_ROWS):
            count = min(BAND_ROWS, strip_rows - first)
            put(first, count, exact_dot(row_band[basis, :count], tall[basis, first : first + WIDE]))
        ends = jnp.concatenate(
            [
                tall[basis, : 2 * halo],
                tall[basis, strip_rows : strip_rows + 2 * halo],
                jnp.zeros((LANES - 4 * halo, width * LANES), jnp.bfloat16),
            ],
            axis=0,
        )
        put(strip_rows, halo, exact_dot(edge_band[basis], ends))
    for side in range(width):
        wide[side] = exact_dot(mixed[side], col_band[...])


def write_payload(out, wide, margin):
    rows = wide.shape[0]
    height = pack_height(rows)
    packed = jnp.zeros((height, LANES), jnp.float32)
    for group, first, count in row_groups(rows):
        out[first : first + count, :] = wide[first : first + count, :LANES].astype(jnp.bfloat16)
        piece = wide[first : first + count, LANES:]
        piece = pltpu.roll(piece, margin + 2 * margin * group, axis=1)
        if count < height:
            piece = jnp.concatenate(
                [piece, jnp.zeros((height - count, LANES), jnp.float32)], axis=0
            )
        packed = packed + piece
    out[rows : rows + height, :] = packed.astype(jnp.bfloat16)


def tall_height(strip_rows, margin):
    return max(padded_rows(strip_rows), strip_rows + 4 * margin)


def band_scratch(bases, margin):
    return [
        pltpu.VMEM((bases, BAND_ROWS, WIDE), jnp.bfloat16),
        pltpu.VMEM((bases, 2 * margin, LANES), jnp.bfloat16),
        pltpu.VMEM((bases * LANES, WIDE), jnp.bfloat16),
    ]


def all_adjoint_kernel(row_taps, col_taps, dual, above, below, out, *scratch, margin, facet_rows):
    bands, (tall, mixed, wide) = scratch[:3], scratch[3:]
    bases, width, strip_rows, _ = dual.shape
    halo = 2 * margin

    @pl.when(pl.program_id(0) == 0)
    def _():
        fill_adjoint_bands(row_taps, col_taps, *bands, margin)
        tall[...] = jnp.zeros(tall.shape, tall.dtype)

    is_top, is_low = is_at_ends(facet_rows)
    for basis in range(bases):
        for side in range(width):
            lanes = slice(side * LANES, (side + 1) * LANES)
            top = above[basis, side]
            low = below[basis, side]
            tall[basis, :halo, lanes] = jnp.where(is_top, jnp.zeros_like(top), top)
            tall[basis, halo : halo + strip_rows, lanes] = dual[basis, side]
            tall[basis, halo + strip_rows : 2 * halo + strip_rows, lanes] = jnp.where(
                is_low, jnp.zeros_like(low), low
            )
    adjoint_of(tall, bands, mixed, wide, strip_rows, margin)
    for side in range(width):
        write_payload(out.at[side], wide.at[side], margin)


def all_adjoint(dual, above, below, row_taps, col_taps, facet_rows):
    bases, count, strip_rows, _ = dual.shape
    margin = row_taps.shape[1] // 2
    width = 2 if count % 2 == 0 else 1
    rows = strip_rows + 2 * margin

    def picked(height):
        return pl.BlockSpec((bases, width, height, LANES), lambda j: (0, j, 0, 0))

    return pl.pallas_call(
        functools.partial(all_adjoint_kernel, margin=margin, facet_rows=facet_rows),
        out_shape=jax.ShapeDtypeStruct((count, payload_rows(rows), LANES), jnp.bfloat16),
        grid=(count // width,),
        in_specs=[in_scalar_memory()] * 2
        + [picked(height) for height in (strip_rows, 2 * margin, 2 * margin)],
        out_specs=pl.BlockSpec((width, payload_rows(rows), LANES), lambda j: (j, 0, 0)),
        scratch_shapes=band_scratch(bases, margin)
        + [
            pltpu.VMEM((bases, tall_height(strip_rows, margin), width * LANES), jnp.bfloat16),
            pltpu.VMEM((width, rows, bases * LANES), jnp.bfloat16),
            pltpu.VMEM((width, rows, WIDE), jnp.float32),
        ],
        name="all_adjoint",
    )(row_taps, col_taps, dual, above, below)


def part_scratch(bases, strip_rows, margin, count):
    rows = strip_rows + 2 * margin
    height = tall_height(strip_rows, margin)
    return band_scratch(bases, margin) + [
        pltpu.VMEM((-(-count // 2), bases, height, 2 * LANES), jnp.bfloat16),
        pltpu.VMEM((2, rows, bases * LANES), jnp.bfloat16),
        pltpu.VMEM((2, rows, WIDE), jnp.float32),
        pltpu.VMEM((count, payload_rows(rows), LANES), jnp.bfloat16),
        pltpu.SemaphoreType.DMA((3 * count,)),
        pltpu.SemaphoreType.DMA((count,)),
    ]


class PartAdjoint:
    def __init__(self, places, dual, above, below, outs, scratch, facet_rows):
        *self.bands, self.tall, self.mixed, self.wide, self.held, loads, self.stores = scratch
        self.places, self.outs = places, outs
        self.strip_rows = dual.shape[2]
        self.halo = above.shape[2]
        self.margin = self.halo // 2
        self.ends = is_at_ends(facet_rows)
        me = lax.axis_index("chan")
        self.copies = []
        for at, place in enumerate(places):
            lanes = pl.ds(at % 2 * LANES, LANES)
            group = []
            for source, first, height in (
                (dual, self.halo, self.strip_rows),
                (above, 0, self.halo),
                (below, self.halo + self.strip_rows, self.halo),
            ):
                group.append(
                    pltpu.make_async_copy(
                        source.at[:, me ^ place],
                        self.tall.at[at // 2, :, pl.ds(first, height), lanes],
                        loads.at[3 * at + len(group)],
                    )
                )
            self.copies.append(group)

    def start(self):
        for group in self.copies:
            for copy in group:
                copy.start()

    def fill(self, row_taps, col_taps):
        fill_adjoint_bands(row_taps, col_taps, *self.bands, self.margin)
        used = self.strip_rows + 2 * self.halo
        pairs, bases, height, lanes = self.tall.shape
        if used < height:
            blank = jnp.zeros((height - used, lanes), jnp.bfloat16)
            for pair in range(pairs):
                for basis in range(bases):
                    self.tall[pair, basis, used:] = blank

    def run(self):
        stores = []
        halo, strip_rows = self.halo, self.strip_rows
        bases, lanes = self.tall.shape[1], self.tall.shape[3]
        for pair in range(len(self.places) // 2):
            for group in self.copies[2 * pair : 2 * pair + 2]:
                for copy in group:
                    copy.wait()
            blank = jnp.zeros((halo, lanes), jnp.bfloat16)
            for condition, first in zip(self.ends, (0, halo + strip_rows)):

                @pl.when(condition)
                def _(first=first):
                    for basis in range(bases):
                        self.tall[pair, basis, first : first + halo] = blank

            adjoint_of(
                self.tall.at[pair], self.bands, self.mixed, self.wide, strip_rows, self.margin
            )
            for side in range(2):
                at = 2 * pair + side
                write_payload(self.held.at[at], self.wide.at[side], self.margin)
                stores.append(
                    pltpu.make_async_copy(self.held.at[at], self.outs[at], self.stores.at[at])
                )
                stores[-1].start()
        return stores


def far_adjoint_kernel(row_taps, col_taps, dual, above, below, *rest, places, facet_rows):
    count = len(places)
    part = PartAdjoint(places, dual, above, below, rest[:count], rest[count:], facet_rows)
    part.start()
    part.fill(row_taps, col_taps)
    for copy in part.run():
        copy.wait()


def far_adjoint(dual, above, below, row_taps, col_taps, places, facet_rows):
    bases, _, strip_rows, _ = dual.shape
    margin = row_taps.shape[1] // 2
    anywhere = pl.BlockSpec(memory_space=pl.ANY)
    rows = payload_rows(strip_rows + 2 * margin)
    return pl.pallas_call(
        functools.partial(far_adjoint_kernel, places=places, facet_rows=facet_rows),
        out_shape=[jax.ShapeDtypeStruct((rows, LANES), jnp.bfloat16)] * len(places),
        in_specs=[in_scalar_memory()] * 2 + [anywhere] * 3,
        out_specs=[anywhere] * len(places),
        scratch_shapes=part_scratch(bases, strip_rows, margin, len(places)),
        name="far_adjoint",
    )(row_taps, col_taps, dual, above, below)


def phase_seeds(pixels):
    step = 2.0 * math.pi / pixels
    coarse = 32
    half = pixels // 2
    scale = 1.0 / math.sqrt(pixels)
    where = np.arange(half)

    def of(rows, factor):
        angle = rows[:, None] * where[None, :] % pixels * step
        return np.cos(angle) * factor, -np.sin(angle) * factor

    big = of(np.arange(pixels // coarse) * coarse, 1.0)
    small = of(np.arange(coarse), scale)
    far = of(np.arange(half // coarse) * coarse * 2, 1.0)
    near = of(np.arange(coarse) * 2, scale)
    even = tuple(np.concatenate([x, y], axis=0) for x, y in zip(far, near))
    return tuple(np.asarray(v, np.float32) for v in (*big, *small, *even))


def twiddles(pixels):
    angle = 2.0 * math.pi / pixels * np.arange(pixels // 2)[:, None] * np.ones((1, LANES))
    return tuple(np.asarray(v, np.float32) for v in (np.cos(angle), -np.sin(angle)))


def spectrum_kernel(
    row_taps, col_taps, dual, above, below, own, other, own_counts, other_counts, *rest,
    places, margin, facet_rows,
):
    seeds, (turn_from_re, turn_from_im, _) = rest[:6], rest[6:9]
    near_outs, rest = rest[9 : 9 + len(places)], rest[9 + len(places) :]
    freq_out, keep, send = rest[:3]
    (
        picture, counts, cosine, sine, freq, turn_re, turn_im, top, low, whole, wide, loads
    ) = rest[3:15]
    split = lax.axis_index("split")
    cols, _, strip_rows, _ = own.shape
    pixels = picture.shape[0]
    half = pixels // 2
    part = half // 2
    if places:
        near = PartAdjoint(places, dual, above, below, near_outs, rest[15:], facet_rows)
        near.start()

    def strip_at(facet_row, which):
        return pl.multiple_of((2 * facet_row + which) * strip_rows, strip_rows)

    copies = []
    for facet_row in range(facet_rows):
        for col in range(cols):
            lanes = pl.ds(col * LANES, LANES)
            for source, which in ((own, split), (other, 1 - split)):
                copies.append(
                    pltpu.make_async_copy(
                        source.at[col, facet_row],
                        picture.at[pl.ds(strip_at(facet_row, which), strip_rows), lanes],
                        loads.at[len(copies)],
                    )
                )
    for source, target in ((turn_from_re, turn_re), (turn_from_im, turn_im)):
        copies.append(pltpu.make_async_copy(source, target, loads.at[len(copies)]))
    count_copies = []
    for source, which in ((own_counts, split), (other_counts, 1 - split)):
        for tile in range(part // LANES):
            lanes = pl.ds(pl.multiple_of(split * part + tile * LANES, LANES), LANES)
            count_copies.append(
                pltpu.make_async_copy(
                    source.at[:, lanes],
                    counts.at[tile, pl.ds(pl.multiple_of(which * half, half), half), :],
                    loads.at[len(copies) + len(count_copies)],
                )
            )
    for copy in (*copies, *count_copies):
        copy.start()
    if places:
        near.fill(row_taps, col_taps)
    fill_transforms(seeds, cosine, sine, freq)
    stores = [
        pltpu.make_async_copy(freq, freq_out, loads.at[len(copies) + len(count_copies)])
    ]
    stores[0].start()
    if places:
        stores += near.run()
    for copy in copies:
        copy.wait()
    block = min(256, half)
    first_table = freq.at[:, pl.ds(0, half)]

    def first(step, carry):
        at = pl.ds(pl.multiple_of(step * block, block), block)
        beyond = pl.ds(pl.multiple_of(half + step * block, block), block)
        one = exact_dot(picture[at, :], first_table[...])
        two = exact_dot(picture[beyond, :], first_table[...])
        total = one + two
        apart = one - two
        re, im = apart[:, :part], apart[:, part:]
        turn_r = jnp.concatenate([turn_re[at, :]] * (part // LANES), axis=1)
        turn_i = jnp.concatenate([turn_im[at, :]] * (part // LANES), axis=1)
        odd_re = (re * turn_r - im * turn_i).astype(jnp.bfloat16)
        odd_im = (re * turn_i + im * turn_r).astype(jnp.bfloat16)
        sum_re = total[:, :part].astype(jnp.bfloat16)
        sum_im = total[:, part:].astype(jnp.bfloat16)
        for place, value in enumerate((sum_re, sum_im, odd_re, odd_im)):
            top[at, place * part : (place + 1) * part] = value
        for place, value in enumerate((-sum_im, sum_re, -odd_im, odd_re)):
            low[at, place * part : (place + 1) * part] = value
        return carry

    lax.fori_loop(0, half // block, first, 0)
    for copy in count_copies:
        copy.wait()

    def second(step, carry):
        at = pl.ds(pl.multiple_of(step * block, block), block)
        vis = exact_dot(cosine[at, :], top[...]) + exact_dot(sine[at, :], low[...])
        for parity in range(2):
            picked = jnp.concatenate(
                [
                    counts.at[tile][pl.ds(2 * step * block + parity, block, stride=2), :]
                    for tile in range(part // LANES)
                ],
                axis=1,
            )
            scale = weight_unit * picked.astype(jnp.float32)
            re = parity * 2 * part
            im = re + part
            whole[at, re : re + part] = (vis[:, re : re + part] * scale).astype(jnp.bfloat16)
            whole[at, im : im + part] = (vis[:, im : im + part] * scale).astype(jnp.bfloat16)
        return carry

    lax.fori_loop(0, half // block, second, 0)
    for parity in range(2):
        re = slice(parity * 2 * part, (parity * 2 + 1) * part)
        im = slice((parity * 2 + 1) * part, (parity * 2 + 2) * part)
        low[:, re] = whole[:, im]
        low[:, im] = -whole[:, re]

    def third(step, carry):
        at = pl.ds(pl.multiple_of(step * block, block), block)
        beyond = pl.ds(pl.multiple_of(half + step * block, block), block)
        value = exact_dot(cosine[at, :], whole[...]) + exact_dot(sine[at, :], low[...])
        even, re, im = value[:, :half], value[:, half : half + part], value[:, half + part :]
        turn_r = jnp.concatenate([turn_re[at, :]] * (part // LANES), axis=1)
        turn_i = jnp.concatenate([turn_im[at, :]] * (part // LANES), axis=1)
        odd = jnp.concatenate([re * turn_r + im * turn_i, im * turn_r - re * turn_i], axis=1)
        wide[at, :] = (even + odd).astype(jnp.bfloat16)
        wide[beyond, :] = (even - odd).astype(jnp.bfloat16)
        return carry

    lax.fori_loop(0, half // block, third, 0)
    rows = strip_rows + 2 * margin
    for facet_row in range(facet_rows):
        for target, which in ((keep, split), (send, 1 - split)):
            at = strip_at(facet_row, which)
            base = facet_row * rows
            target[base : base + strip_rows, :] = wide[pl.ds(at, strip_rows), :]
            before = pl.multiple_of(lax.rem(at + pixels - 16, pixels), 16)
            after = pl.multiple_of(lax.rem(at + strip_rows, pixels), 16)
            ends = jnp.concatenate(
                [
                    wide[pl.ds(before, 16), :].astype(jnp.float32)[16 - margin :],
                    wide[pl.ds(after, 16), :].astype(jnp.float32)[:margin],
                ],
                axis=0,
            )
            target[base + strip_rows : base + rows, :] = ends.astype(jnp.bfloat16)
    for copy in stores:
        copy.wait()


def spectrum(
    own, other, own_counts, other_counts, dual, above, below, row_taps, col_taps, places, margin, after
):
    cols, facet_rows, strip_rows, lanes = own.shape
    bases = dual.shape[0]
    pixels = cols * lanes
    half = pixels // 2
    rows = facet_rows * (strip_rows + 2 * margin)
    shape = jax.ShapeDtypeStruct((rows, half), jnp.bfloat16)
    anywhere = pl.BlockSpec(memory_space=pl.ANY)
    inside = pl.BlockSpec(memory_space=pltpu.VMEM)
    payload = jax.ShapeDtypeStruct((payload_rows(strip_rows + 2 * margin), lanes), jnp.bfloat16)
    result = pl.pallas_call(
        functools.partial(
            spectrum_kernel, places=places, margin=margin, facet_rows=facet_rows
        ),
        out_shape=[payload] * len(places)
        + [jax.ShapeDtypeStruct((pixels, pixels), jnp.bfloat16), shape, shape],
        in_specs=[in_scalar_memory()] * 2 + [anywhere] * 7 + [inside] * 6 + [anywhere] * 3,
        out_specs=[anywhere] * (len(places) + 1) + [inside] * 2,
        scratch_shapes=[
            pltpu.VMEM((pixels, pixels), jnp.bfloat16),
            pltpu.VMEM((half // 2 // LANES, pixels, LANES), jnp.int32),
            pltpu.VMEM((half, half), jnp.bfloat16),
            pltpu.VMEM((half, half), jnp.bfloat16),
            pltpu.VMEM((pixels, pixels), jnp.bfloat16),
            pltpu.VMEM((half, LANES), jnp.float32),
            pltpu.VMEM((half, LANES), jnp.float32),
            pltpu.VMEM((half, pixels), jnp.bfloat16),
            pltpu.VMEM((half, pixels), jnp.bfloat16),
            pltpu.VMEM((half, pixels), jnp.bfloat16),
            pltpu.VMEM((pixels, half), jnp.bfloat16),
            pltpu.SemaphoreType.DMA((2 * cols * facet_rows + 3 + half // LANES,)),
        ]
        + (part_scratch(bases, strip_rows, margin, len(places)) if places else []),
        name="spectrum",
    )(
        row_taps, col_taps, dual, above, below, own, other, own_counts, other_counts,
        *phase_seeds(pixels), *twiddles(pixels), after,
    )
    return result[: len(places)], *result[len(places) :]


def gradient_kernel(
    kept, got, freq, own, above, below, own_dirty, dirty_above, dirty_below,
    stepped, edge_out, joined, *, margin
):
    split = lax.axis_index("split")
    cols, facet_rows, strip_rows, _ = own.shape
    half = kept.shape[1]
    rows = strip_rows + 2 * margin

    @pl.when(pl.program_id(0) == 0)
    def _():
        joined[:, :half] = kept[...]
        joined[:, half:] = got[...]

    def edges(upper, lower, col, facet_row):
        over = jnp.maximum(facet_row - 1 + split, 0)
        under = jnp.minimum(facet_row + split, facet_rows - 1)
        return jnp.concatenate(
            [
                upper[col, over].astype(jnp.float32)[16 - margin :],
                lower[col, under].astype(jnp.float32)[:margin],
            ],
            axis=0,
        )

    value = lax.dot_general(
        joined[...], freq[...], (((1,), (1,)), ((), ())), preferred_element_type=jnp.float32
    )
    for col in range(cols):
        for facet_row in range(facet_rows):
            base = facet_row * rows
            grad = value[base : base + rows, col * LANES : (col + 1) * LANES]
            image = own[col, facet_row]
            dirty = own_dirty[col, facet_row].astype(jnp.float32)
            moved = image.astype(jnp.float32) - primal_step * (grad[:strip_rows] - dirty)
            stepped[col, facet_row, :strip_rows] = moved.astype(jnp.bfloat16)
            image = edges(above, below, col, facet_row)
            dirty = edges(dirty_above, dirty_below, col, facet_row)
            moved = image - primal_step * (grad[strip_rows:] - dirty)
            stepped[col, facet_row, strip_rows:] = moved.astype(jnp.bfloat16)
            edge_out[col, facet_row] = image.astype(jnp.bfloat16)


def gradient_step(kept, got, freq, own, other, own_dirty, other_dirty, margin):
    cols, facet_rows, strip_rows, lanes = own.shape
    pixels = cols * lanes
    rows = strip_rows + 2 * margin
    pair = 2 if cols % 2 == 0 else 1

    def block(height, place):
        return pl.BlockSpec((pair, facet_rows, height, lanes), lambda j: (j, 0, place, 0))

    whole_strip, last, first = block(strip_rows, 0), block(16, strip_rows // 16 - 1), block(16, 0)
    return pl.pallas_call(
        functools.partial(gradient_kernel, margin=margin),
        out_shape=[
            jax.ShapeDtypeStruct((cols, facet_rows, rows, lanes), jnp.bfloat16),
            jax.ShapeDtypeStruct((cols, facet_rows, 2 * margin, lanes), jnp.bfloat16),
        ],
        grid=(cols // pair,),
        in_specs=[
            whole_block(kept.shape),
            whole_block(got.shape),
            pl.BlockSpec((pair * lanes, pixels), lambda j: (j, 0)),
            whole_strip, last, first, whole_strip, last, first,
        ],
        out_specs=[block(rows, 0), block(2 * margin, 0)],
        scratch_shapes=[pltpu.VMEM((kept.shape[0], pixels), jnp.bfloat16)],
        name="gradient",
    )(kept, got, freq, own, other, other, own_dirty, other_dirty, other_dirty)


def unpacked(packed, group, count, margin):
    return pltpu.roll(
        packed[:count], LANES - (margin + 2 * margin * group) % LANES, axis=1
    )


def update_kernel(stepped_from, image_from, edges, *rest, margin, facets, single):
    arrivals = 1 if single else facets
    blocks = rest[:arrivals]
    new_out = rest[arrivals]
    outs = rest[arrivals + 1 : 2 * arrivals + 1]
    stepped, image, new_image, adjoint, extrapolated, leaving, loads, arriving, stores = rest[
        2 * arrivals + 1 :
    ]
    me = lax.axis_index("chan")
    split = lax.axis_index("split")
    cols, facet_rows, rows, _ = stepped.shape
    strip_rows = rows - 2 * margin
    height = pack_height(rows)
    lane = lax.broadcasted_iota(jnp.int32, (1, LANES), 1)
    arrive = []
    for place, block in enumerate(blocks):
        target = adjoint if single else adjoint.at[me ^ place]
        arrive.append(pltpu.make_async_copy(block, target, arriving.at[place]))
        arrive[-1].start()
    load = []
    for col in range(cols):
        load.append(
            (
                pltpu.make_async_copy(stepped_from.at[col], stepped.at[col], loads.at[2 * col]),
                pltpu.make_async_copy(image_from.at[col], image.at[col], loads.at[2 * col + 1]),
            )
        )
        for copy in load[-1]:
            copy.start()
    for copy in arrive:
        copy.wait()

    def sides(take, group, count, left, has_left, right, has_right):
        from_left = take(left, group, count)
        from_right = take(right, group, count)
        return (
            jnp.where(lane < jnp.where(has_left, margin, 0), from_left, 0.0),
            jnp.where(lane >= jnp.where(has_right, LANES - margin, LANES), from_right, 0.0),
        )

    def packed_of(facet, group, count):
        tile = adjoint[facet, rows : rows + height, :].astype(jnp.float32)
        return unpacked(tile, group, count, margin)

    def update(facet):
        col = facet // facet_rows
        facet_row = facet % facet_rows
        left, has_left = jnp.maximum(facet - facet_rows, 0), facet >= facet_rows
        right, has_right = jnp.minimum(facet + facet_rows, facets - 1), facet < facets - facet_rows
        for group, first, count in row_groups(rows):
            add_left, add_right = sides(packed_of, group, count, left, has_left, right, has_right)
            at = slice(first, first + count)
            total = adjoint[facet, at, :].astype(jnp.float32) + add_left + add_right
            value = stepped[col, facet_row, at, :].astype(jnp.float32) - primal_step * total
            value = jnp.maximum(value, 0.0).astype(jnp.bfloat16).astype(jnp.float32)
            main = max(min(first + count, strip_rows) - first, 0)
            before = []
            if main > 0:
                before.append(image[col, facet_row, first : first + main, :].astype(jnp.float32))
            if main < count:
                after = first + main - strip_rows
                before.append(
                    edges[col, facet_row, after : after + count - main, :].astype(jnp.float32)
                )
            ahead = 2.0 * value - (before[0] if len(before) == 1 else jnp.concatenate(before, 0))
            if first + count > strip_rows:
                row = first + lax.broadcasted_iota(jnp.int32, (count, LANES), 0)
                top_there = (facet_row > 0) | (split > 0)
                low_there = (facet_row < facet_rows - 1) | (split < 1)
                middle = strip_rows + margin
                from_top = jnp.where(top_there, middle, strip_rows)
                to_low = jnp.where(low_there, rows, middle)
                ahead = jnp.where((row >= from_top) & (row < middle), 0.0, ahead)
                ahead = jnp.where(row >= to_low, 0.0, ahead)
            extrapolated[facet, at, :] = ahead.astype(jnp.bfloat16)
            if main > 0:
                new_image[col, facet_row, first : first + main, :] = value[:main].astype(jnp.bfloat16)

    stored = []
    for col in range(cols):
        for copy in load[col]:
            copy.wait()
        for facet_row in range(facet_rows):
            update(col * facet_rows + facet_row)
        stored.append(
            pltpu.make_async_copy(new_image.at[col], new_out.at[col], stores.at[col])
        )
        stored[-1].start()

    def whole_of(facet, group, count):
        first = group * height
        return extrapolated[facet, first : first + count, :].astype(jnp.float32)

    def write(out, facet):
        left, has_left = jnp.maximum(facet - facet_rows, 0), facet >= facet_rows
        right, has_right = jnp.minimum(facet + facet_rows, facets - 1), facet < facets - facet_rows
        packed = jnp.zeros((height, LANES), jnp.float32)
        for group, first, count in row_groups(rows):
            after, before = sides(whole_of, group, count, right, has_right, left, has_left)
            side = pltpu.roll(after + before, margin + 2 * margin * group, axis=1)
            if count < height:
                side = jnp.concatenate(
                    [side, jnp.zeros((height - count, LANES), jnp.float32)], axis=0
                )
            packed = packed + side
        out[:rows, :] = extrapolated[facet]
        out[rows:, :] = packed.astype(jnp.bfloat16)

    if single:
        each(facets, lambda facet: write(leaving.at[facet], facet))
        stored.append(pltpu.make_async_copy(leaving, outs[0], stores.at[cols]))
        stored[-1].start()
    else:
        for place in reversed(range(facets)):
            write(leaving.at[place], me ^ place)
            stored.append(
                pltpu.make_async_copy(leaving.at[place], outs[place], stores.at[cols + place])
            )
            stored[-1].start()
    for copy in stored:
        copy.wait()


def update_step(stepped, image, edges, blocks, margin, single):
    cols, facet_rows, rows, lanes = stepped.shape
    facets = cols * facet_rows
    tall_rows = payload_rows(rows)
    arrivals = (
        [jax.ShapeDtypeStruct((facets, tall_rows, lanes), jnp.bfloat16)]
        if single
        else [jax.ShapeDtypeStruct((tall_rows, lanes), jnp.bfloat16)] * facets
    )
    anywhere = pl.BlockSpec(memory_space=pl.ANY)
    results = pl.pallas_call(
        functools.partial(update_kernel, margin=margin, facets=facets, single=single),
        out_shape=[
            jax.ShapeDtypeStruct((cols, facet_rows, rows - 2 * margin, lanes), jnp.bfloat16)
        ]
        + arrivals,
        in_specs=[anywhere] * 2 + [pl.BlockSpec(memory_space=pltpu.VMEM)] + [anywhere] * len(blocks),
        out_specs=[anywhere] * (1 + len(arrivals)),
        scratch_shapes=[
            pltpu.VMEM(stepped.shape, jnp.bfloat16),
            pltpu.VMEM(image.shape, jnp.bfloat16),
            pltpu.VMEM(image.shape, jnp.bfloat16),
            pltpu.VMEM((facets, tall_rows, lanes), jnp.bfloat16),
            pltpu.VMEM((facets, rows, lanes), jnp.bfloat16),
            pltpu.VMEM((facets, tall_rows, lanes), jnp.bfloat16),
            pltpu.SemaphoreType.DMA((2 * cols,)),
            pltpu.SemaphoreType.DMA((len(blocks),)),
            pltpu.SemaphoreType.DMA((cols + len(blocks),)),
        ],
        name="update",
    )(stepped, image, edges, *blocks)
    return results[0], results[1:]


def shrink_kernel(row_taps, col_taps, mask, dual, *rest, margin, channels, single):
    arrivals = 1 if single else channels
    blocks = rest[:arrivals]
    out = rest[arrivals]
    row_band, col_band, wide, tall = rest[arrivals + 1 :]
    me = lax.axis_index("chan")
    basis = pl.program_id(0)
    taps = row_taps.shape[1]
    halo = 2 * margin
    strip_rows = dual.shape[2]
    rows = strip_rows + halo
    height = pack_height(rows)

    @pl.when(basis == 0)
    def _():
        for each_basis in range(row_taps.shape[0]):
            seed = band_seed(row_taps, each_basis, [margin + tap for tap in range(taps)])
            fill_band(row_band.at[each_basis], 0, BAND_ROWS, seed)
            seed = band_seed(col_taps, each_basis, [tap - margin for tap in range(taps)])
            fill_band(col_band.at[each_basis], 0, LANES, seed)
        tall[...] = jnp.zeros(tall.shape, tall.dtype)

        def unpack(channel, block):
            wide[channel, :, :LANES] = block[:rows, :]
            packed = block[rows : rows + height, :].astype(jnp.float32)
            for group, first, count in row_groups(rows):
                side = unpacked(packed, group, count, margin)
                wide[channel, first : first + count, LANES:] = side.astype(jnp.bfloat16)

        if single:
            each(channels, lambda channel: unpack(channel, blocks[0].at[channel]))
        else:
            for place, block in enumerate(blocks):
                unpack(me ^ place, block)

    def columns(channel):
        lanes = pl.ds(hint(channel * LANES, LANES), LANES)
        value = lax.dot_general(
            wide[channel], col_band[basis], (((1,), (1,)), ((), ())),
            preferred_element_type=jnp.float32,
        )
        blank = jnp.zeros((halo - margin, LANES), jnp.float32)
        tall[halo : halo + strip_rows, lanes] = value[:strip_rows].astype(jnp.bfloat16)
        tall[:halo, lanes] = jnp.concatenate(
            [blank, value[strip_rows : strip_rows + margin]], axis=0
        ).astype(jnp.bfloat16)
        tall[halo + strip_rows : 2 * halo + strip_rows, lanes] = jnp.concatenate(
            [value[strip_rows + margin :], blank], axis=0
        ).astype(jnp.bfloat16)

    each(channels, columns)
    piece = min(channels, 8)
    for first in range(0, strip_rows, BAND_ROWS):
        count = min(BAND_ROWS, strip_rows - first)
        stepped = []
        total = jnp.zeros((count, LANES), jnp.float32)
        for channel in range(0, channels, piece):
            value = exact_dot(
                row_band[basis, :count],
                tall[first : first + WIDE, channel * LANES : (channel + piece) * LANES],
            )
            for side in range(piece):
                coefficient = value[:, side * LANES : (side + 1) * LANES]
                moved = (
                    dual[0, channel + side, first : first + count].astype(jnp.float32)
                    + dual_step * coefficient
                )
                stepped.append(moved)
                total = total + moved * moved
        kept = mask[first : first + count].astype(jnp.float32)
        shrink = radius * kept / jnp.maximum(jnp.sqrt(total), radius)
        for channel in range(channels):
            out[0, channel, first : first + count] = (stepped[channel] * shrink).astype(jnp.bfloat16)


def shrink_step(row_taps, col_taps, mask, dual, blocks, single):
    bases, channels, strip_rows, lanes = dual.shape
    margin = row_taps.shape[1] // 2
    rows = strip_rows + 2 * margin
    return pl.pallas_call(
        functools.partial(shrink_kernel, margin=margin, channels=channels, single=single),
        out_shape=jax.ShapeDtypeStruct(dual.shape, jnp.bfloat16),
        grid=(bases,),
        in_specs=[
            in_scalar_memory(),
            in_scalar_memory(),
            whole_block(mask.shape),
            pl.BlockSpec((1, channels, strip_rows, lanes), lambda n: (n, 0, 0, 0)),
        ]
        + [whole_block(block.shape) for block in blocks],
        out_specs=pl.BlockSpec((1, channels, strip_rows, lanes), lambda n: (n, 0, 0, 0)),
        scratch_shapes=[
            pltpu.VMEM((bases, BAND_ROWS, WIDE), jnp.bfloat16),
            pltpu.VMEM((bases, LANES, WIDE), jnp.bfloat16),
            pltpu.VMEM((channels, rows, WIDE), jnp.bfloat16),
            pltpu.VMEM((max(padded_rows(strip_rows), strip_rows + 4 * margin), channels * lanes), jnp.bfloat16),
        ],
        name="shrink",
    )(row_taps, col_taps, mask, dual, *blocks)


def swapped(value):
    return lax.ppermute(value, "split", [(0, 1), (1, 0)])


def along_chain(value, by, facet_rows):
    count = lax.axis_size("chan") * 2
    chain = 2 * facet_rows
    pairs = [
        (i, i + by) for i in range(count) if 0 <= i + by < count and i // chain == (i + by) // chain
    ]
    return lax.ppermute(value, ("chan", "split"), pairs)


def crossed(blocks, single):
    count = lax.axis_size("chan")
    if single:
        return [lax.all_to_all(blocks[0], "chan", split_axis=0, concat_axis=0, tiled=True)]
    result = list(blocks)
    for place in reversed(range(1, count)):
        result[place] = lax.ppermute(blocks[place], "chan", [(i, i ^ place) for i in range(count)])
    return result


def in_parts(count):
    return 4 <= count <= 8 and count & count - 1 == 0


def per_device(sky_image, dirty_image, uv_weights, dual_coeffs, support_mask, row_taps, col_taps):
    facet_cols, facet_rows, strip_rows, lanes = (sky_image.shape[i] for i in (1, 2, 4, 5))
    bases, channels = dual_coeffs.shape[:2]
    margin = row_taps.shape[1] // 2
    count = lax.axis_size("chan")
    single = not in_parts(count)
    image = sky_image.reshape(facet_cols, facet_rows, strip_rows, lanes)
    dirty = dirty_image.reshape(image.shape)
    counts = uv_weights.reshape(uv_weights.shape[1:])
    dual = dual_coeffs.reshape(bases, channels, strip_rows, lanes)
    mask = support_mask.reshape(strip_rows, lanes)
    halo = 2 * margin
    top_rows, low_rows = dual[:, :, :halo], dual[:, :, strip_rows - halo :]
    if facet_rows == 1:
        ends = jnp.where(lax.axis_index("split") == 0, low_rows, top_rows)
        above = below = swapped(ends)
    else:
        above = along_chain(low_rows, 1, facet_rows)
        below = along_chain(top_rows, -1, facet_rows)
    other_image = swapped(image)
    other_counts = swapped(counts)
    other_dirty = swapped(dirty)
    if single:
        blocks = [all_adjoint(dual, above, below, row_taps, col_taps, facet_rows)]
        far, near = blocks, ()
    else:
        near = tuple(range(count // 2))
        far = far_adjoint(
            dual, above, below, row_taps, col_taps, tuple(range(count // 2, count)), facet_rows
        )
    close, freq, kept, sent = spectrum(
        image, other_image, counts, other_counts, dual, above, below,
        row_taps, col_taps, near, margin, far[0],
    )
    if not single:
        blocks = list(close) + list(far)
    arrived = crossed(blocks, single)
    got = swapped(sent)
    stepped, edges = gradient_step(
        kept, got, freq, image, other_image, dirty, other_dirty, margin
    )
    new_image, blocks = update_step(stepped, image, edges, arrived, margin, single)
    arrived = crossed(blocks, single)
    new_dual = shrink_step(row_taps, col_taps, mask, dual, arrived, single)
    return (new_image.reshape(sky_image.shape), new_dual.reshape(dual_coeffs.shape))


def solution(mesh):
    placed = (
        P(("cube", "chan"), None, None, "split", None, None),
        P(("cube", "chan"), None, None, "split", None, None),
        P(("cube", "chan"), "split", None),
        P(None, "cube", "chan", "split", None, None),
        P("chan", "split", None, None),
        P(),
        P(),
    )

    mapped = jax.shard_map(
        per_device,
        mesh=mesh,
        in_specs=placed,
        out_specs=(
            P(("cube", "chan"), None, None, "split", None, None),
            P(None, "cube", "chan", "split", None, None),
        ),
        check_vma=False,
    )
    count = mesh.shape["chan"]
    if not in_parts(count):
        return mapped
    return mapped
```

```python
import functools
import math

import jax
import jax.numpy as jnp
import numpy as np
from jax import lax
from jax.experimental import pallas as pl
from jax.experimental.pallas import tpu as pltpu
from jax.sharding import PartitionSpec as P


LANES = 128
WIDE = 2 * LANES
BAND_ROWS = 224
primal_step = 0.5
dual_step = 0.5
radius = 6.0
weight_unit = 0.25

OWN_COPIES = pltpu.CompilerParams(vmem_limit_bytes=67043328)


def whole_block(shape):
    zeros = (0,) * len(shape)
    return pl.BlockSpec(tuple(shape), lambda *_: zeros)


def in_scalar_memory():
    return pl.BlockSpec(memory_space=pltpu.SMEM)


def exact_dot(left, right):
    return jnp.dot(left, right, preferred_element_type=jnp.float32)


def each(count, body):
    if count <= 8:
        for index in range(count):
            body(index)
    else:

        def step(index, carry):
            body(index)
            return carry

        lax.fori_loop(0, count, step, 0)


def hint(value, multiple):
    return value if isinstance(value, int) else pl.multiple_of(value, multiple)


def band_seed(taps, basis, positions):
    lane = lax.broadcasted_iota(jnp.int32, (8, WIDE), 1)
    row = lax.broadcasted_iota(jnp.int32, (8, WIDE), 0)
    offset = lane - row & WIDE - 1
    seed = jnp.zeros((8, WIDE), jnp.float32)
    for tap, position in enumerate(positions):
        seed = jnp.where(offset == position % WIDE, taps[basis, tap], seed)
    return seed


def fill_band(target, first_row, rows, seed):
    for start in range(0, rows, 16):
        upper = seed if start == 0 else pltpu.roll(seed, start, axis=1)
        lower = pltpu.roll(seed, start + 8, axis=1)
        target[first_row + start : first_row + start + 16, :] = jnp.concatenate(
            [upper, lower], axis=0
        ).astype(jnp.bfloat16)


def fill_col_bands(target, taps, bases, margin):
    for basis in range(bases):
        count = taps.shape[1]
        seed = band_seed(taps, basis, [tap - margin for tap in range(count)])
        fill_band(target, basis * LANES, LANES, seed)


def pack_height(rows):
    return -(-rows // (8 * 16)) * 16


def payload_rows(rows):
    return rows + pack_height(rows)


def row_groups(rows):
    height = pack_height(rows)
    return [(g, g * height, min(height, rows - g * height)) for g in range(-(-rows // height))]


def padded_rows(strip_rows):
    chunks = -(-strip_rows // BAND_ROWS)
    return (chunks - 1) * BAND_ROWS + WIDE


def edge_band_of(taps, basis, margin):
    halo = 2 * margin
    lane = lax.broadcasted_iota(jnp.int32, (halo, LANES), 1)
    row = lax.broadcasted_iota(jnp.int32, (halo, LANES), 0)
    source = jnp.where(
        row < margin,
        jnp.where(lane < 2 * halo, halo + row - lane, -1),
        jnp.where(lane >= 2 * halo, row + 3 * halo - lane, -1),
    )
    edge = jnp.zeros((halo, LANES), jnp.float32)
    for tap in range(taps.shape[1]):
        edge = jnp.where(source == tap, taps[basis, tap], edge)
    return edge


def products(far_re, far_im, near_re, near_im):
    return (
        (far_re * near_re - far_im * near_im).astype(jnp.bfloat16),
        (far_re * near_im + far_im * near_re).astype(jnp.bfloat16),
    )


def fill_transforms(seeds, cosine, sine, freq):
    big_re, big_im, small_re, small_im, even_re, even_im = seeds
    split = lax.axis_index("split")
    coarse = small_re.shape[0]
    half = cosine.shape[0]
    part = half // 2

    def even_rows(group, carry):
        at = pl.ds(pl.multiple_of(group * coarse, coarse), coarse)
        one = pl.ds(group, 1)
        cosine[at, :], sine[at, :] = products(
            even_re[one, :], even_im[one, :], even_re[half // coarse :, :], even_im[half // coarse :, :]
        )
        return carry

    lax.fori_loop(0, half // coarse, even_rows, 0)

    def freq_rows(group, carry):
        at = pl.ds(pl.multiple_of(group * coarse, coarse), coarse)
        one = pl.ds(group, 1)
        for place in range(2):
            side = jnp.where(split == place, 0, 1) * part
            lanes = pl.ds(pl.multiple_of(side, part), part)
            re, im = products(
                big_re[one, lanes], big_im[one, lanes], small_re[:, lanes], small_im[:, lanes]
            )
            freq[at, 2 * place * part : (2 * place + 1) * part] = re
            freq[at, (2 * place + 1) * part : (2 * place + 2) * part] = im
        return carry

    lax.fori_loop(0, 2 * half // coarse, freq_rows, 0)


def fill_adjoint_bands(row_taps, col_taps, row_band, edge_band, col_band, margin):
    bases, taps = row_taps.shape
    for basis in range(bases):
        seed = band_seed(row_taps, basis, [3 * margin - tap for tap in range(taps)])
        fill_band(row_band.at[basis], 0, BAND_ROWS, seed)
        edge_band[basis] = edge_band_of(row_taps, basis, margin).astype(jnp.bfloat16)
    fill_col_bands(col_band, col_taps, bases, margin)


def is_at_ends(facet_rows):
    split = lax.axis_index("split")
    facet_row = lax.rem(lax.axis_index("chan"), facet_rows)
    return (facet_row == 0) & (split == 0), (facet_row == facet_rows - 1) & (split == 1)


def adjoint_of(tall, bands, mixed, wide, strip_rows, margin):
    row_band, edge_band, col_band = bands
    bases = tall.shape[0]
    width = tall.shape[2] // LANES
    halo = 2 * margin
    for basis in range(bases):
        into = slice(basis * LANES, (basis + 1) * LANES)

        def put(first, count, value):
            for side in range(width):
                mixed[side, first : first + count, into] = value[
                    :, side * LANES : (side + 1) * LANES
                ].astype(jnp.bfloat16)

        for first in range(0, strip_rows, BAND_ROWS):
            count = min(BAND_ROWS, strip_rows - first)
            put(first, count, exact_dot(row_band[basis, :count], tall[basis, first : first + WIDE]))
        ends = jnp.concatenate(
            [
                tall[basis, : 2 * halo],
                tall[basis, strip_rows : strip_rows + 2 * halo],
                jnp.zeros((LANES - 4 * halo, width * LANES), jnp.bfloat16),
            ],
            axis=0,
        )
        put(strip_rows, halo, exact_dot(edge_band[basis], ends))
    for side in range(width):
        wide[side] = exact_dot(mixed[side], col_band[...])


def write_payload(out, wide, margin):
    rows = wide.shape[0]
    height = pack_height(rows)
    packed = jnp.zeros((height, LANES), jnp.float32)
    for group, first, count in row_groups(rows):
        out[first : first + count, :] = wide[first : first + count, :LANES].astype(jnp.bfloat16)
        piece = wide[first : first + count, LANES:]
        piece = pltpu.roll(piece, margin + 2 * margin * group, axis=1)
        if count < height:
            piece = jnp.concatenate(
                [piece, jnp.zeros((height - count, LANES), jnp.float32)], axis=0
            )
        packed = packed + piece
    out[rows : rows + height, :] = packed.astype(jnp.bfloat16)


def tall_height(strip_rows, margin):
    return max(padded_rows(strip_rows), strip_rows + 4 * margin)


def band_scratch(bases, margin):
    return [
        pltpu.VMEM((bases, BAND_ROWS, WIDE), jnp.bfloat16),
        pltpu.VMEM((bases, 2 * margin, LANES), jnp.bfloat16),
        pltpu.VMEM((bases * LANES, WIDE), jnp.bfloat16),
    ]


def all_adjoint_kernel(row_taps, col_taps, dual, above, below, out, *scratch, margin, facet_rows):
    bands, (tall, mixed, wide) = scratch[:3], scratch[3:]
    bases, width, strip_rows, _ = dual.shape
    halo = 2 * margin

    @pl.when(pl.program_id(0) == 0)
    def _():
        fill_adjoint_bands(row_taps, col_taps, *bands, margin)
        tall[...] = jnp.zeros(tall.shape, tall.dtype)

    is_top, is_low = is_at_ends(facet_rows)
    for basis in range(bases):
        for side in range(width):
            lanes = slice(side * LANES, (side + 1) * LANES)
            top = above[basis, side]
            low = below[basis, side]
            tall[basis, :halo, lanes] = jnp.where(is_top, jnp.zeros_like(top), top)
            tall[basis, halo : halo + strip_rows, lanes] = dual[basis, side]
            tall[basis, halo + strip_rows : 2 * halo + strip_rows, lanes] = jnp.where(
                is_low, jnp.zeros_like(low), low
            )
    adjoint_of(tall, bands, mixed, wide, strip_rows, margin)
    for side in range(width):
        write_payload(out.at[side], wide.at[side], margin)


def all_adjoint(dual, above, below, row_taps, col_taps, facet_rows):
    bases, count, strip_rows, _ = dual.shape
    margin = row_taps.shape[1] // 2
    width = 2 if count % 2 == 0 else 1
    rows = strip_rows + 2 * margin

    def picked(height):
        return pl.BlockSpec((bases, width, height, LANES), lambda j: (0, j, 0, 0))

    return pl.pallas_call(
        functools.partial(all_adjoint_kernel, margin=margin, facet_rows=facet_rows),
        out_shape=jax.ShapeDtypeStruct((count, payload_rows(rows), LANES), jnp.bfloat16),
        grid=(count // width,),
        in_specs=[in_scalar_memory()] * 2
        + [picked(height) for height in (strip_rows, 2 * margin, 2 * margin)],
        out_specs=pl.BlockSpec((width, payload_rows(rows), LANES), lambda j: (j, 0, 0)),
        scratch_shapes=band_scratch(bases, margin)
        + [
            pltpu.VMEM((bases, tall_height(strip_rows, margin), width * LANES), jnp.bfloat16),
            pltpu.VMEM((width, rows, bases * LANES), jnp.bfloat16),
            pltpu.VMEM((width, rows, WIDE), jnp.float32),
        ],
        name="all_adjoint",
    )(row_taps, col_taps, dual, above, below)


def part_scratch(bases, strip_rows, margin, count):
    rows = strip_rows + 2 * margin
    height = tall_height(strip_rows, margin)
    return band_scratch(bases, margin) + [
        pltpu.VMEM((-(-count // 2), bases, height, 2 * LANES), jnp.bfloat16),
        pltpu.VMEM((2, rows, bases * LANES), jnp.bfloat16),
        pltpu.VMEM((2, rows, WIDE), jnp.float32),
        pltpu.VMEM((count, payload_rows(rows), LANES), jnp.bfloat16),
        pltpu.SemaphoreType.DMA((3 * count,)),
        pltpu.SemaphoreType.DMA((count,)),
    ]


class PartAdjoint:
    def __init__(self, places, dual, above, below, outs, scratch, facet_rows):
        *self.bands, self.tall, self.mixed, self.wide, self.held, loads, self.stores = scratch
        self.places, self.outs = places, outs
        self.strip_rows = dual.shape[2]
        self.halo = above.shape[2]
        self.margin = self.halo // 2
        self.ends = is_at_ends(facet_rows)
        me = lax.axis_index("chan")
        self.copies = []
        for at, place in enumerate(places):
            lanes = pl.ds(at % 2 * LANES, LANES)
            group = []
            for source, first, height in (
                (dual, self.halo, self.strip_rows),
                (above, 0, self.halo),
                (below, self.halo + self.strip_rows, self.halo),
            ):
                group.append(
                    pltpu.make_async_copy(
                        source.at[:, me ^ place],
                        self.tall.at[at // 2, :, pl.ds(first, height), lanes],
                        loads.at[3 * at + len(group)],
                    )
                )
            self.copies.append(group)

    def start(self):
        for group in self.copies:
            for copy in group:
                copy.start()

    def fill(self, row_taps, col_taps):
        fill_adjoint_bands(row_taps, col_taps, *self.bands, self.margin)
        used = self.strip_rows + 2 * self.halo
        pairs, bases, height, lanes = self.tall.shape
        if used < height:
            blank = jnp.zeros((height - used, lanes), jnp.bfloat16)
            for pair in range(pairs):
                for basis in range(bases):
                    self.tall[pair, basis, used:] = blank

    def run(self):
        stores = []
        halo, strip_rows = self.halo, self.strip_rows
        bases, lanes = self.tall.shape[1], self.tall.shape[3]
        for pair in range(len(self.places) // 2):
            for group in self.copies[2 * pair : 2 * pair + 2]:
                for copy in group:
                    copy.wait()
            blank = jnp.zeros((halo, lanes), jnp.bfloat16)
            for condition, first in zip(self.ends, (0, halo + strip_rows)):

                @pl.when(condition)
                def _(first=first):
                    for basis in range(bases):
                        self.tall[pair, basis, first : first + halo] = blank

            adjoint_of(
                self.tall.at[pair], self.bands, self.mixed, self.wide, strip_rows, self.margin
            )
            for side in range(2):
                at = 2 * pair + side
                write_payload(self.held.at[at], self.wide.at[side], self.margin)
                stores.append(
                    pltpu.make_async_copy(self.held.at[at], self.outs[at], self.stores.at[at])
                )
                stores[-1].start()
        return stores


def part_adjoint_kernel(row_taps, col_taps, dual, above, below, _, *rest, places, facet_rows):
    count = len(places)
    part = PartAdjoint(places, dual, above, below, rest[:count], rest[count:], facet_rows)
    part.start()
    part.fill(row_taps, col_taps)
    for copy in part.run():
        copy.wait()


def part_adjoint(dual, above, below, row_taps, col_taps, places, facet_rows, after):
    bases, _, strip_rows, _ = dual.shape
    margin = row_taps.shape[1] // 2
    anywhere = pl.BlockSpec(memory_space=pltpu.HBM)
    rows = payload_rows(strip_rows + 2 * margin)
    return pl.pallas_call(
        functools.partial(part_adjoint_kernel, places=places, facet_rows=facet_rows),
        out_shape=[jax.ShapeDtypeStruct((rows, LANES), jnp.bfloat16)] * len(places),
        in_specs=[in_scalar_memory()] * 2 + [anywhere] * 4,
        out_specs=[anywhere] * len(places),
        scratch_shapes=part_scratch(bases, strip_rows, margin, len(places)),
        compiler_params=OWN_COPIES,
        name="part_adjoint",
    )(row_taps, col_taps, dual, above, below, after)


def phase_seeds(pixels):
    step = 2.0 * math.pi / pixels
    coarse = 32
    half = pixels // 2
    scale = 1.0 / math.sqrt(pixels)
    where = np.arange(half)

    def of(rows, factor):
        angle = rows[:, None] * where[None, :] % pixels * step
        return np.cos(angle) * factor, -np.sin(angle) * factor

    big = of(np.arange(pixels // coarse) * coarse, 1.0)
    small = of(np.arange(coarse), scale)
    far = of(np.arange(half // coarse) * coarse * 2, 1.0)
    near = of(np.arange(coarse) * 2, scale)
    even = tuple(np.concatenate([x, y], axis=0) for x, y in zip(far, near))
    return tuple(np.asarray(v, np.float32) for v in (*big, *small, *even))


def twiddles(pixels):
    angle = 2.0 * math.pi / pixels * np.arange(pixels // 2)[:, None] * np.ones((1, LANES))
    return tuple(np.asarray(v, np.float32) for v in (np.cos(angle), -np.sin(angle)))


def spectrum_kernel(
    row_taps, col_taps, dual, above, below, own, other, own_counts, other_counts, *rest,
    places, margin, facet_rows,
):
    seeds, (turn_from_re, turn_from_im, _) = rest[:6], rest[6:9]
    near_outs, rest = rest[9 : 9 + len(places)], rest[9 + len(places) :]
    freq_out, keep, send = rest[:3]
    (
        picture, counts, cosine, sine, freq, turn_re, turn_im, top, low, whole, wide, loads
    ) = rest[3:15]
    split = lax.axis_index("split")
    cols, _, strip_rows, _ = own.shape
    pixels = picture.shape[0]
    half = pixels // 2
    part = half // 2
    if places:
        near = PartAdjoint(places, dual, above, below, near_outs, rest[15:], facet_rows)
        near.start()

    def strip_at(facet_row, which):
        return pl.multiple_of((2 * facet_row + which) * strip_rows, strip_rows)

    copies = []
    for facet_row in range(facet_rows):
        for col in range(cols):
            lanes = pl.ds(col * LANES, LANES)
            for source, which in ((own, split), (other, 1 - split)):
                copies.append(
                    pltpu.make_async_copy(
                        source.at[col, facet_row],
                        picture.at[pl.ds(strip_at(facet_row, which), strip_rows), lanes],
                        loads.at[len(copies)],
                    )
                )
    for source, target in ((turn_from_re, turn_re), (turn_from_im, turn_im)):
        copies.append(pltpu.make_async_copy(source, target, loads.at[len(copies)]))
    count_copies = []
    for source, which in ((own_counts, split), (other_counts, 1 - split)):
        for tile in range(part // LANES):
            lanes = pl.ds(pl.multiple_of(split * part + tile * LANES, LANES), LANES)
            count_copies.append(
                pltpu.make_async_copy(
                    source.at[:, lanes],
                    counts.at[tile, pl.ds(pl.multiple_of(which * half, half), half), :],
                    loads.at[len(copies) + len(count_copies)],
                )
            )
    for copy in (*copies, *count_copies):
        copy.start()
    if places:
        near.fill(row_taps, col_taps)
    fill_transforms(seeds, cosine, sine, freq)
    stores = [
        pltpu.make_async_copy(freq, freq_out, loads.at[len(copies) + len(count_copies)])
    ]
    stores[0].start()
    if places:
        stores += near.run()
    for copy in copies:
        copy.wait()
    block = min(256, half)
    first_table = freq.at[:, pl.ds(0, half)]

    def first(step, carry):
        at = pl.ds(pl.multiple_of(step * block, block), block)
        beyond = pl.ds(pl.multiple_of(half + step * block, block), block)
        one = exact_dot(picture[at, :], first_table[...])
        two = exact_dot(picture[beyond, :], first_table[...])
        total = one + two
        apart = one - two
        re, im = apart[:, :part], apart[:, part:]
        turn_r = jnp.concatenate([turn_re[at, :]] * (part // LANES), axis=1)
        turn_i = jnp.concatenate([turn_im[at, :]] * (part // LANES), axis=1)
        odd_re = (re * turn_r - im * turn_i).astype(jnp.bfloat16)
        odd_im = (re * turn_i + im * turn_r).astype(jnp.bfloat16)
        sum_re = total[:, :part].astype(jnp.bfloat16)
        sum_im = total[:, part:].astype(jnp.bfloat16)
        for place, value in enumerate((sum_re, sum_im, odd_re, odd_im)):
            top[at, place * part : (place + 1) * part] = value
        for place, value in enumerate((-sum_im, sum_re, -odd_im, odd_re)):
            low[at, place * part : (place + 1) * part] = value
        return carry

    lax.fori_loop(0, half // block, first, 0)
    for copy in count_copies:
        copy.wait()

    def second(step, carry):
        at = pl.ds(pl.multiple_of(step * block, block), block)
        vis = exact_dot(cosine[at, :], top[...]) + exact_dot(sine[at, :], low[...])
        for parity in range(2):
            picked = jnp.concatenate(
                [
                    counts.at[tile][pl.ds(2 * step * block + parity, block, stride=2), :]
                    for tile in range(part // LANES)
                ],
                axis=1,
            )
            scale = weight_unit * picked.astype(jnp.float32)
            re = parity * 2 * part
            im = re + part
            whole[at, re : re + part] = (vis[:, re : re + part] * scale).astype(jnp.bfloat16)
            whole[at, im : im + part] = (vis[:, im : im + part] * scale).astype(jnp.bfloat16)
        return carry

    lax.fori_loop(0, half // block, second, 0)
    for parity in range(2):
        re = slice(parity * 2 * part, (parity * 2 + 1) * part)
        im = slice((parity * 2 + 1) * part, (parity * 2 + 2) * part)
        low[:, re] = whole[:, im]
        low[:, im] = -whole[:, re]

    def third(step, carry):
        at = pl.ds(pl.multiple_of(step * block, block), block)
        beyond = pl.ds(pl.multiple_of(half + step * block, block), block)
        value = exact_dot(cosine[at, :], whole[...]) + exact_dot(sine[at, :], low[...])
        even, re, im = value[:, :half], value[:, half : half + part], value[:, half + part :]
        turn_r = jnp.concatenate([turn_re[at, :]] * (part // LANES), axis=1)
        turn_i = jnp.concatenate([turn_im[at, :]] * (part // LANES), axis=1)
        odd = jnp.concatenate([re * turn_r + im * turn_i, im * turn_r - re * turn_i], axis=1)
        wide[at, :] = (even + odd).astype(jnp.bfloat16)
        wide[beyond, :] = (even - odd).astype(jnp.bfloat16)
        return carry

    lax.fori_loop(0, half // block, third, 0)
    rows = strip_rows + 2 * margin
    for facet_row in range(facet_rows):
        for target, which in ((keep, split), (send, 1 - split)):
            at = strip_at(facet_row, which)
            base = facet_row * rows
            target[base : base + strip_rows, :] = wide[pl.ds(at, strip_rows), :]
            before = pl.multiple_of(lax.rem(at + pixels - 16, pixels), 16)
            after = pl.multiple_of(lax.rem(at + strip_rows, pixels), 16)
            ends = jnp.concatenate(
                [
                    wide[pl.ds(before, 16), :].astype(jnp.float32)[16 - margin :],
                    wide[pl.ds(after, 16), :].astype(jnp.float32)[:margin],
                ],
                axis=0,
            )
            target[base + strip_rows : base + rows, :] = ends.astype(jnp.bfloat16)
    for copy in stores:
        copy.wait()


def spectrum(
    own, other, own_counts, other_counts, dual, above, below, row_taps, col_taps, places, margin, after
):
    cols, facet_rows, strip_rows, lanes = own.shape
    bases = dual.shape[0]
    pixels = cols * lanes
    half = pixels // 2
    rows = facet_rows * (strip_rows + 2 * margin)
    shape = jax.ShapeDtypeStruct((rows, half), jnp.bfloat16)
    anywhere = pl.BlockSpec(memory_space=pltpu.HBM)
    inside = pl.BlockSpec(memory_space=pltpu.VMEM)
    payload = jax.ShapeDtypeStruct((payload_rows(strip_rows + 2 * margin), lanes), jnp.bfloat16)
    result = pl.pallas_call(
        functools.partial(
            spectrum_kernel, places=places, margin=margin, facet_rows=facet_rows
        ),
        out_shape=[payload] * len(places)
        + [jax.ShapeDtypeStruct((pixels, pixels), jnp.bfloat16), shape, shape],
        in_specs=[in_scalar_memory()] * 2 + [anywhere] * 7 + [inside] * 6 + [anywhere] * 3,
        out_specs=[anywhere] * (len(places) + 1) + [inside] * 2,
        scratch_shapes=[
            pltpu.VMEM((pixels, pixels), jnp.bfloat16),
            pltpu.VMEM((half // 2 // LANES, pixels, LANES), jnp.int32),
            pltpu.VMEM((half, half), jnp.bfloat16),
            pltpu.VMEM((half, half), jnp.bfloat16),
            pltpu.VMEM((pixels, pixels), jnp.bfloat16),
            pltpu.VMEM((half, LANES), jnp.float32),
            pltpu.VMEM((half, LANES), jnp.float32),
            pltpu.VMEM((half, pixels), jnp.bfloat16),
            pltpu.VMEM((half, pixels), jnp.bfloat16),
            pltpu.VMEM((half, pixels), jnp.bfloat16),
            pltpu.VMEM((pixels, half), jnp.bfloat16),
            pltpu.SemaphoreType.DMA((2 * cols * facet_rows + 3 + half // LANES,)),
        ]
        + (part_scratch(bases, strip_rows, margin, len(places)) if places else []),
        compiler_params=OWN_COPIES,
        name="spectrum",
    )(
        row_taps, col_taps, dual, above, below, own, other, own_counts, other_counts,
        *phase_seeds(pixels), *twiddles(pixels), after,
    )
    return result[: len(places)], *result[len(places) :]


def gradient_kernel(
    kept, got, freq_from, own_from, other, dirty_from, other_dirty, out, edge_out,
    joined, freq, own, dirty, above, below, dirty_above, dirty_below, stepped, loads, stores,
    *, margin
):
    split = lax.axis_index("split")
    cols, facet_rows, strip_rows, _ = own.shape
    half = kept.shape[1]
    rows = strip_rows + 2 * margin
    pair = 2 if cols % 2 == 0 else 1
    started = []

    def load(source, target):
        copy = pltpu.make_async_copy(source, target, loads.at[len(started)])
        copy.start()
        started.append(copy)
        return copy

    first = [load(kept, joined.at[:, pl.ds(0, half)])]
    steps = []
    for step in range(cols // pair):
        lines = pl.ds(step * pair * LANES, pair * LANES)
        some = pl.ds(step * pair, pair)
        steps.append(
            [
                load(freq_from.at[lines], freq.at[lines]),
                load(own_from.at[some], own.at[some]),
                load(dirty_from.at[some], dirty.at[some]),
            ]
        )
        if step == 0:
            first.append(load(got, joined.at[:, pl.ds(half, half)]))
            last, start = pl.ds(strip_rows - 16, 16), pl.ds(0, 16)
            first.append(load(other.at[:, :, last], above))
            first.append(load(other.at[:, :, start], below))
            first.append(load(other_dirty.at[:, :, last], dirty_above))
            first.append(load(other_dirty.at[:, :, start], dirty_below))

    def edges(upper, lower, col, facet_row):
        over = jnp.maximum(facet_row - 1 + split, 0)
        under = jnp.minimum(facet_row + split, facet_rows - 1)
        return jnp.concatenate(
            [
                upper[col, over].astype(jnp.float32)[16 - margin :],
                lower[col, under].astype(jnp.float32)[:margin],
            ],
            axis=0,
        )

    for copy in first:
        copy.wait()
    stored = []
    for step in range(cols // pair):
        for copy in steps[step]:
            copy.wait()
        value = lax.dot_general(
            joined[...],
            freq[step * pair * LANES : (step + 1) * pair * LANES, :],
            (((1,), (1,)), ((), ())),
            preferred_element_type=jnp.float32,
        )
        for side in range(pair):
            col = step * pair + side
            for facet_row in range(facet_rows):
                base = facet_row * rows
                grad = value[base : base + rows, side * LANES : (side + 1) * LANES]
                moved = own[col, facet_row].astype(jnp.float32) - primal_step * (
                    grad[:strip_rows] - dirty[col, facet_row].astype(jnp.float32)
                )
                stepped[col, facet_row, :strip_rows] = moved.astype(jnp.bfloat16)
                image = edges(above, below, col, facet_row)
                moved = image - primal_step * (
                    grad[strip_rows:] - edges(dirty_above, dirty_below, col, facet_row)
                )
                stepped[col, facet_row, strip_rows:] = moved.astype(jnp.bfloat16)
                edge_out[col, facet_row] = image.astype(jnp.bfloat16)
        some = pl.ds(step * pair, pair)
        stored.append(pltpu.make_async_copy(stepped.at[some], out.at[some], stores.at[step]))
        stored[-1].start()
    for copy in stored:
        copy.wait()


def gradient_step(kept, got, freq, own, other, own_dirty, other_dirty, margin):
    cols, facet_rows, strip_rows, lanes = own.shape
    pixels = cols * lanes
    rows = strip_rows + 2 * margin
    anywhere = pl.BlockSpec(memory_space=pltpu.HBM)
    edge = (cols, facet_rows, 16, lanes)
    return pl.pallas_call(
        functools.partial(gradient_kernel, margin=margin),
        out_shape=[
            jax.ShapeDtypeStruct((cols, facet_rows, rows, lanes), jnp.bfloat16),
            jax.ShapeDtypeStruct((cols, facet_rows, 2 * margin, lanes), jnp.bfloat16),
        ],
        in_specs=[anywhere] * 7,
        out_specs=[anywhere, pl.BlockSpec(memory_space=pltpu.VMEM)],
        scratch_shapes=[
            pltpu.VMEM((kept.shape[0], pixels), jnp.bfloat16),
            pltpu.VMEM(freq.shape, jnp.bfloat16),
            pltpu.VMEM(own.shape, jnp.bfloat16),
            pltpu.VMEM(own.shape, jnp.bfloat16),
            *[pltpu.VMEM(edge, jnp.bfloat16)] * 4,
            pltpu.VMEM((cols, facet_rows, rows, lanes), jnp.bfloat16),
            pltpu.SemaphoreType.DMA((6 + 3 * cols,)),
            pltpu.SemaphoreType.DMA((cols,)),
        ],
        compiler_params=OWN_COPIES,
        name="gradient",
    )(kept, got, freq, own, other, own_dirty, other_dirty)


def unpacked(packed, group, count, margin):
    return pltpu.roll(
        packed[:count], LANES - (margin + 2 * margin * group) % LANES, axis=1
    )


def update_kernel(stepped_from, image_from, edges, *rest, margin, facets, single):
    arrivals = 1 if single else facets
    blocks = rest[:arrivals]
    new_out = rest[arrivals]
    outs = rest[arrivals + 1 : 2 * arrivals + 1]
    stepped, image, new_image, adjoint, apart, extrapolated, leaving = rest[2 * arrivals + 1 : -3]
    loads, arriving, stores = rest[-3:]
    me = lax.axis_index("chan")
    split = lax.axis_index("split")
    cols, facet_rows, rows, _ = stepped.shape
    strip_rows = rows - 2 * margin
    height = pack_height(rows)
    lane = lax.broadcasted_iota(jnp.int32, (1, LANES), 1)
    arrive = []
    for place, block in enumerate(blocks):
        target = adjoint if single else adjoint.at[me ^ place]
        arrive.append(pltpu.make_async_copy(block, target, arriving.at[place]))
        arrive[-1].start()
    load = []
    for col in range(cols):
        load.append(
            (
                pltpu.make_async_copy(stepped_from.at[col], stepped.at[col], loads.at[2 * col]),
                pltpu.make_async_copy(image_from.at[col], image.at[col], loads.at[2 * col + 1]),
            )
        )
        for copy in load[-1]:
            copy.start()

    def unpack(facet):
        tile = adjoint[facet, rows : rows + height, :].astype(jnp.float32)
        for group, first, count in row_groups(rows):
            apart[facet, first : first + count, :] = unpacked(
                tile, group, count, margin
            ).astype(jnp.bfloat16)

    for place, copy in enumerate(arrive):
        copy.wait()
        if not single:
            unpack(me ^ place)
    if single:
        each(facets, unpack)

    def sides(take, group, count, left, has_left, right, has_right):
        from_left = take(left, group, count)
        from_right = take(right, group, count)
        return (
            jnp.where(lane < jnp.where(has_left, margin, 0), from_left, 0.0),
            jnp.where(lane >= jnp.where(has_right, LANES - margin, LANES), from_right, 0.0),
        )

    def apart_of(facet, group, count):
        first = group * height
        return apart[facet, first : first + count, :].astype(jnp.float32)

    def update(facet):
        col = facet // facet_rows
        facet_row = facet % facet_rows
        left, has_left = jnp.maximum(facet - facet_rows, 0), facet >= facet_rows
        right, has_right = jnp.minimum(facet + facet_rows, facets - 1), facet < facets - facet_rows
        for group, first, count in row_groups(rows):
            add_left, add_right = sides(apart_of, group, count, left, has_left, right, has_right)
            at = slice(first, first + count)
            total = adjoint[facet, at, :].astype(jnp.float32) + add_left + add_right
            value = stepped[col, facet_row, at, :].astype(jnp.float32) - primal_step * total
            value = jnp.maximum(value, 0.0).astype(jnp.bfloat16).astype(jnp.float32)
            main = max(min(first + count, strip_rows) - first, 0)
            before = []
            if main > 0:
                before.append(image[col, facet_row, first : first + main, :].astype(jnp.float32))
            if main < count:
                after = first + main - strip_rows
                before.append(
                    edges[col, facet_row, after : after + count - main, :].astype(jnp.float32)
                )
            ahead = 2.0 * value - (before[0] if len(before) == 1 else jnp.concatenate(before, 0))
            if first + count > strip_rows:
                row = first + lax.broadcasted_iota(jnp.int32, (count, LANES), 0)
                top_there = (facet_row > 0) | (split > 0)
                low_there = (facet_row < facet_rows - 1) | (split < 1)
                middle = strip_rows + margin
                from_top = jnp.where(top_there, middle, strip_rows)
                to_low = jnp.where(low_there, rows, middle)
                ahead = jnp.where((row >= from_top) & (row < middle), 0.0, ahead)
                ahead = jnp.where(row >= to_low, 0.0, ahead)
            extrapolated[facet, at, :] = ahead.astype(jnp.bfloat16)
            if main > 0:
                new_image[col, facet_row, first : first + main, :] = value[:main].astype(jnp.bfloat16)

    stored = []
    for col in range(cols):
        for copy in load[col]:
            copy.wait()
        for facet_row in range(facet_rows):
            update(col * facet_rows + facet_row)
        stored.append(
            pltpu.make_async_copy(new_image.at[col], new_out.at[col], stores.at[col])
        )
        stored[-1].start()

    def whole_of(facet, group, count):
        first = group * height
        return extrapolated[facet, first : first + count, :].astype(jnp.float32)

    def write(out, facet):
        left, has_left = jnp.maximum(facet - facet_rows, 0), facet >= facet_rows
        right, has_right = jnp.minimum(facet + facet_rows, facets - 1), facet < facets - facet_rows
        packed = jnp.zeros((height, LANES), jnp.float32)
        for group, first, count in row_groups(rows):
            after, before = sides(whole_of, group, count, right, has_right, left, has_left)
            side = pltpu.roll(after + before, margin + 2 * margin * group, axis=1)
            if count < height:
                side = jnp.concatenate(
                    [side, jnp.zeros((height - count, LANES), jnp.float32)], axis=0
                )
            packed = packed + side
        out[:rows, :] = extrapolated[facet]
        out[rows:, :] = packed.astype(jnp.bfloat16)

    if single:
        each(facets, lambda facet: write(leaving.at[facet], facet))
        stored.append(pltpu.make_async_copy(leaving, outs[0], stores.at[cols]))
        stored[-1].start()
    else:
        for place in reversed(range(facets)):
            write(leaving.at[place], me ^ place)
            stored.append(
                pltpu.make_async_copy(leaving.at[place], outs[place], stores.at[cols + place])
            )
            stored[-1].start()
    for copy in stored:
        copy.wait()


def update_step(stepped, image, edges, blocks, margin, single):
    cols, facet_rows, rows, lanes = stepped.shape
    facets = cols * facet_rows
    tall_rows = payload_rows(rows)
    arrivals = (
        [jax.ShapeDtypeStruct((facets, tall_rows, lanes), jnp.bfloat16)]
        if single
        else [jax.ShapeDtypeStruct((tall_rows, lanes), jnp.bfloat16)] * facets
    )
    anywhere = pl.BlockSpec(memory_space=pltpu.HBM)
    results = pl.pallas_call(
        functools.partial(update_kernel, margin=margin, facets=facets, single=single),
        out_shape=[
            jax.ShapeDtypeStruct((cols, facet_rows, rows - 2 * margin, lanes), jnp.bfloat16)
        ]
        + arrivals,
        in_specs=[anywhere] * 2 + [pl.BlockSpec(memory_space=pltpu.VMEM)] + [anywhere] * len(blocks),
        out_specs=[anywhere] * (1 + len(arrivals)),
        scratch_shapes=[
            pltpu.VMEM(stepped.shape, jnp.bfloat16),
            pltpu.VMEM(image.shape, jnp.bfloat16),
            pltpu.VMEM(image.shape, jnp.bfloat16),
            pltpu.VMEM((facets, tall_rows, lanes), jnp.bfloat16),
            pltpu.VMEM((facets, rows, lanes), jnp.bfloat16),
            pltpu.VMEM((facets, rows, lanes), jnp.bfloat16),
            pltpu.VMEM((facets, tall_rows, lanes), jnp.bfloat16),
            pltpu.SemaphoreType.DMA((2 * cols,)),
            pltpu.SemaphoreType.DMA((len(blocks),)),
            pltpu.SemaphoreType.DMA((cols + len(blocks),)),
        ],
        compiler_params=OWN_COPIES,
        name="update",
    )(stepped, image, edges, *blocks)
    return results[0], results[1:]


def shrink_kernel(row_taps, col_taps, mask, dual, *rest, margin, channels, single):
    arrivals = 1 if single else channels
    blocks = rest[:arrivals]
    out = rest[arrivals]
    row_band, col_band, wide, tall = rest[arrivals + 1 :]
    me = lax.axis_index("chan")
    basis = pl.program_id(0)
    taps = row_taps.shape[1]
    halo = 2 * margin
    strip_rows = dual.shape[2]
    rows = strip_rows + halo
    height = pack_height(rows)

    @pl.when(basis == 0)
    def _():
        for each_basis in range(row_taps.shape[0]):
            seed = band_seed(row_taps, each_basis, [margin + tap for tap in range(taps)])
            fill_band(row_band.at[each_basis], 0, BAND_ROWS, seed)
            seed = band_seed(col_taps, each_basis, [tap - margin for tap in range(taps)])
            fill_band(col_band.at[each_basis], 0, LANES, seed)
        tall[...] = jnp.zeros(tall.shape, tall.dtype)

        def unpack(channel, block):
            wide[channel, :, :LANES] = block[:rows, :]
            packed = block[rows : rows + height, :].astype(jnp.float32)
            for group, first, count in row_groups(rows):
                side = unpacked(packed, group, count, margin)
                wide[channel, first : first + count, LANES:] = side.astype(jnp.bfloat16)

        if single:
            each(channels, lambda channel: unpack(channel, blocks[0].at[channel]))
        else:
            for place, block in enumerate(blocks):
                unpack(me ^ place, block)

    def columns(channel):
        lanes = pl.ds(hint(channel * LANES, LANES), LANES)
        value = lax.dot_general(
            wide[channel], col_band[basis], (((1,), (1,)), ((), ())),
            preferred_element_type=jnp.float32,
        )
        blank = jnp.zeros((halo - margin, LANES), jnp.float32)
        tall[halo : halo + strip_rows, lanes] = value[:strip_rows].astype(jnp.bfloat16)
        tall[:halo, lanes] = jnp.concatenate(
            [blank, value[strip_rows : strip_rows + margin]], axis=0
        ).astype(jnp.bfloat16)
        tall[halo + strip_rows : 2 * halo + strip_rows, lanes] = jnp.concatenate(
            [value[strip_rows + margin :], blank], axis=0
        ).astype(jnp.bfloat16)

    each(channels, columns)
    piece = min(channels, 8)
    for first in range(0, strip_rows, BAND_ROWS):
        count = min(BAND_ROWS, strip_rows - first)
        stepped = []
        total = jnp.zeros((count, LANES), jnp.float32)
        for channel in range(0, channels, piece):
            value = exact_dot(
                row_band[basis, :count],
                tall[first : first + WIDE, channel * LANES : (channel + piece) * LANES],
            )
            for side in range(piece):
                coefficient = value[:, side * LANES : (side + 1) * LANES]
                moved = (
                    dual[0, channel + side, first : first + count].astype(jnp.float32)
                    + dual_step * coefficient
                )
                stepped.append(moved)
                total = total + moved * moved
        kept = mask[first : first + count].astype(jnp.float32)
        shrink = radius * kept / jnp.maximum(jnp.sqrt(total), radius)
        for channel in range(channels):
            out[0, channel, first : first + count] = (stepped[channel] * shrink).astype(jnp.bfloat16)


def shrink_step(row_taps, col_taps, mask, dual, blocks, single):
    bases, channels, strip_rows, lanes = dual.shape
    margin = row_taps.shape[1] // 2
    rows = strip_rows + 2 * margin
    return pl.pallas_call(
        functools.partial(shrink_kernel, margin=margin, channels=channels, single=single),
        out_shape=jax.ShapeDtypeStruct(dual.shape, jnp.bfloat16),
        grid=(bases,),
        in_specs=[
            in_scalar_memory(),
            in_scalar_memory(),
            whole_block(mask.shape),
            pl.BlockSpec((1, channels, strip_rows, lanes), lambda n: (n, 0, 0, 0)),
        ]
        + [whole_block(block.shape) for block in blocks],
        out_specs=pl.BlockSpec((1, channels, strip_rows, lanes), lambda n: (n, 0, 0, 0)),
        scratch_shapes=[
            pltpu.VMEM((bases, BAND_ROWS, WIDE), jnp.bfloat16),
            pltpu.VMEM((bases, LANES, WIDE), jnp.bfloat16),
            pltpu.VMEM((channels, rows, WIDE), jnp.bfloat16),
            pltpu.VMEM((max(padded_rows(strip_rows), strip_rows + 4 * margin), channels * lanes), jnp.bfloat16),
        ],
        name="shrink",
    )(row_taps, col_taps, mask, dual, *blocks)


def shrink_part_kernel(row_taps, col_taps, dual, *rest, places, margin, final):
    count = len(places)
    blocks, rest = rest[:count], rest[count:]
    if final:
        mask, before_from, total_from, out_to = rest[:4]
        rest = rest[4:]
    else:
        out_to, total_to = rest[:2]
        rest = rest[2:]
    row_band, col_band, arrived, wide, tall, field, held, before, total, loads, stores = rest
    me = lax.axis_index("chan")
    bases, taps = row_taps.shape
    halo = 2 * margin
    strip_rows = dual.shape[2]
    rows = strip_rows + halo
    height = pack_height(rows)
    started = []

    def load(source, target):
        copy = pltpu.make_async_copy(source, target, loads.at[len(started)])
        copy.start()
        started.append(copy)
        return copy

    stored = []

    def store(source, target):
        copy = pltpu.make_async_copy(source, target, stores.at[len(stored)])
        copy.start()
        stored.append(copy)

    arrive = [load(block, arrived.at[at]) for at, block in enumerate(blocks)]
    fields = []
    for basis in range(bases):
        group = [
            load(dual.at[basis, me ^ place], field.at[basis, at]) for at, place in enumerate(places)
        ]
        if final:
            group.append(load(before_from.at[basis], before.at[basis]))
            group.append(load(total_from.at[basis], total.at[basis]))
        fields.append(group)
    for basis in range(bases):
        seed = band_seed(row_taps, basis, [margin + tap for tap in range(taps)])
        fill_band(row_band.at[basis], 0, BAND_ROWS, seed)
        used = strip_rows + 2 * halo
        if used < tall.shape[1]:
            tall[basis, used:] = jnp.zeros((tall.shape[1] - used, tall.shape[2]), jnp.bfloat16)
    fill_col_bands(col_band, col_taps, bases, margin)
    for at in range(count):
        arrive[at].wait()
        block = arrived.at[at]
        wide[at, :, :LANES] = block[:rows, :]
        packed = block[rows : rows + height, :].astype(jnp.float32)
        for group, first, some in row_groups(rows):
            side = unpacked(packed, group, some, margin)
            wide[at, first : first + some, LANES:] = side.astype(jnp.bfloat16)
        value = lax.dot_general(
            wide[at], col_band[...], (((1,), (1,)), ((), ())), preferred_element_type=jnp.float32
        )
        blank = jnp.zeros((halo - margin, LANES), jnp.float32)
        lanes = slice(at * LANES, (at + 1) * LANES)
        for basis in range(bases):
            mine = value[:, basis * LANES : (basis + 1) * LANES]
            tall[basis, halo : halo + strip_rows, lanes] = mine[:strip_rows].astype(jnp.bfloat16)
            tall[basis, :halo, lanes] = jnp.concatenate(
                [blank, mine[strip_rows : strip_rows + margin]], axis=0
            ).astype(jnp.bfloat16)
            tall[basis, halo + strip_rows : 2 * halo + strip_rows, lanes] = jnp.concatenate(
                [mine[strip_rows + margin :], blank], axis=0
            ).astype(jnp.bfloat16)
    for basis in range(bases):
        for copy in fields[basis]:
            copy.wait()
        for first in range(0, strip_rows, BAND_ROWS):
            some = min(BAND_ROWS, strip_rows - first)
            here = slice(first, first + some)
            value = exact_dot(row_band[basis, :some], tall[basis, first : first + WIDE])
            if final:
                squares = total[basis, here]
            else:
                squares = jnp.zeros((some, LANES), jnp.float32)
            stepped = []
            for at in range(count):
                moved = (
                    field[basis, at, here].astype(jnp.float32)
                    + dual_step * value[:, at * LANES : (at + 1) * LANES]
                )
                stepped.append(moved)
                squares = squares + moved * moved
            if final:
                kept = mask[here].astype(jnp.float32)
                scale = radius * kept / jnp.maximum(jnp.sqrt(squares), radius)
                for at in range(count):
                    held[basis, at, here] = (stepped[at] * scale).astype(jnp.bfloat16)
                    earlier = before[basis, at, here].astype(jnp.float32)
                    before[basis, at, here] = (earlier * scale).astype(jnp.bfloat16)
            else:
                total[basis, here] = squares
                for at in range(count):
                    held[basis, at, here] = stepped[at].astype(jnp.bfloat16)
        if final:
            for at, place in enumerate(places):
                store(held.at[basis, at], out_to.at[basis, me ^ place])
                store(before.at[basis, at], out_to.at[basis, me ^ place ^ count])
        else:
            store(held.at[basis], out_to.at[basis])
            store(total.at[basis], total_to.at[basis])
    for copy in stored:
        copy.wait()


def shrink_part(row_taps, col_taps, dual, blocks, places, earlier=None):
    bases, _, strip_rows, lanes = dual.shape
    count = len(places)
    margin = row_taps.shape[1] // 2
    rows = strip_rows + 2 * margin
    anywhere = pl.BlockSpec(memory_space=pltpu.HBM)
    part = (bases, count, strip_rows, lanes)
    final = earlier is not None
    if final:
        more = (pl.BlockSpec(memory_space=pltpu.VMEM), anywhere, anywhere)
        out_shape = jax.ShapeDtypeStruct(dual.shape, jnp.bfloat16)
        out_specs = anywhere
    else:
        more, earlier = (), ()
        out_shape = [
            jax.ShapeDtypeStruct(part, jnp.bfloat16),
            jax.ShapeDtypeStruct((bases, strip_rows, lanes), jnp.float32),
        ]
        out_specs = [anywhere, anywhere]
    return pl.pallas_call(
        functools.partial(shrink_part_kernel, places=places, margin=margin, final=final),
        out_shape=out_shape,
        in_specs=[in_scalar_memory()] * 2 + [anywhere] * (1 + count) + list(more),
        out_specs=out_specs,
        scratch_shapes=[
            pltpu.VMEM((bases, BAND_ROWS, WIDE), jnp.bfloat16),
            pltpu.VMEM((bases * LANES, WIDE), jnp.bfloat16),
            pltpu.VMEM((count, payload_rows(rows), lanes), jnp.bfloat16),
            pltpu.VMEM((count, rows, WIDE), jnp.bfloat16),
            pltpu.VMEM((bases, tall_height(strip_rows, margin), count * lanes), jnp.bfloat16),
            pltpu.VMEM(part, jnp.bfloat16),
            pltpu.VMEM(part, jnp.bfloat16),
            pltpu.VMEM(part if final else (1, 1, 16, lanes), jnp.bfloat16),
            pltpu.VMEM((bases, strip_rows, lanes), jnp.float32),
            pltpu.SemaphoreType.DMA((count + bases * (count + 2),)),
            pltpu.SemaphoreType.DMA((2 * bases * count,)),
        ],
        compiler_params=OWN_COPIES,
        name="shrink_part",
    )(row_taps, col_taps, dual, *blocks, *earlier)


def swapped(value):
    return lax.ppermute(value, "split", [(0, 1), (1, 0)])


def along_chain(value, by, facet_rows):
    count = lax.axis_size("chan") * 2
    chain = 2 * facet_rows
    pairs = [
        (i, i + by) for i in range(count) if 0 <= i + by < count and i // chain == (i + by) // chain
    ]
    return lax.ppermute(value, ("chan", "split"), pairs)


def crossed(blocks, single):
    count = lax.axis_size("chan")
    if single:
        return [lax.all_to_all(blocks[0], "chan", split_axis=0, concat_axis=0, tiled=True)]
    result = list(blocks)
    for place in reversed(range(1, count)):
        result[place] = lax.ppermute(blocks[place], "chan", [(i, i ^ place) for i in range(count)])
    return result


def in_parts(count):
    return 4 <= count <= 8 and count & count - 1 == 0


def per_device(sky_image, dirty_image, uv_weights, dual_coeffs, support_mask, row_taps, col_taps):
    facet_cols, facet_rows, strip_rows, lanes = (sky_image.shape[i] for i in (1, 2, 4, 5))
    bases, channels = dual_coeffs.shape[:2]
    margin = row_taps.shape[1] // 2
    count = lax.axis_size("chan")
    single = not in_parts(count)
    image = sky_image.reshape(facet_cols, facet_rows, strip_rows, lanes)
    dirty = dirty_image.reshape(image.shape)
    counts = uv_weights.reshape(uv_weights.shape[1:])
    dual = dual_coeffs.reshape(bases, channels, strip_rows, lanes)
    mask = support_mask.reshape(strip_rows, lanes)
    halo = 2 * margin
    top_rows, low_rows = dual[:, :, :halo], dual[:, :, strip_rows - halo :]
    if facet_rows == 1:
        ends = jnp.where(lax.axis_index("split") == 0, low_rows, top_rows)
        above = below = swapped(ends)
    else:
        above = along_chain(low_rows, 1, facet_rows)
        below = along_chain(top_rows, -1, facet_rows)
    other_image = swapped(image)
    other_counts = swapped(counts)
    other_dirty = swapped(dirty)
    if single:
        blocks = [all_adjoint(dual, above, below, row_taps, col_taps, facet_rows)]
        far = blocks
    else:
        adjoint = functools.partial(part_adjoint, dual, above, below, row_taps, col_taps)
        far = adjoint(tuple(range(count // 2, count)), facet_rows, row_taps)
        near = adjoint(tuple(range(count // 2)), facet_rows, far[0])
        blocks = [*near, *far]
    _, freq, kept, sent = spectrum(
        image, other_image, counts, other_counts, dual, above, below,
        row_taps, col_taps, (), margin, blocks[0],
    )
    arrived = crossed(blocks, single)
    got = swapped(sent)
    stepped, edges = gradient_step(
        kept, got, freq, image, other_image, dirty, other_dirty, margin
    )
    new_image, blocks = update_step(stepped, image, edges, arrived, margin, single)
    arrived = crossed(blocks, single)
    if single:
        new_dual = shrink_step(row_taps, col_taps, mask, dual, arrived, single)
    else:
        shrink = functools.partial(shrink_part, row_taps, col_taps, dual)
        middle = count // 2
        earlier = shrink(arrived[:middle], tuple(range(middle)))
        new_dual = shrink(arrived[middle:], tuple(range(middle, count)), (mask, *earlier))
    return (new_image.reshape(sky_image.shape), new_dual.reshape(dual_coeffs.shape))


def solution(mesh):
    placed = (
        P(("cube", "chan"), None, None, "split", None, None),
        P(("cube", "chan"), None, None, "split", None, None),
        P(("cube", "chan"), "split", None),
        P(None, "cube", "chan", "split", None, None),
        P("chan", "split", None, None),
        P(),
        P(),
    )

    mapped = jax.shard_map(
        per_device,
        mesh=mesh,
        in_specs=placed,
        out_specs=(
            P(("cube", "chan"), None, None, "split", None, None),
            P(None, "cube", "chan", "split", None, None),
        ),
        check_vma=False,
    )
    count = mesh.shape["chan"]
    if not in_parts(count):
        return mapped
    return mapped
```

```python
import functools
import math

import jax
import jax.numpy as jnp
import numpy as np
from jax import lax
from jax.experimental import pallas as pl
from jax.experimental.pallas import tpu as pltpu
from jax.sharding import PartitionSpec as P


LANES = 128
WIDE = 2 * LANES
BAND_ROWS = 224
primal_step = 0.5
dual_step = 0.5
radius = 6.0
weight_unit = 0.25

OWN_COPIES = pltpu.CompilerParams(vmem_limit_bytes=67043328)
SOME_ROOM = pltpu.CompilerParams(vmem_limit_bytes=41943040)


def held_inside(values):
    return [pltpu.with_memory_space_constraint(value, pltpu.VMEM) for value in values]


def held_outside(values):
    return [pltpu.with_memory_space_constraint(value, pltpu.HBM) for value in values]


def whole_block(shape):
    zeros = (0,) * len(shape)
    return pl.BlockSpec(tuple(shape), lambda *_: zeros)


def in_scalar_memory():
    return pl.BlockSpec(memory_space=pltpu.SMEM)


def exact_dot(left, right):
    return jnp.dot(left, right, preferred_element_type=jnp.float32)


def each(count, body):
    if count <= 8:
        for index in range(count):
            body(index)
    else:

        def step(index, carry):
            body(index)
            return carry

        lax.fori_loop(0, count, step, 0)


def hint(value, multiple):
    return value if isinstance(value, int) else pl.multiple_of(value, multiple)


def band_seed(taps, basis, positions):
    lane = lax.broadcasted_iota(jnp.int32, (8, WIDE), 1)
    row = lax.broadcasted_iota(jnp.int32, (8, WIDE), 0)
    offset = lane - row & WIDE - 1
    seed = jnp.zeros((8, WIDE), jnp.float32)
    for tap, position in enumerate(positions):
        seed = jnp.where(offset == position % WIDE, taps[basis, tap], seed)
    return seed


def fill_band(target, first_row, rows, seed):
    for start in range(0, rows, 16):
        upper = seed if start == 0 else pltpu.roll(seed, start, axis=1)
        lower = pltpu.roll(seed, start + 8, axis=1)
        target[first_row + start : first_row + start + 16, :] = jnp.concatenate(
            [upper, lower], axis=0
        ).astype(jnp.bfloat16)


def fill_col_bands(target, taps, bases, margin):
    for basis in range(bases):
        count = taps.shape[1]
        seed = band_seed(taps, basis, [tap - margin for tap in range(count)])
        fill_band(target, basis * LANES, LANES, seed)


def pack_height(rows):
    return -(-rows // (8 * 16)) * 16


def payload_rows(rows):
    return rows + pack_height(rows)


def row_groups(rows):
    height = pack_height(rows)
    return [(g, g * height, min(height, rows - g * height)) for g in range(-(-rows // height))]


def padded_rows(strip_rows):
    chunks = -(-strip_rows // BAND_ROWS)
    return (chunks - 1) * BAND_ROWS + WIDE


def edge_band_of(taps, basis, margin):
    halo = 2 * margin
    lane = lax.broadcasted_iota(jnp.int32, (halo, LANES), 1)
    row = lax.broadcasted_iota(jnp.int32, (halo, LANES), 0)
    source = jnp.where(
        row < margin,
        jnp.where(lane < 2 * halo, halo + row - lane, -1),
        jnp.where(lane >= 2 * halo, row + 3 * halo - lane, -1),
    )
    edge = jnp.zeros((halo, LANES), jnp.float32)
    for tap in range(taps.shape[1]):
        edge = jnp.where(source == tap, taps[basis, tap], edge)
    return edge


def products(far_re, far_im, near_re, near_im):
    return (
        (far_re * near_re - far_im * near_im).astype(jnp.bfloat16),
        (far_re * near_im + far_im * near_re).astype(jnp.bfloat16),
    )


def fill_transforms(seeds, cosine, sine, freq):
    big_re, big_im, small_re, small_im, even_re, even_im = seeds
    split = lax.axis_index("split")
    coarse = small_re.shape[0]
    half = cosine.shape[0]
    part = half // 2

    def even_rows(group, carry):
        at = pl.ds(pl.multiple_of(group * coarse, coarse), coarse)
        one = pl.ds(group, 1)
        cosine[at, :], sine[at, :] = products(
            even_re[one, :], even_im[one, :], even_re[half // coarse :, :], even_im[half // coarse :, :]
        )
        return carry

    lax.fori_loop(0, half // coarse, even_rows, 0)

    def freq_rows(group, carry):
        at = pl.ds(pl.multiple_of(group * coarse, coarse), coarse)
        one = pl.ds(group, 1)
        for place in range(2):
            side = jnp.where(split == place, 0, 1) * part
            lanes = pl.ds(pl.multiple_of(side, part), part)
            re, im = products(
                big_re[one, lanes], big_im[one, lanes], small_re[:, lanes], small_im[:, lanes]
            )
            freq[at, 2 * place * part : (2 * place + 1) * part] = re
            freq[at, (2 * place + 1) * part : (2 * place + 2) * part] = im
        return carry

    lax.fori_loop(0, 2 * half // coarse, freq_rows, 0)


def fill_adjoint_bands(row_taps, col_taps, row_band, edge_band, col_band, margin):
    bases, taps = row_taps.shape
    for basis in range(bases):
        seed = band_seed(row_taps, basis, [3 * margin - tap for tap in range(taps)])
        fill_band(row_band.at[basis], 0, BAND_ROWS, seed)
        edge_band[basis] = edge_band_of(row_taps, basis, margin).astype(jnp.bfloat16)
    fill_col_bands(col_band, col_taps, bases, margin)


def is_at_ends(facet_rows):
    split = lax.axis_index("split")
    facet_row = lax.rem(lax.axis_index("chan"), facet_rows)
    return (facet_row == 0) & (split == 0), (facet_row == facet_rows - 1) & (split == 1)


def adjoint_of(tall, bands, mixed, wide, strip_rows, margin):
    row_band, edge_band, col_band = bands
    bases = tall.shape[0]
    width = tall.shape[2] // LANES
    halo = 2 * margin
    for basis in range(bases):
        into = slice(basis * LANES, (basis + 1) * LANES)

        def put(first, count, value):
            for side in range(width):
                mixed[side, first : first + count, into] = value[
                    :, side * LANES : (side + 1) * LANES
                ].astype(jnp.bfloat16)

        for first in range(0, strip_rows, BAND_ROWS):
            count = min(BAND_ROWS, strip_rows - first)
            put(first, count, exact_dot(row_band[basis, :count], tall[basis, first : first + WIDE]))
        ends = jnp.concatenate(
            [
                tall[basis, : 2 * halo],
                tall[basis, strip_rows : strip_rows + 2 * halo],
                jnp.zeros((LANES - 4 * halo, width * LANES), jnp.bfloat16),
            ],
            axis=0,
        )
        put(strip_rows, halo, exact_dot(edge_band[basis], ends))
    for side in range(width):
        wide[side] = exact_dot(mixed[side], col_band[...])


def write_payload(out, wide, margin):
    rows = wide.shape[0]
    height = pack_height(rows)
    packed = jnp.zeros((height, LANES), jnp.float32)
    for group, first, count in row_groups(rows):
        out[first : first + count, :] = wide[first : first + count, :LANES].astype(jnp.bfloat16)
        piece = wide[first : first + count, LANES:]
        piece = pltpu.roll(piece, margin + 2 * margin * group, axis=1)
        if count < height:
            piece = jnp.concatenate(
                [piece, jnp.zeros((height - count, LANES), jnp.float32)], axis=0
            )
        packed = packed + piece
    out[rows : rows + height, :] = packed.astype(jnp.bfloat16)


def tall_height(strip_rows, margin):
    return max(padded_rows(strip_rows), strip_rows + 4 * margin)


def band_scratch(bases, margin):
    return [
        pltpu.VMEM((bases, BAND_ROWS, WIDE), jnp.bfloat16),
        pltpu.VMEM((bases, 2 * margin, LANES), jnp.bfloat16),
        pltpu.VMEM((bases * LANES, WIDE), jnp.bfloat16),
    ]


def all_adjoint_kernel(row_taps, col_taps, dual, above, below, out, *scratch, margin, facet_rows):
    bands, (tall, mixed, wide) = scratch[:3], scratch[3:]
    bases, width, strip_rows, _ = dual.shape
    halo = 2 * margin

    @pl.when(pl.program_id(0) == 0)
    def _():
        fill_adjoint_bands(row_taps, col_taps, *bands, margin)
        tall[...] = jnp.zeros(tall.shape, tall.dtype)

    is_top, is_low = is_at_ends(facet_rows)
    for basis in range(bases):
        for side in range(width):
            lanes = slice(side * LANES, (side + 1) * LANES)
            top = above[basis, side]
            low = below[basis, side]
            tall[basis, :halo, lanes] = jnp.where(is_top, jnp.zeros_like(top), top)
            tall[basis, halo : halo + strip_rows, lanes] = dual[basis, side]
            tall[basis, halo + strip_rows : 2 * halo + strip_rows, lanes] = jnp.where(
                is_low, jnp.zeros_like(low), low
            )
    adjoint_of(tall, bands, mixed, wide, strip_rows, margin)
    for side in range(width):
        write_payload(out.at[side], wide.at[side], margin)


def all_adjoint(dual, above, below, row_taps, col_taps, facet_rows):
    bases, count, strip_rows, _ = dual.shape
    margin = row_taps.shape[1] // 2
    width = 2 if count % 2 == 0 else 1
    rows = strip_rows + 2 * margin

    def picked(height):
        return pl.BlockSpec((bases, width, height, LANES), lambda j: (0, j, 0, 0))

    return pl.pallas_call(
        functools.partial(all_adjoint_kernel, margin=margin, facet_rows=facet_rows),
        out_shape=jax.ShapeDtypeStruct((count, payload_rows(rows), LANES), jnp.bfloat16),
        grid=(count // width,),
        in_specs=[in_scalar_memory()] * 2
        + [picked(height) for height in (strip_rows, 2 * margin, 2 * margin)],
        out_specs=pl.BlockSpec((width, payload_rows(rows), LANES), lambda j: (j, 0, 0)),
        scratch_shapes=band_scratch(bases, margin)
        + [
            pltpu.VMEM((bases, tall_height(strip_rows, margin), width * LANES), jnp.bfloat16),
            pltpu.VMEM((width, rows, bases * LANES), jnp.bfloat16),
            pltpu.VMEM((width, rows, WIDE), jnp.float32),
        ],
        name="all_adjoint",
    )(row_taps, col_taps, dual, above, below)


def part_scratch(bases, strip_rows, margin, count):
    rows = strip_rows + 2 * margin
    height = tall_height(strip_rows, margin)
    return band_scratch(bases, margin) + [
        pltpu.VMEM((-(-count // 2), bases, height, 2 * LANES), jnp.bfloat16),
        pltpu.VMEM((2, rows, bases * LANES), jnp.bfloat16),
        pltpu.VMEM((2, rows, WIDE), jnp.float32),
        pltpu.SemaphoreType.DMA((count,)),
    ]


class PartAdjoint:
    def __init__(self, places, dual, above, below, outs, scratch, facet_rows):
        *self.bands, self.tall, self.mixed, self.wide, loads = scratch
        self.places, self.outs = places, outs
        self.strip_rows = dual.shape[2]
        self.halo = above.shape[2]
        self.margin = self.halo // 2
        self.ends = is_at_ends(facet_rows)
        me = lax.axis_index("chan")
        self.above, self.below = above, below
        self.copies = []
        for at, place in enumerate(places):
            lanes = pl.ds(at % 2 * LANES, LANES)
            self.copies.append(
                pltpu.make_async_copy(
                    dual.at[:, me ^ place],
                    self.tall.at[at // 2, :, pl.ds(self.halo, self.strip_rows), lanes],
                    loads.at[at],
                )
            )

    def start(self):
        for copy in self.copies:
            copy.start()

    def fill(self, row_taps, col_taps):
        fill_adjoint_bands(row_taps, col_taps, *self.bands, self.margin)
        used = self.strip_rows + 2 * self.halo
        pairs, bases, height, lanes = self.tall.shape
        is_top, is_low = self.ends
        me = lax.axis_index("chan")
        for at, place in enumerate(self.places):
            mine = slice(at % 2 * LANES, (at % 2 + 1) * LANES)
            for basis in range(bases):
                top = self.above[basis, me ^ place]
                low = self.below[basis, me ^ place]
                self.tall[at // 2, basis, : self.halo, mine] = jnp.where(
                    is_top, jnp.zeros_like(top), top
                )
                self.tall[at // 2, basis, used - self.halo : used, mine] = jnp.where(
                    is_low, jnp.zeros_like(low), low
                )
        if used < height:
            blank = jnp.zeros((height - used, lanes), jnp.bfloat16)
            for pair in range(pairs):
                for basis in range(bases):
                    self.tall[pair, basis, used:] = blank

    def run(self):
        strip_rows = self.strip_rows
        for pair in range(len(self.places) // 2):
            for copy in self.copies[2 * pair : 2 * pair + 2]:
                copy.wait()
            adjoint_of(
                self.tall.at[pair], self.bands, self.mixed, self.wide, strip_rows, self.margin
            )
            for side in range(2):
                at = 2 * pair + side
                write_payload(self.outs[at], self.wide.at[side], self.margin)


def part_adjoint_kernel(row_taps, col_taps, dual, above, below, _, *rest, places, facet_rows):
    count = len(places)
    part = PartAdjoint(places, dual, above, below, rest[:count], rest[count:], facet_rows)
    part.start()
    part.fill(row_taps, col_taps)
    part.run()


def part_adjoint(dual, above, below, row_taps, col_taps, places, facet_rows, after):
    bases, _, strip_rows, _ = dual.shape
    margin = row_taps.shape[1] // 2
    anywhere = pl.BlockSpec(memory_space=pltpu.HBM)
    rows = payload_rows(strip_rows + 2 * margin)
    return pl.pallas_call(
        functools.partial(part_adjoint_kernel, places=places, facet_rows=facet_rows),
        out_shape=[pltpu.VMEM((rows, LANES), jnp.bfloat16)] * len(places),
        in_specs=[in_scalar_memory()] * 2
        + [anywhere]
        + [pl.BlockSpec(memory_space=pltpu.VMEM)] * 2
        + [pl.BlockSpec(memory_space=pl.ANY)],
        out_specs=[pl.BlockSpec(memory_space=pltpu.VMEM)] * len(places),
        scratch_shapes=part_scratch(bases, strip_rows, margin, len(places)),
        compiler_params=SOME_ROOM,
        name="part_adjoint",
    )(*held_outside((row_taps, col_taps, dual)), *held_inside((above, below)), after)


def phase_seeds(pixels):
    step = 2.0 * math.pi / pixels
    coarse = 32
    half = pixels // 2
    scale = 1.0 / math.sqrt(pixels)
    where = np.arange(half)

    def of(rows, factor):
        angle = rows[:, None] * where[None, :] % pixels * step
        return np.cos(angle) * factor, -np.sin(angle) * factor

    big = of(np.arange(pixels // coarse) * coarse, 1.0)
    small = of(np.arange(coarse), scale)
    far = of(np.arange(half // coarse) * coarse * 2, 1.0)
    near = of(np.arange(coarse) * 2, scale)
    even = tuple(np.concatenate([x, y], axis=0) for x, y in zip(far, near))
    return tuple(np.asarray(v, np.float32) for v in (*big, *small, *even))


def twiddles(pixels):
    angle = 2.0 * math.pi / pixels * np.arange(pixels // 2)[:, None] * np.ones((1, LANES))
    return tuple(np.asarray(v, np.float32) for v in (np.cos(angle), -np.sin(angle)))


def spectrum_kernel(
    own, other, own_counts, other_counts, *rest, margin
):
    seeds, (turn_from_re, turn_from_im, _) = rest[:6], rest[6:9]
    freq, keep, send = rest[9:12]
    picture, counts, cosine, sine, turn_re, turn_im, top, low, whole, wide, loads = rest[12:]
    split = lax.axis_index("split")
    cols, facet_rows, strip_rows, _ = own.shape
    pixels = picture.shape[0]
    half = pixels // 2
    part = half // 2

    def strip_at(facet_row, which):
        return pl.multiple_of((2 * facet_row + which) * strip_rows, strip_rows)

    copies = []
    for facet_row in range(facet_rows):
        for col in range(cols):
            lanes = pl.ds(col * LANES, LANES)
            copies.append(
                pltpu.make_async_copy(
                    own.at[col, facet_row],
                    picture.at[pl.ds(strip_at(facet_row, split), strip_rows), lanes],
                    loads.at[len(copies)],
                )
            )
    for source, target in ((turn_from_re, turn_re), (turn_from_im, turn_im)):
        copies.append(pltpu.make_async_copy(source, target, loads.at[len(copies)]))
    count_copies = []
    for tile in range(part // LANES):
        lanes = pl.ds(pl.multiple_of(split * part + tile * LANES, LANES), LANES)
        count_copies.append(
            pltpu.make_async_copy(
                own_counts.at[:, lanes],
                counts.at[tile, pl.ds(pl.multiple_of(split * half, half), half), :],
                loads.at[len(copies) + len(count_copies)],
            )
        )
    for copy in (*copies, *count_copies):
        copy.start()
    fill_transforms(seeds, cosine, sine, freq)
    for facet_row in range(facet_rows):
        there = pl.ds(strip_at(facet_row, 1 - split), strip_rows)
        for col in range(cols):
            picture[there, col * LANES : (col + 1) * LANES] = other[col, facet_row]
    for tile in range(part // LANES):
        lanes = pl.ds(pl.multiple_of(split * part + tile * LANES, LANES), LANES)
        there = pl.ds(pl.multiple_of((1 - split) * half, half), half)
        counts[tile, there, :] = other_counts[:, lanes]
    for copy in copies:
        copy.wait()
    block = min(256, half)
    first_table = freq.at[:, pl.ds(0, half)]

    def first(step, carry):
        at = pl.ds(pl.multiple_of(step * block, block), block)
        beyond = pl.ds(pl.multiple_of(half + step * block, block), block)
        one = exact_dot(picture[at, :], first_table[...])
        two = exact_dot(picture[beyond, :], first_table[...])
        total = one + two
        apart = one - two
        re, im = apart[:, :part], apart[:, part:]
        turn_r = jnp.concatenate([turn_re[at, :]] * (part // LANES), axis=1)
        turn_i = jnp.concatenate([turn_im[at, :]] * (part // LANES), axis=1)
        odd_re = (re * turn_r - im * turn_i).astype(jnp.bfloat16)
        odd_im = (re * turn_i + im * turn_r).astype(jnp.bfloat16)
        sum_re = total[:, :part].astype(jnp.bfloat16)
        sum_im = total[:, part:].astype(jnp.bfloat16)
        for place, value in enumerate((sum_re, sum_im, odd_re, odd_im)):
            top[at, place * part : (place + 1) * part] = value
        for place, value in enumerate((-sum_im, sum_re, -odd_im, odd_re)):
            low[at, place * part : (place + 1) * part] = value
        return carry

    lax.fori_loop(0, half // block, first, 0)
    for copy in count_copies:
        copy.wait()

    def second(step, carry):
        at = pl.ds(pl.multiple_of(step * block, block), block)
        vis = exact_dot(cosine[at, :], top[...]) + exact_dot(sine[at, :], low[...])
        for parity in range(2):
            picked = jnp.concatenate(
                [
                    counts.at[tile][pl.ds(2 * step * block + parity, block, stride=2), :]
                    for tile in range(part // LANES)
                ],
                axis=1,
            )
            scale = weight_unit * picked.astype(jnp.float32)
            re = parity * 2 * part
            im = re + part
            whole[at, re : re + part] = (vis[:, re : re + part] * scale).astype(jnp.bfloat16)
            whole[at, im : im + part] = (vis[:, im : im + part] * scale).astype(jnp.bfloat16)
        return carry

    lax.fori_loop(0, half // block, second, 0)
    for parity in range(2):
        re = slice(parity * 2 * part, (parity * 2 + 1) * part)
        im = slice((parity * 2 + 1) * part, (parity * 2 + 2) * part)
        low[:, re] = whole[:, im]
        low[:, im] = -whole[:, re]

    def third(step, carry):
        at = pl.ds(pl.multiple_of(step * block, block), block)
        beyond = pl.ds(pl.multiple_of(half + step * block, block), block)
        value = exact_dot(cosine[at, :], whole[...]) + exact_dot(sine[at, :], low[...])
        even, re, im = value[:, :half], value[:, half : half + part], value[:, half + part :]
        turn_r = jnp.concatenate([turn_re[at, :]] * (part // LANES), axis=1)
        turn_i = jnp.concatenate([turn_im[at, :]] * (part // LANES), axis=1)
        odd = jnp.concatenate([re * turn_r + im * turn_i, im * turn_r - re * turn_i], axis=1)
        wide[at, :] = (even + odd).astype(jnp.bfloat16)
        wide[beyond, :] = (even - odd).astype(jnp.bfloat16)
        return carry

    lax.fori_loop(0, half // block, third, 0)
    rows = strip_rows + 2 * margin
    for facet_row in range(facet_rows):
        for target, which in ((keep, split), (send, 1 - split)):
            at = strip_at(facet_row, which)
            base = facet_row * rows
            target[base : base + strip_rows, :] = wide[pl.ds(at, strip_rows), :]
            before = pl.multiple_of(lax.rem(at + pixels - 16, pixels), 16)
            after = pl.multiple_of(lax.rem(at + strip_rows, pixels), 16)
            ends = jnp.concatenate(
                [
                    wide[pl.ds(before, 16), :].astype(jnp.float32)[16 - margin :],
                    wide[pl.ds(after, 16), :].astype(jnp.float32)[:margin],
                ],
                axis=0,
            )
            target[base + strip_rows : base + rows, :] = ends.astype(jnp.bfloat16)


def spectrum(own, other, own_counts, other_counts, margin, after):
    cols, facet_rows, strip_rows, lanes = own.shape
    pixels = cols * lanes
    half = pixels // 2
    rows = facet_rows * (strip_rows + 2 * margin)
    anywhere = pl.BlockSpec(memory_space=pltpu.HBM)
    inside = pl.BlockSpec(memory_space=pltpu.VMEM)
    return pl.pallas_call(
        functools.partial(spectrum_kernel, margin=margin),
        out_shape=[
            pltpu.VMEM((pixels, pixels), jnp.bfloat16),
            pltpu.VMEM((rows, half), jnp.bfloat16),
            pltpu.VMEM((rows, half), jnp.bfloat16),
        ],
        in_specs=[anywhere, inside] * 2
        + [inside] * 6
        + [anywhere] * 2
        + [pl.BlockSpec(memory_space=pl.ANY)],
        out_specs=[inside] * 3,
        scratch_shapes=[
            pltpu.VMEM((pixels, pixels), jnp.bfloat16),
            pltpu.VMEM((half // 2 // LANES, pixels, LANES), jnp.int32),
            pltpu.VMEM((half, half), jnp.bfloat16),
            pltpu.VMEM((half, half), jnp.bfloat16),
            pltpu.VMEM((half, LANES), jnp.float32),
            pltpu.VMEM((half, LANES), jnp.float32),
            pltpu.VMEM((half, pixels), jnp.bfloat16),
            pltpu.VMEM((half, pixels), jnp.bfloat16),
            pltpu.VMEM((half, pixels), jnp.bfloat16),
            pltpu.VMEM((pixels, half), jnp.bfloat16),
            pltpu.SemaphoreType.DMA((cols * facet_rows + 2 + half // LANES,)),
        ],
        compiler_params=SOME_ROOM,
        name="spectrum",
    )(
        *held_outside((own,)), *held_inside((other,)),
        *held_outside((own_counts,)), *held_inside((other_counts,)),
        *phase_seeds(pixels), *twiddles(pixels), after,
    )


def gradient_kernel(
    kept, got, freq, own_from, other, dirty_from, other_dirty, stepped, edge_out, own,
    joined, dirty, loads, *, margin
):
    split = lax.axis_index("split")
    cols, facet_rows, strip_rows, _ = own.shape
    half = kept.shape[1]
    rows = strip_rows + 2 * margin
    pair = 2 if cols % 2 == 0 else 1
    started = []

    def load(source, target):
        copy = pltpu.make_async_copy(source, target, loads.at[len(started)])
        copy.start()
        started.append(copy)
        return copy

    steps = []
    for step in range(cols // pair):
        some = pl.ds(step * pair, pair)
        steps.append(
            [
                load(own_from.at[some], own.at[some]),
                load(dirty_from.at[some], dirty.at[some]),
            ]
        )

    def edges(source, col, facet_row):
        over = jnp.maximum(facet_row - 1 + split, 0)
        under = jnp.minimum(facet_row + split, facet_rows - 1)
        return jnp.concatenate(
            [
                source[col, over, strip_rows - 16 :].astype(jnp.float32)[16 - margin :],
                source[col, under, :16].astype(jnp.float32)[:margin],
            ],
            axis=0,
        )

    joined[:, :half] = kept[...]
    joined[:, half:] = got[...]
    for step in range(cols // pair):
        for copy in steps[step]:
            copy.wait()
        value = lax.dot_general(
            joined[...],
            freq[step * pair * LANES : (step + 1) * pair * LANES, :],
            (((1,), (1,)), ((), ())),
            preferred_element_type=jnp.float32,
        )
        for side in range(pair):
            col = step * pair + side
            for facet_row in range(facet_rows):
                base = facet_row * rows
                grad = value[base : base + rows, side * LANES : (side + 1) * LANES]
                moved = own[col, facet_row].astype(jnp.float32) - primal_step * (
                    grad[:strip_rows] - dirty[col, facet_row].astype(jnp.float32)
                )
                stepped[col, facet_row, :strip_rows] = moved.astype(jnp.bfloat16)
                image = edges(other, col, facet_row)
                moved = image - primal_step * (
                    grad[strip_rows:] - edges(other_dirty, col, facet_row)
                )
                stepped[col, facet_row, strip_rows:] = moved.astype(jnp.bfloat16)
                edge_out[col, facet_row] = image.astype(jnp.bfloat16)


def gradient_step(kept, got, freq, own, other, own_dirty, other_dirty, margin):
    cols, facet_rows, strip_rows, lanes = own.shape
    pixels = cols * lanes
    rows = strip_rows + 2 * margin
    anywhere = pl.BlockSpec(memory_space=pltpu.HBM)
    inside = pl.BlockSpec(memory_space=pltpu.VMEM)
    return pl.pallas_call(
        functools.partial(gradient_kernel, margin=margin),
        out_shape=[
            pltpu.VMEM((cols, facet_rows, rows, lanes), jnp.bfloat16),
            pltpu.VMEM((cols, facet_rows, 2 * margin, lanes), jnp.bfloat16),
            pltpu.VMEM(own.shape, jnp.bfloat16),
        ],
        in_specs=[inside] * 3 + [anywhere, inside] * 2,
        out_specs=[inside] * 3,
        scratch_shapes=[
            pltpu.VMEM((kept.shape[0], pixels), jnp.bfloat16),
            pltpu.VMEM(own.shape, jnp.bfloat16),
            pltpu.SemaphoreType.DMA((2 * cols,)),
        ],
        compiler_params=SOME_ROOM,
        name="gradient",
    )(
        *held_inside((kept, got, freq)), *held_outside((own,)), *held_inside((other,)),
        *held_outside((own_dirty,)), *held_inside((other_dirty,)),
    )


def unpacked(packed, group, count, margin):
    return pltpu.roll(
        packed[:count], LANES - (margin + 2 * margin * group) % LANES, axis=1
    )


def update_kernel(stepped, edges, image, *rest, margin, facets, single):
    arrivals = 1 if single else facets
    blocks = rest[:arrivals]
    new_out = rest[arrivals]
    outs = rest[arrivals + 1 : 2 * arrivals + 1]
    new_image, adjoint, apart, extrapolated, stores = rest[2 * arrivals + 1 :]
    me = lax.axis_index("chan")
    split = lax.axis_index("split")
    cols, facet_rows, rows, _ = stepped.shape
    strip_rows = rows - 2 * margin
    height = pack_height(rows)
    lane = lax.broadcasted_iota(jnp.int32, (1, LANES), 1)

    def unpack(facet):
        tile = adjoint[facet, rows : rows + height, :].astype(jnp.float32)
        for group, first, count in row_groups(rows):
            apart[facet, first : first + count, :] = unpacked(
                tile, group, count, margin
            ).astype(jnp.bfloat16)

    if single:
        adjoint = blocks[0]
        each(facets, unpack)
    else:
        for place, block in enumerate(blocks):
            adjoint[me ^ place] = block[...]
            unpack(me ^ place)

    def sides(take, group, count, left, has_left, right, has_right):
        from_left = take(left, group, count)
        from_right = take(right, group, count)
        return (
            jnp.where(lane < jnp.where(has_left, margin, 0), from_left, 0.0),
            jnp.where(lane >= jnp.where(has_right, LANES - margin, LANES), from_right, 0.0),
        )

    def apart_of(facet, group, count):
        first = group * height
        return apart[facet, first : first + count, :].astype(jnp.float32)

    def update(facet):
        col = facet // facet_rows
        facet_row = facet % facet_rows
        left, has_left = jnp.maximum(facet - facet_rows, 0), facet >= facet_rows
        right, has_right = jnp.minimum(facet + facet_rows, facets - 1), facet < facets - facet_rows
        for group, first, count in row_groups(rows):
            add_left, add_right = sides(apart_of, group, count, left, has_left, right, has_right)
            at = slice(first, first + count)
            total = adjoint[facet, at, :].astype(jnp.float32) + add_left + add_right
            value = stepped[col, facet_row, at, :].astype(jnp.float32) - primal_step * total
            value = jnp.maximum(value, 0.0).astype(jnp.bfloat16).astype(jnp.float32)
            main = max(min(first + count, strip_rows) - first, 0)
            before = []
            if main > 0:
                before.append(image[col, facet_row, first : first + main, :].astype(jnp.float32))
            if main < count:
                after = first + main - strip_rows
                before.append(
                    edges[col, facet_row, after : after + count - main, :].astype(jnp.float32)
                )
            ahead = 2.0 * value - (before[0] if len(before) == 1 else jnp.concatenate(before, 0))
            if first + count > strip_rows:
                row = first + lax.broadcasted_iota(jnp.int32, (count, LANES), 0)
                top_there = (facet_row > 0) | (split > 0)
                low_there = (facet_row < facet_rows - 1) | (split < 1)
                middle = strip_rows + margin
                from_top = jnp.where(top_there, middle, strip_rows)
                to_low = jnp.where(low_there, rows, middle)
                ahead = jnp.where((row >= from_top) & (row < middle), 0.0, ahead)
                ahead = jnp.where(row >= to_low, 0.0, ahead)
            extrapolated[facet, at, :] = ahead.astype(jnp.bfloat16)
            if main > 0:
                new_image[col, facet_row, first : first + main, :] = value[:main].astype(jnp.bfloat16)

    stored = []
    for col in range(cols):
        for facet_row in range(facet_rows):
            update(col * facet_rows + facet_row)
        stored.append(
            pltpu.make_async_copy(new_image.at[col], new_out.at[col], stores.at[col])
        )
        stored[-1].start()

    def whole_of(facet, group, count):
        first = group * height
        return extrapolated[facet, first : first + count, :].astype(jnp.float32)

    def write(out, facet):
        left, has_left = jnp.maximum(facet - facet_rows, 0), facet >= facet_rows
        right, has_right = jnp.minimum(facet + facet_rows, facets - 1), facet < facets - facet_rows
        packed = jnp.zeros((height, LANES), jnp.float32)
        for group, first, count in row_groups(rows):
            after, before = sides(whole_of, group, count, right, has_right, left, has_left)
            side = pltpu.roll(after + before, margin + 2 * margin * group, axis=1)
            if count < height:
                side = jnp.concatenate(
                    [side, jnp.zeros((height - count, LANES), jnp.float32)], axis=0
                )
            packed = packed + side
        out[:rows, :] = extrapolated[facet]
        out[rows:, :] = packed.astype(jnp.bfloat16)

    if single:
        each(facets, lambda facet: write(outs[0].at[facet], facet))
    else:
        for place, out in enumerate(outs):
            write(out, me ^ place)
    for copy in stored:
        copy.wait()


def update_step(stepped, edges, image, blocks, margin, single):
    cols, facet_rows, rows, lanes = stepped.shape
    facets = cols * facet_rows
    tall_rows = payload_rows(rows)
    arrivals = (
        [pltpu.VMEM((facets, tall_rows, lanes), jnp.bfloat16)]
        if single
        else [pltpu.VMEM((tall_rows, lanes), jnp.bfloat16)] * facets
    )
    anywhere = pl.BlockSpec(memory_space=pltpu.HBM)
    results = pl.pallas_call(
        functools.partial(update_kernel, margin=margin, facets=facets, single=single),
        out_shape=[
            jax.ShapeDtypeStruct((cols, facet_rows, rows - 2 * margin, lanes), jnp.bfloat16)
        ]
        + arrivals,
        in_specs=[pl.BlockSpec(memory_space=pltpu.VMEM)] * (3 + len(blocks)),
        out_specs=[anywhere] + [pl.BlockSpec(memory_space=pltpu.VMEM)] * len(arrivals),
        scratch_shapes=[
            pltpu.VMEM(image.shape, jnp.bfloat16),
            pltpu.VMEM((1, 16, lanes) if single else (facets, tall_rows, lanes), jnp.bfloat16),
            pltpu.VMEM((facets, rows, lanes), jnp.bfloat16),
            pltpu.VMEM((facets, rows, lanes), jnp.bfloat16),
            pltpu.SemaphoreType.DMA((cols,)),
        ],
        compiler_params=SOME_ROOM,
        name="update",
    )(*held_inside((stepped, edges, image, *blocks)))
    return results[0], results[1:]


def shrink_kernel(row_taps, col_taps, mask, dual, *rest, margin, channels, single):
    arrivals = 1 if single else channels
    blocks = rest[:arrivals]
    out = rest[arrivals]
    row_band, col_band, wide, tall = rest[arrivals + 1 :]
    me = lax.axis_index("chan")
    basis = pl.program_id(0)
    taps = row_taps.shape[1]
    halo = 2 * margin
    strip_rows = dual.shape[2]
    rows = strip_rows + halo
    height = pack_height(rows)

    @pl.when(basis == 0)
    def _():
        for each_basis in range(row_taps.shape[0]):
            seed = band_seed(row_taps, each_basis, [margin + tap for tap in range(taps)])
            fill_band(row_band.at[each_basis], 0, BAND_ROWS, seed)
            seed = band_seed(col_taps, each_basis, [tap - margin for tap in range(taps)])
            fill_band(col_band.at[each_basis], 0, LANES, seed)
        tall[...] = jnp.zeros(tall.shape, tall.dtype)

        def unpack(channel, block):
            wide[channel, :, :LANES] = block[:rows, :]
            packed = block[rows : rows + height, :].astype(jnp.float32)
            for group, first, count in row_groups(rows):
                side = unpacked(packed, group, count, margin)
                wide[channel, first : first + count, LANES:] = side.astype(jnp.bfloat16)

        if single:
            each(channels, lambda channel: unpack(channel, blocks[0].at[channel]))
        else:
            for place, block in enumerate(blocks):
                unpack(me ^ place, block)

    def columns(channel):
        lanes = pl.ds(hint(channel * LANES, LANES), LANES)
        value = lax.dot_general(
            wide[channel], col_band[basis], (((1,), (1,)), ((), ())),
            preferred_element_type=jnp.float32,
        )
        blank = jnp.zeros((halo - margin, LANES), jnp.float32)
        tall[halo : halo + strip_rows, lanes] = value[:strip_rows].astype(jnp.bfloat16)
        tall[:halo, lanes] = jnp.concatenate(
            [blank, value[strip_rows : strip_rows + margin]], axis=0
        ).astype(jnp.bfloat16)
        tall[halo + strip_rows : 2 * halo + strip_rows, lanes] = jnp.concatenate(
            [value[strip_rows + margin :], blank], axis=0
        ).astype(jnp.bfloat16)

    each(channels, columns)
    piece = min(channels, 8)
    for first in range(0, strip_rows, BAND_ROWS):
        count = min(BAND_ROWS, strip_rows - first)
        stepped = []
        total = jnp.zeros((count, LANES), jnp.float32)
        for channel in range(0, channels, piece):
            value = exact_dot(
                row_band[basis, :count],
                tall[first : first + WIDE, channel * LANES : (channel + piece) * LANES],
            )
            for side in range(piece):
                coefficient = value[:, side * LANES : (side + 1) * LANES]
                moved = (
                    dual[0, channel + side, first : first + count].astype(jnp.float32)
                    + dual_step * coefficient
                )
                stepped.append(moved)
                total = total + moved * moved
        kept = mask[first : first + count].astype(jnp.float32)
        shrink = radius * kept / jnp.maximum(jnp.sqrt(total), radius)
        for channel in range(channels):
            out[0, channel, first : first + count] = (stepped[channel] * shrink).astype(jnp.bfloat16)


def shrink_step(row_taps, col_taps, mask, dual, blocks, single):
    bases, channels, strip_rows, lanes = dual.shape
    margin = row_taps.shape[1] // 2
    rows = strip_rows + 2 * margin
    return pl.pallas_call(
        functools.partial(shrink_kernel, margin=margin, channels=channels, single=single),
        out_shape=jax.ShapeDtypeStruct(dual.shape, jnp.bfloat16),
        grid=(bases,),
        in_specs=[
            in_scalar_memory(),
            in_scalar_memory(),
            whole_block(mask.shape),
            pl.BlockSpec((1, channels, strip_rows, lanes), lambda n: (n, 0, 0, 0)),
        ]
        + [whole_block(block.shape) for block in blocks],
        out_specs=pl.BlockSpec((1, channels, strip_rows, lanes), lambda n: (n, 0, 0, 0)),
        scratch_shapes=[
            pltpu.VMEM((bases, BAND_ROWS, WIDE), jnp.bfloat16),
            pltpu.VMEM((bases, LANES, WIDE), jnp.bfloat16),
            pltpu.VMEM((channels, rows, WIDE), jnp.bfloat16),
            pltpu.VMEM((max(padded_rows(strip_rows), strip_rows + 4 * margin), channels * lanes), jnp.bfloat16),
        ],
        name="shrink",
    )(row_taps, col_taps, mask, dual, *blocks)


def shrink_part_kernel(row_taps, col_taps, dual, *rest, places, margin, final):
    count = len(places)
    blocks, rest = rest[:count], rest[count:]
    if final:
        mask, before, total, field, out_to = rest[:5]
        row_band, col_band, wide, tall, held, scaled, loads, stores = rest[5:]
    else:
        held, total, ahead = rest[:3]
        row_band, col_band, wide, tall, field, loads, stores = rest[3:]
    me = lax.axis_index("chan")
    bases, taps = row_taps.shape
    halo = 2 * margin
    strip_rows = dual.shape[2]
    rows = strip_rows + halo
    height = pack_height(rows)
    started = []

    def load(source, target):
        copy = pltpu.make_async_copy(source, target, loads.at[len(started)])
        copy.start()
        started.append(copy)
        return copy

    stored = []

    def store(source, target):
        copy = pltpu.make_async_copy(source, target, stores.at[len(stored)])
        copy.start()
        stored.append(copy)

    fields = []
    for basis in range(0 if final else bases):
        fields.append(
            [
                load(dual.at[basis, me ^ place], field.at[basis, at])
                for at, place in enumerate(places)
            ]
        )
    further = []
    for basis in range(0 if final else bases):
        for at, place in enumerate(places):
            further.append(load(dual.at[basis, me ^ place ^ count], ahead.at[basis, at]))
    for basis in range(bases):
        seed = band_seed(row_taps, basis, [margin + tap for tap in range(taps)])
        fill_band(row_band.at[basis], 0, BAND_ROWS, seed)
        used = strip_rows + 2 * halo
        if used < tall.shape[1]:
            tall[basis, used:] = jnp.zeros((tall.shape[1] - used, tall.shape[2]), jnp.bfloat16)
    fill_col_bands(col_band, col_taps, bases, margin)
    for at in range(count):
        block = blocks[at]
        wide[at, :, :LANES] = block[:rows, :]
        packed = block[rows : rows + height, :].astype(jnp.float32)
        for group, first, some in row_groups(rows):
            side = unpacked(packed, group, some, margin)
            wide[at, first : first + some, LANES:] = side.astype(jnp.bfloat16)
        value = lax.dot_general(
            wide[at], col_band[...], (((1,), (1,)), ((), ())), preferred_element_type=jnp.float32
        )
        blank = jnp.zeros((halo - margin, LANES), jnp.float32)
        lanes = slice(at * LANES, (at + 1) * LANES)
        for basis in range(bases):
            mine = value[:, basis * LANES : (basis + 1) * LANES]
            tall[basis, halo : halo + strip_rows, lanes] = mine[:strip_rows].astype(jnp.bfloat16)
            tall[basis, :halo, lanes] = jnp.concatenate(
                [blank, mine[strip_rows : strip_rows + margin]], axis=0
            ).astype(jnp.bfloat16)
            tall[basis, halo + strip_rows : 2 * halo + strip_rows, lanes] = jnp.concatenate(
                [mine[strip_rows + margin :], blank], axis=0
            ).astype(jnp.bfloat16)
    for basis in range(bases):
        if not final:
            for copy in fields[basis]:
                copy.wait()
        for first in range(0, strip_rows, BAND_ROWS):
            some = min(BAND_ROWS, strip_rows - first)
            here = slice(first, first + some)
            value = exact_dot(row_band[basis, :some], tall[basis, first : first + WIDE])
            if final:
                squares = total[basis, here]
            else:
                squares = jnp.zeros((some, LANES), jnp.float32)
            stepped = []
            for at in range(count):
                moved = (
                    field[basis, at, here].astype(jnp.float32)
                    + dual_step * value[:, at * LANES : (at + 1) * LANES]
                )
                stepped.append(moved)
                squares = squares + moved * moved
            if final:
                kept = mask[here].astype(jnp.float32)
                scale = radius * kept / jnp.maximum(jnp.sqrt(squares), radius)
                for at in range(count):
                    held[basis, at, here] = (stepped[at] * scale).astype(jnp.bfloat16)
                    earlier = before[basis, at, here].astype(jnp.float32)
                    scaled[basis, at, here] = (earlier * scale).astype(jnp.bfloat16)
            else:
                total[basis, here] = squares
                for at in range(count):
                    held[basis, at, here] = stepped[at].astype(jnp.bfloat16)
        if final:
            for at, place in enumerate(places):
                store(held.at[basis, at], out_to.at[basis, me ^ place])
                store(scaled.at[basis, at], out_to.at[basis, me ^ place ^ count])
    for copy in (*stored, *further):
        copy.wait()


def shrink_part(row_taps, col_taps, dual, blocks, places, earlier=None):
    bases, _, strip_rows, lanes = dual.shape
    count = len(places)
    margin = row_taps.shape[1] // 2
    rows = strip_rows + 2 * margin
    anywhere = pl.BlockSpec(memory_space=pltpu.HBM)
    part = (bases, count, strip_rows, lanes)
    final = earlier is not None
    inside = pl.BlockSpec(memory_space=pltpu.VMEM)
    bands = [
        pltpu.VMEM((bases, BAND_ROWS, WIDE), jnp.bfloat16),
        pltpu.VMEM((bases * LANES, WIDE), jnp.bfloat16),
        pltpu.VMEM((count, rows, WIDE), jnp.bfloat16),
        pltpu.VMEM((bases, tall_height(strip_rows, margin), count * lanes), jnp.bfloat16),
    ]
    field = pltpu.VMEM(part, jnp.bfloat16)
    if final:
        out_shape = jax.ShapeDtypeStruct(dual.shape, jnp.bfloat16)
        out_specs = anywhere
        scratch = [field, field]
    else:
        earlier = ()
        out_shape = [field, pltpu.VMEM((bases, strip_rows, lanes), jnp.float32), field]
        out_specs = [inside] * 3
        scratch = [field]
    return pl.pallas_call(
        functools.partial(shrink_part_kernel, places=places, margin=margin, final=final),
        out_shape=out_shape,
        in_specs=[in_scalar_memory()] * 2 + [anywhere] + [inside] * (count + len(earlier)),
        out_specs=out_specs,
        scratch_shapes=bands
        + scratch
        + [
            pltpu.SemaphoreType.DMA((2 * bases * count,)),
            pltpu.SemaphoreType.DMA((2 * bases * count,)),
        ],
        compiler_params=SOME_ROOM,
        name="shrink_part",
    )(
        *held_outside((row_taps, col_taps, dual)),
        *held_inside((*blocks, *earlier)),
    )


def swapped(value):
    return lax.ppermute(value, "split", [(0, 1), (1, 0)])


def along_chain(value, by, facet_rows):
    count = lax.axis_size("chan") * 2
    chain = 2 * facet_rows
    pairs = [
        (i, i + by) for i in range(count) if 0 <= i + by < count and i // chain == (i + by) // chain
    ]
    return lax.ppermute(value, ("chan", "split"), pairs)


def crossed(blocks, single):
    count = lax.axis_size("chan")
    if single:
        return [lax.all_to_all(blocks[0], "chan", split_axis=0, concat_axis=0, tiled=True)]
    result = list(blocks)
    for place in reversed(range(1, count)):
        result[place] = lax.ppermute(blocks[place], "chan", [(i, i ^ place) for i in range(count)])
    return result


def in_parts(count):
    return 4 <= count <= 8 and count & count - 1 == 0


def per_device(sky_image, dirty_image, uv_weights, dual_coeffs, support_mask, row_taps, col_taps):
    facet_cols, facet_rows, strip_rows, lanes = (sky_image.shape[i] for i in (1, 2, 4, 5))
    bases, channels = dual_coeffs.shape[:2]
    margin = row_taps.shape[1] // 2
    count = lax.axis_size("chan")
    single = not in_parts(count)
    image = sky_image.reshape(facet_cols, facet_rows, strip_rows, lanes)
    dirty = dirty_image.reshape(image.shape)
    counts = uv_weights.reshape(uv_weights.shape[1:])
    dual = dual_coeffs.reshape(bases, channels, strip_rows, lanes)
    mask = support_mask.reshape(strip_rows, lanes)
    halo = 2 * margin
    top_rows, low_rows = dual[:, :, :halo], dual[:, :, strip_rows - halo :]
    if facet_rows == 1:
        ends = jnp.where(lax.axis_index("split") == 0, low_rows, top_rows)
        above = below = swapped(ends)
    else:
        above = along_chain(low_rows, 1, facet_rows)
        below = along_chain(top_rows, -1, facet_rows)
    other_image = swapped(image)
    other_counts = swapped(counts)
    other_dirty = swapped(dirty)
    if single:
        blocks = [all_adjoint(dual, above, below, row_taps, col_taps, facet_rows)]
        far = blocks
    else:
        adjoint = functools.partial(part_adjoint, dual, above, below, row_taps, col_taps)
        far = adjoint(tuple(range(count // 2, count)), facet_rows, row_taps)
        near = adjoint(tuple(range(count // 2)), facet_rows, far[0])
        blocks = [*near, *far]
    freq, kept, sent = spectrum(image, other_image, counts, other_counts, margin, blocks[0])
    arrived = crossed(blocks, single)
    got = swapped(sent)
    stepped, edges, pixels = gradient_step(
        kept, got, freq, image, other_image, dirty, other_dirty, margin
    )
    new_image, blocks = update_step(stepped, edges, pixels, arrived, margin, single)
    arrived = crossed(blocks, single)
    if single:
        new_dual = shrink_step(row_taps, col_taps, mask, dual, arrived, single)
    else:
        shrink = functools.partial(shrink_part, row_taps, col_taps, dual)
        middle = count // 2
        earlier = shrink(arrived[:middle], tuple(range(middle)))
        new_dual = shrink(arrived[middle:], tuple(range(middle, count)), (mask, *earlier))
    return (new_image.reshape(sky_image.shape), new_dual.reshape(dual_coeffs.shape))


def solution(mesh):
    placed = (
        P(("cube", "chan"), None, None, "split", None, None),
        P(("cube", "chan"), None, None, "split", None, None),
        P(("cube", "chan"), "split", None),
        P(None, "cube", "chan", "split", None, None),
        P("chan", "split", None, None),
        P(),
        P(),
    )

    mapped = jax.shard_map(
        per_device,
        mesh=mesh,
        in_specs=placed,
        out_specs=(
            P(("cube", "chan"), None, None, "split", None, None),
            P(None, "cube", "chan", "split", None, None),
        ),
        check_vma=False,
    )
    count = mesh.shape["chan"]
    if not in_parts(count):
        return mapped
    return mapped
```

```python
import functools
import math

import jax
import jax.numpy as jnp
import numpy as np
from jax import lax
from jax.experimental import pallas as pl
from jax.experimental.pallas import tpu as pltpu
from jax.sharding import PartitionSpec as P


LANES = 128
WIDE = 2 * LANES
BAND_ROWS = 224
primal_step = 0.5
dual_step = 0.5
radius = 6.0
weight_unit = 0.25

OWN_COPIES = pltpu.CompilerParams(vmem_limit_bytes=67043328)
SOME_ROOM = pltpu.CompilerParams(vmem_limit_bytes=41943040)


def held_inside(values):
    return [pltpu.with_memory_space_constraint(value, pltpu.VMEM) for value in values]


def held_outside(values):
    return [pltpu.with_memory_space_constraint(value, pltpu.HBM) for value in values]


def whole_block(shape):
    zeros = (0,) * len(shape)
    return pl.BlockSpec(tuple(shape), lambda *_: zeros)


def in_scalar_memory():
    return pl.BlockSpec(memory_space=pltpu.SMEM)


def exact_dot(left, right):
    return jnp.dot(left, right, preferred_element_type=jnp.float32)


def each(count, body):
    if count <= 8:
        for index in range(count):
            body(index)
    else:

        def step(index, carry):
            body(index)
            return carry

        lax.fori_loop(0, count, step, 0)


def hint(value, multiple):
    return value if isinstance(value, int) else pl.multiple_of(value, multiple)


def band_seed(taps, basis, positions):
    lane = lax.broadcasted_iota(jnp.int32, (8, WIDE), 1)
    row = lax.broadcasted_iota(jnp.int32, (8, WIDE), 0)
    offset = lane - row & WIDE - 1
    seed = jnp.zeros((8, WIDE), jnp.float32)
    for tap, position in enumerate(positions):
        seed = jnp.where(offset == position % WIDE, taps[basis, tap], seed)
    return seed


def fill_band(target, first_row, rows, seed):
    for start in range(0, rows, 16):
        upper = seed if start == 0 else pltpu.roll(seed, start, axis=1)
        lower = pltpu.roll(seed, start + 8, axis=1)
        target[first_row + start : first_row + start + 16, :] = jnp.concatenate(
            [upper, lower], axis=0
        ).astype(jnp.bfloat16)


def fill_col_bands(target, taps, bases, margin):
    for basis in range(bases):
        count = taps.shape[1]
        seed = band_seed(taps, basis, [tap - margin for tap in range(count)])
        fill_band(target, basis * LANES, LANES, seed)


def pack_height(rows):
    return -(-rows // (8 * 16)) * 16


def payload_rows(rows):
    return rows + pack_height(rows)


def row_groups(rows):
    height = pack_height(rows)
    return [(g, g * height, min(height, rows - g * height)) for g in range(-(-rows // height))]


def padded_rows(strip_rows):
    chunks = -(-strip_rows // BAND_ROWS)
    return (chunks - 1) * BAND_ROWS + WIDE


def edge_band_of(taps, basis, margin):
    halo = 2 * margin
    lane = lax.broadcasted_iota(jnp.int32, (halo, LANES), 1)
    row = lax.broadcasted_iota(jnp.int32, (halo, LANES), 0)
    source = jnp.where(
        row < margin,
        jnp.where(lane < 2 * halo, halo + row - lane, -1),
        jnp.where(lane >= 2 * halo, row + 3 * halo - lane, -1),
    )
    edge = jnp.zeros((halo, LANES), jnp.float32)
    for tap in range(taps.shape[1]):
        edge = jnp.where(source == tap, taps[basis, tap], edge)
    return edge


def products(far_re, far_im, near_re, near_im):
    return (
        (far_re * near_re - far_im * near_im).astype(jnp.bfloat16),
        (far_re * near_im + far_im * near_re).astype(jnp.bfloat16),
    )


def fill_transforms(seeds, cosine, sine, freq):
    big_re, big_im, small_re, small_im, even_re, even_im = seeds
    split = lax.axis_index("split")
    coarse = small_re.shape[0]
    half = cosine.shape[0]
    part = half // 2

    def even_rows(group, carry):
        at = pl.ds(pl.multiple_of(group * coarse, coarse), coarse)
        one = pl.ds(group, 1)
        cosine[at, :], sine[at, :] = products(
            even_re[one, :], even_im[one, :], even_re[half // coarse :, :], even_im[half // coarse :, :]
        )
        return carry

    lax.fori_loop(0, half // coarse, even_rows, 0)

    def freq_rows(group, carry):
        at = pl.ds(pl.multiple_of(group * coarse, coarse), coarse)
        one = pl.ds(group, 1)
        for place in range(2):
            side = jnp.where(split == place, 0, 1) * part
            lanes = pl.ds(pl.multiple_of(side, part), part)
            re, im = products(
                big_re[one, lanes], big_im[one, lanes], small_re[:, lanes], small_im[:, lanes]
            )
            freq[at, 2 * place * part : (2 * place + 1) * part] = re
            freq[at, (2 * place + 1) * part : (2 * place + 2) * part] = im
        return carry

    lax.fori_loop(0, 2 * half // coarse, freq_rows, 0)


def fill_adjoint_bands(row_taps, col_taps, row_band, edge_band, col_band, margin):
    bases, taps = row_taps.shape
    for basis in range(bases):
        seed = band_seed(row_taps, basis, [3 * margin - tap for tap in range(taps)])
        fill_band(row_band.at[basis], 0, BAND_ROWS, seed)
        edge_band[basis] = edge_band_of(row_taps, basis, margin).astype(jnp.bfloat16)
    fill_col_bands(col_band, col_taps, bases, margin)


def is_at_ends(facet_rows):
    split = lax.axis_index("split")
    facet_row = lax.rem(lax.axis_index("chan"), facet_rows)
    return (facet_row == 0) & (split == 0), (facet_row == facet_rows - 1) & (split == 1)


def adjoint_of(tall, bands, mixed, wide, strip_rows, margin):
    row_band, edge_band, col_band = bands
    bases = tall.shape[0]
    width = tall.shape[2] // LANES
    halo = 2 * margin
    for basis in range(bases):
        into = slice(basis * LANES, (basis + 1) * LANES)

        def put(first, count, value):
            for side in range(width):
                mixed[side, first : first + count, into] = value[
                    :, side * LANES : (side + 1) * LANES
                ].astype(jnp.bfloat16)

        for first in range(0, strip_rows, BAND_ROWS):
            count = min(BAND_ROWS, strip_rows - first)
            put(first, count, exact_dot(row_band[basis, :count], tall[basis, first : first + WIDE]))
        ends = jnp.concatenate(
            [
                tall[basis, : 2 * halo],
                tall[basis, strip_rows : strip_rows + 2 * halo],
                jnp.zeros((LANES - 4 * halo, width * LANES), jnp.bfloat16),
            ],
            axis=0,
        )
        put(strip_rows, halo, exact_dot(edge_band[basis], ends))
    for side in range(width):
        wide[side] = exact_dot(mixed[side], col_band[...])


def write_payload(out, wide, margin):
    rows = wide.shape[0]
    height = pack_height(rows)
    packed = jnp.zeros((height, LANES), jnp.float32)
    for group, first, count in row_groups(rows):
        out[first : first + count, :] = wide[first : first + count, :LANES].astype(jnp.bfloat16)
        piece = wide[first : first + count, LANES:]
        piece = pltpu.roll(piece, margin + 2 * margin * group, axis=1)
        if count < height:
            piece = jnp.concatenate(
                [piece, jnp.zeros((height - count, LANES), jnp.float32)], axis=0
            )
        packed = packed + piece
    out[rows : rows + height, :] = packed.astype(jnp.bfloat16)


def tall_height(strip_rows, margin):
    return max(padded_rows(strip_rows), strip_rows + 4 * margin)


def band_scratch(bases, margin):
    return [
        pltpu.VMEM((bases, BAND_ROWS, WIDE), jnp.bfloat16),
        pltpu.VMEM((bases, 2 * margin, LANES), jnp.bfloat16),
        pltpu.VMEM((bases * LANES, WIDE), jnp.bfloat16),
    ]


def all_adjoint_kernel(row_taps, col_taps, dual, above, below, out, *scratch, margin, facet_rows):
    bands, (tall, mixed, wide) = scratch[:3], scratch[3:]
    bases, width, strip_rows, _ = dual.shape
    halo = 2 * margin

    @pl.when(pl.program_id(0) == 0)
    def _():
        fill_adjoint_bands(row_taps, col_taps, *bands, margin)
        tall[...] = jnp.zeros(tall.shape, tall.dtype)

    is_top, is_low = is_at_ends(facet_rows)
    for basis in range(bases):
        for side in range(width):
            lanes = slice(side * LANES, (side + 1) * LANES)
            top = above[basis, side]
            low = below[basis, side]
            tall[basis, :halo, lanes] = jnp.where(is_top, jnp.zeros_like(top), top)
            tall[basis, halo : halo + strip_rows, lanes] = dual[basis, side]
            tall[basis, halo + strip_rows : 2 * halo + strip_rows, lanes] = jnp.where(
                is_low, jnp.zeros_like(low), low
            )
    adjoint_of(tall, bands, mixed, wide, strip_rows, margin)
    for side in range(width):
        write_payload(out.at[side], wide.at[side], margin)


def all_adjoint(dual, above, below, row_taps, col_taps, facet_rows):
    bases, count, strip_rows, _ = dual.shape
    margin = row_taps.shape[1] // 2
    width = 2 if count % 2 == 0 else 1
    rows = strip_rows + 2 * margin

    def picked(height):
        return pl.BlockSpec((bases, width, height, LANES), lambda j: (0, j, 0, 0))

    return pl.pallas_call(
        functools.partial(all_adjoint_kernel, margin=margin, facet_rows=facet_rows),
        out_shape=jax.ShapeDtypeStruct((count, payload_rows(rows), LANES), jnp.bfloat16),
        grid=(count // width,),
        in_specs=[in_scalar_memory()] * 2
        + [picked(height) for height in (strip_rows, 2 * margin, 2 * margin)],
        out_specs=pl.BlockSpec((width, payload_rows(rows), LANES), lambda j: (j, 0, 0)),
        scratch_shapes=band_scratch(bases, margin)
        + [
            pltpu.VMEM((bases, tall_height(strip_rows, margin), width * LANES), jnp.bfloat16),
            pltpu.VMEM((width, rows, bases * LANES), jnp.bfloat16),
            pltpu.VMEM((width, rows, WIDE), jnp.float32),
        ],
        name="all_adjoint",
    )(row_taps, col_taps, dual, above, below)


def part_scratch(bases, strip_rows, margin, count):
    rows = strip_rows + 2 * margin
    height = tall_height(strip_rows, margin)
    return band_scratch(bases, margin) + [
        pltpu.VMEM((-(-count // 2), bases, height, 2 * LANES), jnp.bfloat16),
        pltpu.VMEM((2, rows, bases * LANES), jnp.bfloat16),
        pltpu.VMEM((2, rows, WIDE), jnp.float32),
        pltpu.SemaphoreType.DMA((count,)),
    ]


class PartAdjoint:
    def __init__(self, places, dual, above, below, outs, scratch, facet_rows):
        *self.bands, self.tall, self.mixed, self.wide, loads = scratch
        self.places, self.outs = places, outs
        self.strip_rows = dual.shape[2]
        self.halo = above.shape[2]
        self.margin = self.halo // 2
        self.ends = is_at_ends(facet_rows)
        me = lax.axis_index("chan")
        self.above, self.below = above, below
        self.copies = []
        for at, place in enumerate(places):
            lanes = pl.ds(at % 2 * LANES, LANES)
            self.copies.append(
                pltpu.make_async_copy(
                    dual.at[:, me ^ place],
                    self.tall.at[at // 2, :, pl.ds(self.halo, self.strip_rows), lanes],
                    loads.at[at],
                )
            )

    def start(self):
        for copy in self.copies:
            copy.start()

    def fill(self, row_taps, col_taps):
        fill_adjoint_bands(row_taps, col_taps, *self.bands, self.margin)
        used = self.strip_rows + 2 * self.halo
        pairs, bases, height, lanes = self.tall.shape
        is_top, is_low = self.ends
        me = lax.axis_index("chan")
        for at, place in enumerate(self.places):
            mine = slice(at % 2 * LANES, (at % 2 + 1) * LANES)
            for basis in range(bases):
                top = self.above[basis, me ^ place]
                low = self.below[basis, me ^ place]
                self.tall[at // 2, basis, : self.halo, mine] = jnp.where(
                    is_top, jnp.zeros_like(top), top
                )
                self.tall[at // 2, basis, used - self.halo : used, mine] = jnp.where(
                    is_low, jnp.zeros_like(low), low
                )
        if used < height:
            blank = jnp.zeros((height - used, lanes), jnp.bfloat16)
            for pair in range(pairs):
                for basis in range(bases):
                    self.tall[pair, basis, used:] = blank

    def run(self):
        strip_rows = self.strip_rows
        for pair in range(len(self.places) // 2):
            for copy in self.copies[2 * pair : 2 * pair + 2]:
                copy.wait()
            adjoint_of(
                self.tall.at[pair], self.bands, self.mixed, self.wide, strip_rows, self.margin
            )
            for side in range(2):
                at = 2 * pair + side
                write_payload(self.outs[at], self.wide.at[side], self.margin)


def part_adjoint_kernel(row_taps, col_taps, dual, above, below, _, *rest, places, facet_rows):
    count = len(places)
    part = PartAdjoint(places, dual, above, below, rest[:count], rest[count:], facet_rows)
    part.start()
    part.fill(row_taps, col_taps)
    part.run()


def part_adjoint(dual, above, below, row_taps, col_taps, places, facet_rows, after):
    bases, _, strip_rows, _ = dual.shape
    margin = row_taps.shape[1] // 2
    anywhere = pl.BlockSpec(memory_space=pltpu.HBM)
    rows = payload_rows(strip_rows + 2 * margin)
    return pl.pallas_call(
        functools.partial(part_adjoint_kernel, places=places, facet_rows=facet_rows),
        out_shape=[pltpu.VMEM((rows, LANES), jnp.bfloat16)] * len(places),
        in_specs=[in_scalar_memory()] * 2
        + [anywhere]
        + [pl.BlockSpec(memory_space=pltpu.VMEM)] * 2
        + [pl.BlockSpec(memory_space=pl.ANY)],
        out_specs=[pl.BlockSpec(memory_space=pltpu.VMEM)] * len(places),
        scratch_shapes=part_scratch(bases, strip_rows, margin, len(places)),
        compiler_params=SOME_ROOM,
        name="part_adjoint",
    )(*held_outside((row_taps, col_taps, dual)), *held_inside((above, below)), after)


def phase_seeds(pixels):
    step = 2.0 * math.pi / pixels
    coarse = 32
    half = pixels // 2
    scale = 1.0 / math.sqrt(pixels)
    where = np.arange(half)

    def of(rows, factor):
        angle = rows[:, None] * where[None, :] % pixels * step
        return np.cos(angle) * factor, -np.sin(angle) * factor

    big = of(np.arange(pixels // coarse) * coarse, 1.0)
    small = of(np.arange(coarse), scale)
    far = of(np.arange(half // coarse) * coarse * 2, 1.0)
    near = of(np.arange(coarse) * 2, scale)
    even = tuple(np.concatenate([x, y], axis=0) for x, y in zip(far, near))
    return tuple(np.asarray(v, np.float32) for v in (*big, *small, *even))


def twiddles(pixels):
    angle = 2.0 * math.pi / pixels * np.arange(pixels // 2)[:, None] * np.ones((1, LANES))
    return tuple(np.asarray(v, np.float32) for v in (np.cos(angle), -np.sin(angle)))


def spectrum_kernel(
    own, other, own_counts, other_counts, *rest, margin
):
    seeds, (turn_from_re, turn_from_im, _) = rest[:6], rest[6:9]
    freq, keep, send = rest[9:12]
    picture, counts, cosine, sine, turn_re, turn_im, top, low, whole, wide, loads = rest[12:]
    split = lax.axis_index("split")
    cols, facet_rows, strip_rows, _ = own.shape
    pixels = picture.shape[0]
    half = pixels // 2
    part = half // 2

    def strip_at(facet_row, which):
        return pl.multiple_of((2 * facet_row + which) * strip_rows, strip_rows)

    copies = []
    for source, target in ((turn_from_re, turn_re), (turn_from_im, turn_im)):
        copies.append(pltpu.make_async_copy(source, target, loads.at[len(copies)]))
    for copy in copies:
        copy.start()
    fill_transforms(seeds, cosine, sine, freq)
    for facet_row in range(facet_rows):
        for source, which in ((own, split), (other, 1 - split)):
            there = pl.ds(strip_at(facet_row, which), strip_rows)
            for col in range(cols):
                picture[there, col * LANES : (col + 1) * LANES] = source[col, facet_row]
    for tile in range(part // LANES):
        lanes = pl.ds(pl.multiple_of(split * part + tile * LANES, LANES), LANES)
        for source, which in ((own_counts, split), (other_counts, 1 - split)):
            there = pl.ds(pl.multiple_of(which * half, half), half)
            counts[tile, there, :] = source[:, lanes]
    for copy in copies:
        copy.wait()
    block = min(256, half)
    first_table = freq.at[:, pl.ds(0, half)]

    def first(step, carry):
        at = pl.ds(pl.multiple_of(step * block, block), block)
        beyond = pl.ds(pl.multiple_of(half + step * block, block), block)
        one = exact_dot(picture[at, :], first_table[...])
        two = exact_dot(picture[beyond, :], first_table[...])
        total = one + two
        apart = one - two
        re, im = apart[:, :part], apart[:, part:]
        turn_r = jnp.concatenate([turn_re[at, :]] * (part // LANES), axis=1)
        turn_i = jnp.concatenate([turn_im[at, :]] * (part // LANES), axis=1)
        odd_re = (re * turn_r - im * turn_i).astype(jnp.bfloat16)
        odd_im = (re * turn_i + im * turn_r).astype(jnp.bfloat16)
        sum_re = total[:, :part].astype(jnp.bfloat16)
        sum_im = total[:, part:].astype(jnp.bfloat16)
        for place, value in enumerate((sum_re, sum_im, odd_re, odd_im)):
            top[at, place * part : (place + 1) * part] = value
        for place, value in enumerate((-sum_im, sum_re, -odd_im, odd_re)):
            low[at, place * part : (place + 1) * part] = value
        return carry

    lax.fori_loop(0, half // block, first, 0)

    def second(step, carry):
        at = pl.ds(pl.multiple_of(step * block, block), block)
        vis = exact_dot(cosine[at, :], top[...]) + exact_dot(sine[at, :], low[...])
        for parity in range(2):
            picked = jnp.concatenate(
                [
                    counts.at[tile][pl.ds(2 * step * block + parity, block, stride=2), :]
                    for tile in range(part // LANES)
                ],
                axis=1,
            )
            scale = weight_unit * picked.astype(jnp.float32)
            re = parity * 2 * part
            im = re + part
            whole[at, re : re + part] = (vis[:, re : re + part] * scale).astype(jnp.bfloat16)
            whole[at, im : im + part] = (vis[:, im : im + part] * scale).astype(jnp.bfloat16)
        return carry

    lax.fori_loop(0, half // block, second, 0)
    for parity in range(2):
        re = slice(parity * 2 * part, (parity * 2 + 1) * part)
        im = slice((parity * 2 + 1) * part, (parity * 2 + 2) * part)
        low[:, re] = whole[:, im]
        low[:, im] = -whole[:, re]

    def third(step, carry):
        at = pl.ds(pl.multiple_of(step * block, block), block)
        beyond = pl.ds(pl.multiple_of(half + step * block, block), block)
        value = exact_dot(cosine[at, :], whole[...]) + exact_dot(sine[at, :], low[...])
        even, re, im = value[:, :half], value[:, half : half + part], value[:, half + part :]
        turn_r = jnp.concatenate([turn_re[at, :]] * (part // LANES), axis=1)
        turn_i = jnp.concatenate([turn_im[at, :]] * (part // LANES), axis=1)
        odd = jnp.concatenate([re * turn_r + im * turn_i, im * turn_r - re * turn_i], axis=1)
        wide[at, :] = (even + odd).astype(jnp.bfloat16)
        wide[beyond, :] = (even - odd).astype(jnp.bfloat16)
        return carry

    lax.fori_loop(0, half // block, third, 0)
    rows = strip_rows + 2 * margin
    for facet_row in range(facet_rows):
        for target, which in ((keep, split), (send, 1 - split)):
            at = strip_at(facet_row, which)
            base = facet_row * rows
            target[base : base + strip_rows, :] = wide[pl.ds(at, strip_rows), :]
            before = pl.multiple_of(lax.rem(at + pixels - 16, pixels), 16)
            after = pl.multiple_of(lax.rem(at + strip_rows, pixels), 16)
            ends = jnp.concatenate(
                [
                    wide[pl.ds(before, 16), :].astype(jnp.float32)[16 - margin :],
                    wide[pl.ds(after, 16), :].astype(jnp.float32)[:margin],
                ],
                axis=0,
            )
            target[base + strip_rows : base + rows, :] = ends.astype(jnp.bfloat16)


def spectrum(own, other, own_counts, other_counts, margin, after):
    cols, facet_rows, strip_rows, lanes = own.shape
    pixels = cols * lanes
    half = pixels // 2
    rows = facet_rows * (strip_rows + 2 * margin)
    anywhere = pl.BlockSpec(memory_space=pltpu.HBM)
    inside = pl.BlockSpec(memory_space=pltpu.VMEM)
    return pl.pallas_call(
        functools.partial(spectrum_kernel, margin=margin),
        out_shape=[
            pltpu.VMEM((pixels, pixels), jnp.bfloat16),
            pltpu.VMEM((rows, half), jnp.bfloat16),
            pltpu.VMEM((rows, half), jnp.bfloat16),
        ],
        in_specs=[inside] * 4
        + [inside] * 6
        + [anywhere] * 2
        + [pl.BlockSpec(memory_space=pl.ANY)],
        out_specs=[inside] * 3,
        scratch_shapes=[
            pltpu.VMEM((pixels, pixels), jnp.bfloat16),
            pltpu.VMEM((half // 2 // LANES, pixels, LANES), jnp.int32),
            pltpu.VMEM((half, half), jnp.bfloat16),
            pltpu.VMEM((half, half), jnp.bfloat16),
            pltpu.VMEM((half, LANES), jnp.float32),
            pltpu.VMEM((half, LANES), jnp.float32),
            pltpu.VMEM((half, pixels), jnp.bfloat16),
            pltpu.VMEM((half, pixels), jnp.bfloat16),
            pltpu.VMEM((half, pixels), jnp.bfloat16),
            pltpu.VMEM((pixels, half), jnp.bfloat16),
            pltpu.SemaphoreType.DMA((2,)),
        ],
        compiler_params=SOME_ROOM,
        name="spectrum",
    )(
        *held_inside((own, other, own_counts, other_counts)),
        *phase_seeds(pixels), *twiddles(pixels), after,
    )


def gradient_kernel(
    kept, got, freq, own, other, dirty, other_dirty, stepped, edge_out, joined, *, margin
):
    split = lax.axis_index("split")
    cols, facet_rows, strip_rows, _ = own.shape
    half = kept.shape[1]
    rows = strip_rows + 2 * margin
    pair = 2 if cols % 2 == 0 else 1

    def edges(source, col, facet_row):
        over = jnp.maximum(facet_row - 1 + split, 0)
        under = jnp.minimum(facet_row + split, facet_rows - 1)
        return jnp.concatenate(
            [
                source[col, over, strip_rows - 16 :].astype(jnp.float32)[16 - margin :],
                source[col, under, :16].astype(jnp.float32)[:margin],
            ],
            axis=0,
        )

    joined[:, :half] = kept[...]
    joined[:, half:] = got[...]
    for step in range(cols // pair):
        value = lax.dot_general(
            joined[...],
            freq[step * pair * LANES : (step + 1) * pair * LANES, :],
            (((1,), (1,)), ((), ())),
            preferred_element_type=jnp.float32,
        )
        for side in range(pair):
            col = step * pair + side
            for facet_row in range(facet_rows):
                base = facet_row * rows
                grad = value[base : base + rows, side * LANES : (side + 1) * LANES]
                moved = own[col, facet_row].astype(jnp.float32) - primal_step * (
                    grad[:strip_rows] - dirty[col, facet_row].astype(jnp.float32)
                )
                stepped[col, facet_row, :strip_rows] = moved.astype(jnp.bfloat16)
                image = edges(other, col, facet_row)
                moved = image - primal_step * (
                    grad[strip_rows:] - edges(other_dirty, col, facet_row)
                )
                stepped[col, facet_row, strip_rows:] = moved.astype(jnp.bfloat16)
                edge_out[col, facet_row] = image.astype(jnp.bfloat16)


def gradient_step(kept, got, freq, own, other, own_dirty, other_dirty, margin):
    cols, facet_rows, strip_rows, lanes = own.shape
    pixels = cols * lanes
    rows = strip_rows + 2 * margin
    anywhere = pl.BlockSpec(memory_space=pltpu.HBM)
    inside = pl.BlockSpec(memory_space=pltpu.VMEM)
    return pl.pallas_call(
        functools.partial(gradient_kernel, margin=margin),
        out_shape=[
            pltpu.VMEM((cols, facet_rows, rows, lanes), jnp.bfloat16),
            pltpu.VMEM((cols, facet_rows, 2 * margin, lanes), jnp.bfloat16),
        ],
        in_specs=[inside] * 7,
        out_specs=[inside] * 2,
        scratch_shapes=[pltpu.VMEM((kept.shape[0], pixels), jnp.bfloat16)],
        compiler_params=SOME_ROOM,
        name="gradient",
    )(
        *held_inside((kept, got, freq, own, other, own_dirty, other_dirty))
    )


def unpacked(packed, group, count, margin):
    return pltpu.roll(
        packed[:count], LANES - (margin + 2 * margin * group) % LANES, axis=1
    )


def update_kernel(stepped, edges, image, *rest, margin, facets, single):
    arrivals = 1 if single else facets
    blocks = rest[:arrivals]
    new_out = rest[arrivals]
    outs = rest[arrivals + 1 : 2 * arrivals + 1]
    new_image, adjoint, apart, extrapolated, stores = rest[2 * arrivals + 1 :]
    me = lax.axis_index("chan")
    split = lax.axis_index("split")
    cols, facet_rows, rows, _ = stepped.shape
    strip_rows = rows - 2 * margin
    height = pack_height(rows)
    lane = lax.broadcasted_iota(jnp.int32, (1, LANES), 1)

    def unpack(facet):
        tile = adjoint[facet, rows : rows + height, :].astype(jnp.float32)
        for group, first, count in row_groups(rows):
            apart[facet, first : first + count, :] = unpacked(
                tile, group, count, margin
            ).astype(jnp.bfloat16)

    if single:
        adjoint = blocks[0]
        each(facets, unpack)
    else:
        for place, block in enumerate(blocks):
            adjoint[me ^ place] = block[...]
            unpack(me ^ place)

    def sides(take, group, count, left, has_left, right, has_right):
        from_left = take(left, group, count)
        from_right = take(right, group, count)
        return (
            jnp.where(lane < jnp.where(has_left, margin, 0), from_left, 0.0),
            jnp.where(lane >= jnp.where(has_right, LANES - margin, LANES), from_right, 0.0),
        )

    def apart_of(facet, group, count):
        first = group * height
        return apart[facet, first : first + count, :].astype(jnp.float32)

    def update(facet):
        col = facet // facet_rows
        facet_row = facet % facet_rows
        left, has_left = jnp.maximum(facet - facet_rows, 0), facet >= facet_rows
        right, has_right = jnp.minimum(facet + facet_rows, facets - 1), facet < facets - facet_rows
        for group, first, count in row_groups(rows):
            add_left, add_right = sides(apart_of, group, count, left, has_left, right, has_right)
            at = slice(first, first + count)
            total = adjoint[facet, at, :].astype(jnp.float32) + add_left + add_right
            value = stepped[col, facet_row, at, :].astype(jnp.float32) - primal_step * total
            value = jnp.maximum(value, 0.0).astype(jnp.bfloat16).astype(jnp.float32)
            main = max(min(first + count, strip_rows) - first, 0)
            before = []
            if main > 0:
                before.append(image[col, facet_row, first : first + main, :].astype(jnp.float32))
            if main < count:
                after = first + main - strip_rows
                before.append(
                    edges[col, facet_row, after : after + count - main, :].astype(jnp.float32)
                )
            ahead = 2.0 * value - (before[0] if len(before) == 1 else jnp.concatenate(before, 0))
            if first + count > strip_rows:
                row = first + lax.broadcasted_iota(jnp.int32, (count, LANES), 0)
                top_there = (facet_row > 0) | (split > 0)
                low_there = (facet_row < facet_rows - 1) | (split < 1)
                middle = strip_rows + margin
                from_top = jnp.where(top_there, middle, strip_rows)
                to_low = jnp.where(low_there, rows, middle)
                ahead = jnp.where((row >= from_top) & (row < middle), 0.0, ahead)
                ahead = jnp.where(row >= to_low, 0.0, ahead)
            extrapolated[facet, at, :] = ahead.astype(jnp.bfloat16)
            if main > 0:
                new_image[col, facet_row, first : first + main, :] = value[:main].astype(jnp.bfloat16)

    stored = []
    for col in range(cols):
        for facet_row in range(facet_rows):
            update(col * facet_rows + facet_row)
        stored.append(
            pltpu.make_async_copy(new_image.at[col], new_out.at[col], stores.at[col])
        )
        stored[-1].start()

    def whole_of(facet, group, count):
        first = group * height
        return extrapolated[facet, first : first + count, :].astype(jnp.float32)

    def write(out, facet):
        left, has_left = jnp.maximum(facet - facet_rows, 0), facet >= facet_rows
        right, has_right = jnp.minimum(facet + facet_rows, facets - 1), facet < facets - facet_rows
        packed = jnp.zeros((height, LANES), jnp.float32)
        for group, first, count in row_groups(rows):
            after, before = sides(whole_of, group, count, right, has_right, left, has_left)
            side = pltpu.roll(after + before, margin + 2 * margin * group, axis=1)
            if count < height:
                side = jnp.concatenate(
                    [side, jnp.zeros((height - count, LANES), jnp.float32)], axis=0
                )
            packed = packed + side
        out[:rows, :] = extrapolated[facet]
        out[rows:, :] = packed.astype(jnp.bfloat16)

    if single:
        each(facets, lambda facet: write(outs[0].at[facet], facet))
    else:
        for place, out in enumerate(outs):
            write(out, me ^ place)
    for copy in stored:
        copy.wait()


def update_step(stepped, edges, image, blocks, margin, single):
    cols, facet_rows, rows, lanes = stepped.shape
    facets = cols * facet_rows
    tall_rows = payload_rows(rows)
    arrivals = (
        [pltpu.VMEM((facets, tall_rows, lanes), jnp.bfloat16)]
        if single
        else [pltpu.VMEM((tall_rows, lanes), jnp.bfloat16)] * facets
    )
    anywhere = pl.BlockSpec(memory_space=pltpu.HBM)
    results = pl.pallas_call(
        functools.partial(update_kernel, margin=margin, facets=facets, single=single),
        out_shape=[
            jax.ShapeDtypeStruct((cols, facet_rows, rows - 2 * margin, lanes), jnp.bfloat16)
        ]
        + arrivals,
        in_specs=[pl.BlockSpec(memory_space=pltpu.VMEM)] * (3 + len(blocks)),
        out_specs=[anywhere] + [pl.BlockSpec(memory_space=pltpu.VMEM)] * len(arrivals),
        scratch_shapes=[
            pltpu.VMEM(image.shape, jnp.bfloat16),
            pltpu.VMEM((1, 16, lanes) if single else (facets, tall_rows, lanes), jnp.bfloat16),
            pltpu.VMEM((facets, rows, lanes), jnp.bfloat16),
            pltpu.VMEM((facets, rows, lanes), jnp.bfloat16),
            pltpu.SemaphoreType.DMA((cols,)),
        ],
        compiler_params=SOME_ROOM,
        name="update",
    )(*held_inside((stepped, edges, image, *blocks)))
    return results[0], results[1:]


def shrink_kernel(row_taps, col_taps, mask, dual, *rest, margin, channels, single):
    arrivals = 1 if single else channels
    blocks = rest[:arrivals]
    out = rest[arrivals]
    row_band, col_band, wide, tall = rest[arrivals + 1 :]
    me = lax.axis_index("chan")
    basis = pl.program_id(0)
    taps = row_taps.shape[1]
    halo = 2 * margin
    strip_rows = dual.shape[2]
    rows = strip_rows + halo
    height = pack_height(rows)

    @pl.when(basis == 0)
    def _():
        for each_basis in range(row_taps.shape[0]):
            seed = band_seed(row_taps, each_basis, [margin + tap for tap in range(taps)])
            fill_band(row_band.at[each_basis], 0, BAND_ROWS, seed)
            seed = band_seed(col_taps, each_basis, [tap - margin for tap in range(taps)])
            fill_band(col_band.at[each_basis], 0, LANES, seed)
        tall[...] = jnp.zeros(tall.shape, tall.dtype)

        def unpack(channel, block):
            wide[channel, :, :LANES] = block[:rows, :]
            packed = block[rows : rows + height, :].astype(jnp.float32)
            for group, first, count in row_groups(rows):
                side = unpacked(packed, group, count, margin)
                wide[channel, first : first + count, LANES:] = side.astype(jnp.bfloat16)

        if single:
            each(channels, lambda channel: unpack(channel, blocks[0].at[channel]))
        else:
            for place, block in enumerate(blocks):
                unpack(me ^ place, block)

    def columns(channel):
        lanes = pl.ds(hint(channel * LANES, LANES), LANES)
        value = lax.dot_general(
            wide[channel], col_band[basis], (((1,), (1,)), ((), ())),
            preferred_element_type=jnp.float32,
        )
        blank = jnp.zeros((halo - margin, LANES), jnp.float32)
        tall[halo : halo + strip_rows, lanes] = value[:strip_rows].astype(jnp.bfloat16)
        tall[:halo, lanes] = jnp.concatenate(
            [blank, value[strip_rows : strip_rows + margin]], axis=0
        ).astype(jnp.bfloat16)
        tall[halo + strip_rows : 2 * halo + strip_rows, lanes] = jnp.concatenate(
            [value[strip_rows + margin :], blank], axis=0
        ).astype(jnp.bfloat16)

    each(channels, columns)
    piece = min(channels, 8)
    for first in range(0, strip_rows, BAND_ROWS):
        count = min(BAND_ROWS, strip_rows - first)
        stepped = []
        total = jnp.zeros((count, LANES), jnp.float32)
        for channel in range(0, channels, piece):
            value = exact_dot(
                row_band[basis, :count],
                tall[first : first + WIDE, channel * LANES : (channel + piece) * LANES],
            )
            for side in range(piece):
                coefficient = value[:, side * LANES : (side + 1) * LANES]
                moved = (
                    dual[0, channel + side, first : first + count].astype(jnp.float32)
                    + dual_step * coefficient
                )
                stepped.append(moved)
                total = total + moved * moved
        kept = mask[first : first + count].astype(jnp.float32)
        shrink = radius * kept / jnp.maximum(jnp.sqrt(total), radius)
        for channel in range(channels):
            out[0, channel, first : first + count] = (stepped[channel] * shrink).astype(jnp.bfloat16)


def shrink_step(row_taps, col_taps, mask, dual, blocks, single):
    bases, channels, strip_rows, lanes = dual.shape
    margin = row_taps.shape[1] // 2
    rows = strip_rows + 2 * margin
    return pl.pallas_call(
        functools.partial(shrink_kernel, margin=margin, channels=channels, single=single),
        out_shape=jax.ShapeDtypeStruct(dual.shape, jnp.bfloat16),
        grid=(bases,),
        in_specs=[
            in_scalar_memory(),
            in_scalar_memory(),
            whole_block(mask.shape),
            pl.BlockSpec((1, channels, strip_rows, lanes), lambda n: (n, 0, 0, 0)),
        ]
        + [whole_block(block.shape) for block in blocks],
        out_specs=pl.BlockSpec((1, channels, strip_rows, lanes), lambda n: (n, 0, 0, 0)),
        scratch_shapes=[
            pltpu.VMEM((bases, BAND_ROWS, WIDE), jnp.bfloat16),
            pltpu.VMEM((bases, LANES, WIDE), jnp.bfloat16),
            pltpu.VMEM((channels, rows, WIDE), jnp.bfloat16),
            pltpu.VMEM((max(padded_rows(strip_rows), strip_rows + 4 * margin), channels * lanes), jnp.bfloat16),
        ],
        name="shrink",
    )(row_taps, col_taps, mask, dual, *blocks)


def shrink_part_kernel(row_taps, col_taps, dual, *rest, places, margin, final):
    count = len(places)
    blocks, rest = rest[:count], rest[count:]
    if final:
        mask, before, total, field, out_to = rest[:5]
        row_band, col_band, wide, tall, held, scaled, loads, stores = rest[5:]
    else:
        held, total, ahead = rest[:3]
        row_band, col_band, wide, tall, field, loads, stores = rest[3:]
    me = lax.axis_index("chan")
    bases, taps = row_taps.shape
    halo = 2 * margin
    strip_rows = dual.shape[2]
    rows = strip_rows + halo
    height = pack_height(rows)
    started = []

    def load(source, target):
        copy = pltpu.make_async_copy(source, target, loads.at[len(started)])
        copy.start()
        started.append(copy)
        return copy

    stored = []

    def store(source, target):
        copy = pltpu.make_async_copy(source, target, stores.at[len(stored)])
        copy.start()
        stored.append(copy)

    fields = []
    for basis in range(0 if final else bases):
        fields.append(
            [
                load(dual.at[basis, me ^ place], field.at[basis, at])
                for at, place in enumerate(places)
            ]
        )
    further = []
    for basis in range(0 if final else bases):
        for at, place in enumerate(places):
            further.append(load(dual.at[basis, me ^ place ^ count], ahead.at[basis, at]))
    for basis in range(bases):
        seed = band_seed(row_taps, basis, [margin + tap for tap in range(taps)])
        fill_band(row_band.at[basis], 0, BAND_ROWS, seed)
        used = strip_rows + 2 * halo
        if used < tall.shape[1]:
            tall[basis, used:] = jnp.zeros((tall.shape[1] - used, tall.shape[2]), jnp.bfloat16)
    fill_col_bands(col_band, col_taps, bases, margin)
    for at in range(count):
        block = blocks[at]
        wide[at, :, :LANES] = block[:rows, :]
        packed = block[rows : rows + height, :].astype(jnp.float32)
        for group, first, some in row_groups(rows):
            side = unpacked(packed, group, some, margin)
            wide[at, first : first + some, LANES:] = side.astype(jnp.bfloat16)
        value = lax.dot_general(
            wide[at], col_band[...], (((1,), (1,)), ((), ())), preferred_element_type=jnp.float32
        )
        blank = jnp.zeros((halo - margin, LANES), jnp.float32)
        lanes = slice(at * LANES, (at + 1) * LANES)
        for basis in range(bases):
            mine = value[:, basis * LANES : (basis + 1) * LANES]
            tall[basis, halo : halo + strip_rows, lanes] = mine[:strip_rows].astype(jnp.bfloat16)
            tall[basis, :halo, lanes] = jnp.concatenate(
                [blank, mine[strip_rows : strip_rows + margin]], axis=0
            ).astype(jnp.bfloat16)
            tall[basis, halo + strip_rows : 2 * halo + strip_rows, lanes] = jnp.concatenate(
                [mine[strip_rows + margin :], blank], axis=0
            ).astype(jnp.bfloat16)
    for basis in range(bases):
        if not final:
            for copy in fields[basis]:
                copy.wait()
        for first in range(0, strip_rows, BAND_ROWS):
            some = min(BAND_ROWS, strip_rows - first)
            here = slice(first, first + some)
            value = exact_dot(row_band[basis, :some], tall[basis, first : first + WIDE])
            if final:
                squares = total[basis, here]
            else:
                squares = jnp.zeros((some, LANES), jnp.float32)
            stepped = []
            for at in range(count):
                moved = (
                    field[basis, at, here].astype(jnp.float32)
                    + dual_step * value[:, at * LANES : (at + 1) * LANES]
                )
                stepped.append(moved)
                squares = squares + moved * moved
            if final:
                kept = mask[here].astype(jnp.float32)
                scale = radius * kept / jnp.maximum(jnp.sqrt(squares), radius)
                for at in range(count):
                    held[basis, at, here] = (stepped[at] * scale).astype(jnp.bfloat16)
                    earlier = before[basis, at, here].astype(jnp.float32)
                    scaled[basis, at, here] = (earlier * scale).astype(jnp.bfloat16)
            else:
                total[basis, here] = squares
                for at in range(count):
                    held[basis, at, here] = stepped[at].astype(jnp.bfloat16)
        if final:
            for at, place in enumerate(places):
                store(held.at[basis, at], out_to.at[basis, me ^ place])
                store(scaled.at[basis, at], out_to.at[basis, me ^ place ^ count])
    for copy in (*stored, *further):
        copy.wait()


def shrink_part(row_taps, col_taps, dual, blocks, places, earlier=None):
    bases, _, strip_rows, lanes = dual.shape
    count = len(places)
    margin = row_taps.shape[1] // 2
    rows = strip_rows + 2 * margin
    anywhere = pl.BlockSpec(memory_space=pltpu.HBM)
    part = (bases, count, strip_rows, lanes)
    final = earlier is not None
    inside = pl.BlockSpec(memory_space=pltpu.VMEM)
    bands = [
        pltpu.VMEM((bases, BAND_ROWS, WIDE), jnp.bfloat16),
        pltpu.VMEM((bases * LANES, WIDE), jnp.bfloat16),
        pltpu.VMEM((count, rows, WIDE), jnp.bfloat16),
        pltpu.VMEM((bases, tall_height(strip_rows, margin), count * lanes), jnp.bfloat16),
    ]
    field = pltpu.VMEM(part, jnp.bfloat16)
    if final:
        out_shape = jax.ShapeDtypeStruct(dual.shape, jnp.bfloat16)
        out_specs = anywhere
        scratch = [field, field]
    else:
        earlier = ()
        out_shape = [field, pltpu.VMEM((bases, strip_rows, lanes), jnp.float32), field]
        out_specs = [inside] * 3
        scratch = [field]
    return pl.pallas_call(
        functools.partial(shrink_part_kernel, places=places, margin=margin, final=final),
        out_shape=out_shape,
        in_specs=[in_scalar_memory()] * 2 + [anywhere] + [inside] * (count + len(earlier)),
        out_specs=out_specs,
        scratch_shapes=bands
        + scratch
        + [
            pltpu.SemaphoreType.DMA((2 * bases * count,)),
            pltpu.SemaphoreType.DMA((2 * bases * count,)),
        ],
        compiler_params=SOME_ROOM,
        name="shrink_part",
    )(
        *held_outside((row_taps, col_taps, dual)),
        *held_inside((*blocks, *earlier)),
    )


def swapped(value):
    return lax.ppermute(value, "split", [(0, 1), (1, 0)])


def along_chain(value, by, facet_rows):
    count = lax.axis_size("chan") * 2
    chain = 2 * facet_rows
    pairs = [
        (i, i + by) for i in range(count) if 0 <= i + by < count and i // chain == (i + by) // chain
    ]
    return lax.ppermute(value, ("chan", "split"), pairs)


def crossed(blocks, single):
    count = lax.axis_size("chan")
    if single:
        return [lax.all_to_all(blocks[0], "chan", split_axis=0, concat_axis=0, tiled=True)]
    result = list(blocks)
    for place in reversed(range(1, count)):
        result[place] = lax.ppermute(blocks[place], "chan", [(i, i ^ place) for i in range(count)])
    return result


def in_parts(count):
    return 4 <= count <= 8 and count & count - 1 == 0


def per_device(sky_image, dirty_image, uv_weights, dual_coeffs, support_mask, row_taps, col_taps):
    facet_cols, facet_rows, strip_rows, lanes = (sky_image.shape[i] for i in (1, 2, 4, 5))
    bases, channels = dual_coeffs.shape[:2]
    margin = row_taps.shape[1] // 2
    count = lax.axis_size("chan")
    single = not in_parts(count)
    image = sky_image.reshape(facet_cols, facet_rows, strip_rows, lanes)
    dirty = dirty_image.reshape(image.shape)
    counts = uv_weights.reshape(uv_weights.shape[1:])
    dual = dual_coeffs.reshape(bases, channels, strip_rows, lanes)
    mask = support_mask.reshape(strip_rows, lanes)
    halo = 2 * margin
    top_rows, low_rows = dual[:, :, :halo], dual[:, :, strip_rows - halo :]
    if facet_rows == 1:
        ends = jnp.where(lax.axis_index("split") == 0, low_rows, top_rows)
        above = below = swapped(ends)
    else:
        above = along_chain(low_rows, 1, facet_rows)
        below = along_chain(top_rows, -1, facet_rows)
    other_image = swapped(image)
    other_counts = swapped(counts)
    other_dirty = swapped(dirty)
    if single:
        blocks = [all_adjoint(dual, above, below, row_taps, col_taps, facet_rows)]
        far = blocks
    else:
        adjoint = functools.partial(part_adjoint, dual, above, below, row_taps, col_taps)
        far = adjoint(tuple(range(count // 2, count)), facet_rows, row_taps)
        near = adjoint(tuple(range(count // 2)), facet_rows, far[0])
        blocks = [*near, *far]
    freq, kept, sent = spectrum(image, other_image, counts, other_counts, margin, blocks[0])
    arrived = crossed(blocks, single)
    got = swapped(sent)
    stepped, edges = gradient_step(
        kept, got, freq, image, other_image, dirty, other_dirty, margin
    )
    new_image, blocks = update_step(stepped, edges, image, arrived, margin, single)
    arrived = crossed(blocks, single)
    if single:
        new_dual = shrink_step(row_taps, col_taps, mask, dual, arrived, single)
    else:
        shrink = functools.partial(shrink_part, row_taps, col_taps, dual)
        middle = count // 2
        earlier = shrink(arrived[:middle], tuple(range(middle)))
        new_dual = shrink(arrived[middle:], tuple(range(middle, count)), (mask, *earlier))
    return (new_image.reshape(sky_image.shape), new_dual.reshape(dual_coeffs.shape))


def solution(mesh):
    placed = (
        P(("cube", "chan"), None, None, "split", None, None),
        P(("cube", "chan"), None, None, "split", None, None),
        P(("cube", "chan"), "split", None),
        P(None, "cube", "chan", "split", None, None),
        P("chan", "split", None, None),
        P(),
        P(),
    )

    mapped = jax.shard_map(
        per_device,
        mesh=mesh,
        in_specs=placed,
        out_specs=(
            P(("cube", "chan"), None, None, "split", None, None),
            P(None, "cube", "chan", "split", None, None),
        ),
        check_vma=False,
    )
    count = mesh.shape["chan"]
    if not in_parts(count):
        return mapped
    return mapped
```
